32 devices in a mesh: gz: 32 (over z, y, x, core).
Axes of the slice: x: 2, y: 2, z: 4, core: 2. Of those that a mesh axis runs over, the one named last changes fastest.
Arguments:
- u_face: float32 [64, 1024, 512], P('gz')
- v_face: float32 [64, 1024, 512], P('gz')
- w_face: float32 [64, 1024, 512], P('gz')
- smoke: float32 [64, 1024, 512], P('gz'), may hold values from 0 to 2
- obstacles: int32 [64, 32, 512], P('gz'), may hold values from -2147483648 to 2147483647, as said below
Outputs:
- impulse: float32 [64, 1024, 512], P('gz')
- relative_residual: float32 [64, 1024, 512], P('gz')
The draws below stay inside these ranges and needn't reach their ends.
Inputs may be any that keep to these rules, and one draw needn't show every extreme that they name: Bit k of obstacles[z, b, x] is 1 where cell (z, 32 b + k, x) is solid and 0 where it holds fluid; every bit of a word is used.
All inputs are finite; a program needn't handle non-finite values. Where the reference program divides by a largest or mean magnitude, that divisor is 1e-20 or more.
Results may differ from the reference program's by a relative error of at most 0.00011.
Values sent between devices are 32-bit elements; how exact they have to be, the bound alone decides.
A program may use at most 192 MiB of HBM per device.

```python
import jax
import jax.numpy as jnp
from jax import lax

NX = 512
NY = 1024
ITERS = 2
NZ = 64


def velocity_field(key):
    first = jax.random.fold_in(key, 0)
    depth = jnp.arange(NZ, dtype=jnp.float32) / max(NZ - 1, 1)
    ramp = 1.0 + 2.0 * depth[:, None, None]
    base = jax.random.normal(first, (NZ, NY, NX), jnp.float32)
    return jnp.clip(base, -6.0, 6.0) * ramp


def draw_u_face(key, part):
    return velocity_field(jax.random.fold_in(key, 11))


def draw_v_face(key, part):
    return velocity_field(jax.random.fold_in(key, 23))


def draw_w_face(key, part):
    return velocity_field(jax.random.fold_in(key, 37))


def draw_obstacles(key, part):
    first, second = jax.random.split(jax.random.fold_in(key, 53))
    shape = (NZ, NY // 32, NX)
    left = jax.random.randint(first, shape, -2147483648, 2147483647, dtype=jnp.int32)
    right = jax.random.randint(second, shape, -2147483648, 2147483647, dtype=jnp.int32)
    return left & right


def levels(stream_key, shape, cuts, smallest, largest):
    gain, own = 1.0, jax.random.fold_in(stream_key, 6)
    for position, blocks in cuts:
        steps = jnp.exp(jax.random.uniform(jax.random.fold_in(own, position), (blocks,), jnp.float32, smallest / len(cuts), largest / len(cuts)))
        gain = gain * jnp.repeat(steps, shape[position] // blocks).reshape([-1 if axis == position else 1 for axis in range(len(shape))])
    return gain


def setup_inputs(seed: int = 0) -> dict:
    splits = jax.random.split(jax.random.key(seed), 6)
    return {
        "u_face": draw_u_face(jax.random.fold_in(splits[5], 71), 0),
        "v_face": draw_v_face(jax.random.fold_in(splits[5], 71), 0),
        "w_face": draw_w_face(jax.random.fold_in(splits[5], 71), 0),
        "smoke": jnp.clip(2.0 * jax.random.uniform(splits[3], (NZ, NY, NX), jnp.float32) ** levels(splits[3], (NZ, NY, NX), ((0, 32),), -0.2, 0.2), 0.0, 2.0),
        "obstacles": draw_obstacles(jax.random.fold_in(splits[5], 71), 0),
    }


EPS = 1e-06
CFL = 0.5
BUOYANCY = 100.0

def unpack_flags(packed):
    places = jnp.arange(32, dtype=jnp.int32)
    flags = jnp.right_shift(packed[:, :, None, :], places[None, None, :, None]) & 1
    return flags.reshape(packed.shape[0], packed.shape[1] * 32, packed.shape[2])

def next_along(field, axis):
    widths = [(0, 0), (0, 0), (0, 0)]
    widths[axis] = (0, 1)
    padded = jnp.pad(field, widths)
    return lax.slice_in_dim(padded, 1, field.shape[axis] + 1, axis=axis)

def neighbour_sum(field):
    padded = jnp.pad(field, 1)
    total = padded[2:, 1:-1, 1:-1] + padded[:-2, 1:-1, 1:-1]
    total = total + padded[1:-1, 2:, 1:-1] + padded[1:-1, :-2, 1:-1]
    return total + padded[1:-1, 1:-1, 2:] + padded[1:-1, 1:-1, :-2]

def reference(u_face, v_face, w_face, smoke, obstacles):
    solid_cells = unpack_flags(obstacles).astype(jnp.float32)
    fluid_cells = 1.0 - solid_cells
    fastest = jnp.maximum(jnp.maximum(jnp.max(jnp.abs(u_face)), jnp.max(jnp.abs(v_face))), jnp.max(jnp.abs(w_face)))
    time_step = CFL / (fastest + EPS)
    lift = time_step * BUOYANCY
    lifted_w = w_face + lift * smoke
    divergence = fluid_cells * (next_along(u_face, 2) - u_face + (next_along(v_face, 1) - v_face) + (next_along(lifted_w, 0) - lifted_w))
    div_squares = jnp.sum(divergence * divergence)
    fluid_total = jnp.maximum(jnp.sum(fluid_cells), 1.0)
    open_count = 6.0 - neighbour_sum(solid_cells)
    scaling = fluid_cells * jnp.maximum(open_count, 1.0) + solid_cells

    def apply_operator(search):
        return fluid_cells * (open_count * search - neighbour_sum(fluid_cells * search)) + solid_cells * search
    residual = divergence / time_step
    solution = jnp.zeros_like(residual)
    search = residual / scaling
    rz_now = jnp.sum(residual * residual / scaling)
    for step in range(ITERS):
        image = apply_operator(search)
        alpha = rz_now / jnp.sum(search * image)
        solution = solution + alpha * search
        residual = residual - alpha * image
        if step + 1 < ITERS:
            precond = residual / scaling
            rz_next = jnp.sum(residual * precond)
            search = precond + rz_next / rz_now * search
            rz_now = rz_next
    impulse = time_step * solution
    relative_residual = residual * time_step / jnp.sqrt(div_squares / fluid_total + EPS)
    return (impulse, relative_residual)
```

```python
import functools

import jax
import jax.numpy as jnp
from jax import lax
from jax.experimental import pallas as pl
from jax.experimental.pallas import tpu as pltpu
from jax.sharding import PartitionSpec as P

EPS = 1e-06
CFL = 0.5
BUOYANCY = 100.0

ROWS = 32
PAD = 8


def kernel(n, chunks, u_hbm, v_hbm, w_hbm, s_hbm, ob_hbm, w, s,
           u, v, z, y, code, ay, lw, lw_next, ob, cw, acc, cf, mx, mx_all, st, st_all,
           in_sem, ob_send, ob_recv, lw_send, lw_recv, dn_send, dn_recv, up_send, up_recv,
           mx_send, mx_recv, st_send, st_recv):
    depth, ny, nx = w.shape
    nb = ny // ROWS
    crow = ny // chunks
    me = lax.axis_index("gz")
    has_low, has_high = me > 0, me < n - 1
    low, high = jnp.maximum(me - 1, 0), jnp.minimum(me + 1, n - 1)

    def at(device):
        return dict(device_id=(device,), device_id_type=pl.DeviceIdType.MESH)

    ins = [(u_hbm, u), (v_hbm, v), (w_hbm, w), (s_hbm, s)]

    def load(k, p):
        src, dst = ins[k]
        return pltpu.make_async_copy(src.at[p], dst.at[p, pl.ds(0, ny)], in_sem.at[k * depth + p])

    ob_in = pltpu.make_async_copy(ob_hbm, ob.at[pl.ds(2, depth)], in_sem.at[4 * depth])
    ob_in.start()
    for k in range(4):
        for p in range(depth):
            load(k, p).start()

    barrier = pltpu.get_barrier_semaphore()

    def greet(i, carry):
        pl.semaphore_signal(barrier, inc=1, **at(lax.rem(me + i, n)))
        return carry

    lax.fori_loop(1, n, greet, 0)

    zrow = jnp.zeros((PAD, nx), jnp.float32)
    for p in range(depth + 4):
        z[p, 0:PAD, :] = zrow
        z[p, ny + PAD : ny + 2 * PAD, :] = zrow
    for p in range(depth + 2):
        y[p, 0:PAD, :] = zrow
        y[p, ny + PAD : ny + 2 * PAD, :] = zrow
    for p in range(depth):
        v[p, ny : ny + PAD, :] = zrow
    acc[...] = jnp.zeros_like(acc)

    def zero_planes(ref, planes, offset):
        def body(i, carry):
            for p in planes:
                ref[p, pl.ds(pl.multiple_of(i * ROWS + offset, 8), ROWS), :] = jnp.zeros((ROWS, nx), jnp.float32)
            return carry
        lax.fori_loop(0, nb, body, 0)

    ob_in.wait()
    pl.semaphore_wait(barrier, n - 1)

    ob_down = pltpu.make_async_remote_copy(
        ob.at[pl.ds(2, 2)], ob.at[pl.ds(depth + 2, 2)], ob_send.at[0], ob_recv.at[0], **at(low))
    ob_up = pltpu.make_async_remote_copy(
        ob.at[pl.ds(depth, 2)], ob.at[pl.ds(0, 2)], ob_send.at[1], ob_recv.at[1], **at(high))

    @pl.when(has_low)
    def _():
        ob_down.start()

    @pl.when(has_high)
    def _():
        ob_up.start()

    @pl.when(jnp.logical_not(has_low))
    def _():
        ob[0:2] = jnp.zeros((2,) + ob.shape[1:], jnp.int32)
        zero_planes(z, (0, 1), PAD)

    @pl.when(jnp.logical_not(has_high))
    def _():
        ob[depth + 2 : depth + 4] = jnp.zeros((2,) + ob.shape[1:], jnp.int32)
        zero_planes(z, (depth + 2, depth + 3), PAD)
        zero_planes(lw_next, (0,), 0)

    mx[...] = jnp.zeros_like(mx)
    for k in range(3):
        ref = ins[k][1]
        for p in range(depth):
            load(k, p).wait()

            def body(i, m, ref=ref, p=p):
                a = jnp.abs(ref[p, pl.ds(pl.multiple_of(i * ROWS, 8), ROWS), :])
                return jnp.maximum(m, jnp.max(a.reshape(ROWS // 8, 8, nx), axis=0))

            m = lax.fori_loop(0, nb, body, jnp.zeros((8, nx), jnp.float32))
            m = jnp.max(m, axis=0, keepdims=True)
            for c in range(0, nx, 128):
                mx[...] = jnp.maximum(mx[...], jnp.broadcast_to(m[:, c : c + 128], mx.shape))

    def spread(src, dst, send, recv):
        def copy(i):
            return pltpu.make_async_remote_copy(
                src, dst.at[i], send.at[i], recv.at[i], **at(lax.rem(me + i, n)))

        def start(i, carry):
            copy(i).start()
            return carry

        def wait(i, carry):
            copy(i).wait_recv()
            copy(i).wait_send()
            return carry

        return (lambda: lax.fori_loop(1, n, start, 0)), (lambda: lax.fori_loop(1, n, wait, 0))

    mx_start, mx_wait = spread(mx, mx_all, mx_send, mx_recv)
    mx_start()

    @pl.when(has_low)
    def _():
        ob_down.wait_send()
        ob_up.wait_recv()

    @pl.when(has_high)
    def _():
        ob_up.wait_send()
        ob_down.wait_recv()

    row_id = lax.broadcasted_iota(jnp.int32, (nb, nx), 0)
    col_id = lax.broadcasted_iota(jnp.int32, (nb, nx), 1)
    srl = lax.shift_right_logical
    c1, c31 = jnp.int32(1), jnp.int32(31)
    full1, full31 = jnp.full((nb, nx), c1), jnp.full((nb, nx), c31)
    for p in range(depth + 2):
        mid = ob[p + 1]
        after = jnp.where(row_id == nb - 1, 0, pltpu.roll(mid, nb - 1, 0))
        before = jnp.where(row_id == 0, 0, pltpu.roll(mid, 1, 0))
        a = srl(mid, full1) | (after << full31)
        b = (mid << full1) | srl(before, full31)
        c = jnp.where(col_id == nx - 1, 0, pltpu.roll(mid, nx - 1, 1))
        d = jnp.where(col_id == 0, 0, pltpu.roll(mid, 1, 1))
        e, f = ob[p], ob[p + 2]
        s1, k1 = a ^ b ^ c, (a & b) | (c & (a | b))
        s2, k2 = d ^ e ^ f, (d & e) | (f & (d | e))
        k3 = s1 & s2
        cw[p, 0] = s1 ^ s2
        cw[p, 1] = k1 ^ k2 ^ k3
        cw[p, 2] = (k1 & k2) | (k3 & (k1 | k2))
        outside = None
        if p == 0:
            outside = jnp.logical_not(has_low)
        if p == depth + 1:
            outside = jnp.logical_not(has_high)
        cw[p, 3] = mid
        if outside is not None:
            @pl.when(outside)
            def _(p=p):
                cw[p, 3] = jnp.full((nb, nx), -1, jnp.int32)

    half = 16
    places = lax.broadcasted_iota(jnp.int32, (half, nx), 0)

    def code_rows(b, carry):
        for p in range(depth + 2):
            for k0 in range(0, ROWS, half):
                bits = [
                    srl(jnp.broadcast_to(cw[p, j, pl.ds(b, 1), :], (half, nx)), places + k0) & 1
                    for j in range(4)
                ]
                count = bits[0] + (bits[1] << 1) + (bits[2] << 2)
                code[p, pl.ds(pl.multiple_of(b * ROWS + k0, 8), half), :] = jnp.where(
                    bits[3] == 1, -1, 6 - count).astype(jnp.float32)
        return carry

    for p in range(depth):
        load(3, p).wait()
    mx_wait()
    mx_all[0] = mx[...]
    top = jnp.max(jnp.max(mx_all[...], axis=0), axis=1, keepdims=True)[0:1]
    top = jnp.broadcast_to(top, (1, nx))
    cf[0:1, :] = (CFL / (top + EPS)) * BUOYANCY

    lane = lax.broadcasted_iota(jnp.int32, (ROWS, nx), 1)

    def lifted(p, r):
        rows = pl.ds(r, ROWS)
        return w[p, rows, :] + cf[0:1, :] * s[p, rows, :]

    def chunked(prepare, compute, sends):
        def body(c, carry):
            @pl.when(c < chunks)
            def _():
                prepare(c)

                def inner(i, k):
                    compute(pl.multiple_of(c * crow + i * ROWS, 8))
                    return k
                lax.fori_loop(0, crow // ROWS, inner, 0)

            @pl.when(c > 0)
            def _():
                for cond, copy in sends:
                    @pl.when(cond)
                    def _(copy=copy):
                        copy(c - 1)
            return carry
        lax.fori_loop(0, chunks + 1, body, 0)

    def lw_copy(c):
        rows = pl.ds(pl.multiple_of(c * crow, 8), crow)
        return pltpu.make_async_remote_copy(
            lw.at[0, rows], lw_next.at[0, rows], lw_send.at[c], lw_recv.at[c], **at(low))

    def lw_rows(r):
        lw[0, pl.ds(r, ROWS), :] = lifted(0, r)

    chunked(lambda c: None, lw_rows, [(has_low, lambda c: lw_copy(c).start())])
    lax.fori_loop(0, nb, code_rows, 0)

    def z_copy(src, dst, send, recv, base, device):
        def copy(c):
            rows = pl.ds(pl.multiple_of(c * crow + PAD, 8), crow)
            return pltpu.make_async_remote_copy(
                z.at[src, rows], z.at[dst, rows], send.at[base + c], recv.at[base + c], **at(device))
        return copy

    down = [z_copy(2 + j, depth + 2 + j, dn_send, dn_recv, j * chunks, low) for j in range(2)]
    up = [z_copy(depth + j, j, up_send, up_recv, j * chunks, high) for j in range(2)]

    def z_rows(p, r):
        rows = pl.ds(r, ROWS)
        a = u[p, rows, :]
        flat = jnp.where(lane == nx - 1, 0.0, pltpu.roll(a, nx - 1, 1)) - a
        b = v[p, pl.ds(r, ROWS + PAD), :]
        flat = flat + (b[1 : ROWS + 1] - b[:ROWS])
        above = lifted(p + 1, r) if p + 1 < depth else lw_next[0, rows, :]
        own = lw[0, rows, :] if p == 0 else lifted(p, r)
        div = flat + (above - own)
        k = code[p + 1, rows, :]
        z[p + 2, pl.ds(pl.multiple_of(r + PAD, 8), ROWS), :] = (
            jnp.where(k >= 0.0, div, 0.0) / jnp.maximum(k, 1.0))

    def gated(before, copy):
        def start(c):
            before(c).wait_send()
            copy(c).start()
        return start

    top_plane = [] if depth > 2 else [(has_high, lambda c: up[0](c).start())]
    chunked(lambda c: None, functools.partial(z_rows, 0), top_plane)
    for p in range(1, depth - 1):
        sends = [(has_high, lambda c: up[0](c).start())] if p == depth - 2 else []
        chunked(lambda c: None, functools.partial(z_rows, p), sends)

    def above_wait(c):
        @pl.when(has_high)
        def _():
            lw_copy(c).wait_recv()

    chunked(above_wait, functools.partial(z_rows, depth - 1),
            [(has_high, gated(up[0], up[1])), (has_low, gated(lw_copy, down[0]))])

    def wait_all(cond, copy):
        def body(c, carry):
            @pl.when(cond)
            def _():
                copy(c).wait_recv()
            return carry
        lax.fori_loop(0, chunks, body, 0)

    def image(ref, slot, zm, zp, r, k):
        x = ref[slot, pl.ds(r, ROWS + 2 * PAD), :]
        mid = x[PAD : PAD + ROWS]
        beside = x[PAD + 1 : PAD + 1 + ROWS] + x[PAD - 1 : PAD - 1 + ROWS]
        beside = beside + jnp.where(lane == nx - 1, 0.0, pltpu.roll(mid, nx - 1, 1))
        beside = beside + jnp.where(lane == 0, 0.0, pltpu.roll(mid, 1, 1))
        beside = beside + zm + zp
        return mid, jnp.where(k >= 0.0, k * mid - beside, mid)

    def add(j, x):
        acc[j] += jnp.sum(x.reshape(ROWS // 8, 8, nx), axis=0)

    def y_rows(p, r):
        inner = pl.ds(pl.multiple_of(r + PAD, 8), ROWS)
        k = code[p + 1, pl.ds(r, ROWS), :]
        mid, q = image(z, p + 2, z[p + 1, inner, :], z[p + 3, inner, :], r, k)
        scaling = jnp.maximum(k, 1.0)
        out = q / scaling
        y[p + 1, inner, :] = out
        if 0 <= p < depth:
            d = scaling * mid
            add(0, d * mid)
            add(1, d * d)
            add(2, jnp.where(k >= 0.0, 1.0, 0.0))
            add(3, mid * q)
            add(4, q * out)

    def a_rows(p, r):
        inner = pl.ds(pl.multiple_of(r + PAD, 8), ROWS)
        k = code[p + 1, pl.ds(r, ROWS), :]
        mid, q = image(y, p + 1, y[p, inner, :], y[p + 2, inner, :], r, k)
        ay[p, pl.ds(r, ROWS), :] = q
        add(5, mid * q)

    def sweep(fn):
        def body(i, carry):
            fn(pl.multiple_of(i * ROWS, 8))
            return carry
        lax.fori_loop(0, nb, body, 0)

    for p in range(1, depth - 1):
        sweep(functools.partial(y_rows, p))
    wait_all(has_low, up[0])

    def push(c, carry):
        @pl.when(has_low)
        def _():
            gated(down[0], down[1])(c)
        return carry

    lax.fori_loop(0, chunks, push, 0)

    def middle(c, carry):
        def over(c, fn):
            def inner(i, k):
                fn(pl.multiple_of(c * crow + i * ROWS, 8))
                return k
            lax.fori_loop(0, crow // ROWS, inner, 0)

        def ahead(r):
            for p in sorted({0, depth - 1, depth}):
                y_rows(p, r)

        def behind(r):
            y_rows(-1, r)
            for p in range(depth):
                a_rows(p, r)

        @pl.when(c < chunks)
        def _():
            @pl.when(has_low)
            def _():
                up[1](c).wait_recv()

            @pl.when(has_high)
            def _():
                down[1](c).wait_recv()

                @pl.when(c == 0)
                def _():
                    down[0](0).wait_recv()

                @pl.when(c + 1 < chunks)
                def _():
                    down[0](c + 1).wait_recv()

            over(c, ahead)

        @pl.when(c > 0)
        def _():
            over(c - 1, behind)
        return carry

    lax.fori_loop(0, chunks + 1, middle, 0)

    for j in range(6):
        t = jnp.sum(acc[j], axis=0, keepdims=True)
        part = t[:, 0:128]
        for c in range(128, nx, 128):
            part = part + t[:, c : c + 128]
        st[j : j + 1, :] = part
    st[6:8, :] = jnp.zeros((2, 128), jnp.float32)
    st_start, st_wait = spread(st, st_all, st_send, st_recv)
    st_start()

    def drain(c, carry):
        @pl.when(has_low)
        def _():
            down[1](c).wait_send()

        @pl.when(has_high)
        def _():
            up[1](c).wait_send()
        return carry

    lax.fori_loop(0, chunks, drain, 0)
    st_wait()
    st_all[0] = st[...]
    total = jnp.sum(jnp.sum(st_all[...], axis=0), axis=1, keepdims=True)
    total = jnp.broadcast_to(total, (8, nx))
    gamma, squares, fluid = total[0:1], total[1:2], total[2:3]
    delta, eta, theta = total[3:4], total[4:5], total[5:6]
    alpha = gamma / delta
    gamma_next = gamma - 2.0 * alpha * delta + alpha * alpha * eta
    beta = gamma_next / gamma
    mixed = delta - alpha * eta
    curve = (delta - 2.0 * alpha * eta + alpha * alpha * theta) + 2.0 * beta * mixed + beta * beta * delta
    alpha_next = gamma_next / curve
    cf[1:2, :] = alpha + alpha_next * (1.0 + beta)
    cf[2:3, :] = alpha * alpha_next
    cf[3:4, :] = 1.0 / jnp.sqrt(squares / jnp.maximum(fluid, 1.0) + EPS)

    for p in range(depth):
        def out_rows(r, p=p):
            inner = pl.ds(pl.multiple_of(r + PAD, 8), ROWS)
            rows = pl.ds(r, ROWS)
            zz, yy = z[p + 2, inner, :], y[p + 1, inner, :]
            scaling = jnp.maximum(code[p + 1, rows, :], 1.0)
            a, b = cf[1:2, :], cf[2:3, :]
            w[p, rows, :] = a * zz - b * yy
            s[p, rows, :] = (scaling * (zz - a * yy) + b * ay[p, rows, :]) * cf[3:4, :]

        sweep(out_rows)


def solution(mesh):
    n = mesh.shape["gz"]

    def local(u_face, v_face, w_face, smoke, obstacles):
        depth, ny, nx = u_face.shape
        nw = obstacles.shape[1]
        chunks = 8
        f32, i32 = jnp.float32, jnp.int32
        dma = pltpu.SemaphoreType.DMA
        any_spec = pl.BlockSpec(memory_space=pl.ANY)
        shape = pltpu.VMEM((depth, ny, nx), f32)
        vmem_spec = pl.BlockSpec(memory_space=pltpu.VMEM)
        return pl.pallas_call(
            functools.partial(kernel, n, chunks),
            out_shape=(shape, shape),
            in_specs=[any_spec] * 5,
            out_specs=(vmem_spec, vmem_spec),
            scratch_shapes=[
                pltpu.VMEM((depth, ny, nx), f32),
                pltpu.VMEM((depth, ny + PAD, nx), f32),
                pltpu.VMEM((depth + 4, ny + 2 * PAD, nx), f32),
                pltpu.VMEM((depth + 2, ny + 2 * PAD, nx), f32),
                pltpu.VMEM((depth + 2, ny, nx), f32),
                pltpu.VMEM((depth, ny, nx), f32),
                pltpu.VMEM((1, ny, nx), f32),
                pltpu.VMEM((1, ny, nx), f32),
                pltpu.VMEM((depth + 4, nw, nx), i32),
                pltpu.VMEM((depth + 2, 4, nw, nx), i32),
                pltpu.VMEM((6, 8, nx), f32),
                pltpu.VMEM((8, nx), f32),
                pltpu.VMEM((8, 128), f32),
                pltpu.VMEM((n, 8, 128), f32),
                pltpu.VMEM((8, 128), f32),
                pltpu.VMEM((n, 8, 128), f32),
                dma((4 * depth + 1,)),
                dma((2,)), dma((2,)),
                dma((chunks,)), dma((chunks,)),
                dma((2 * chunks,)), dma((2 * chunks,)),
                dma((2 * chunks,)), dma((2 * chunks,)),
                dma((n,)), dma((n,)),
                dma((n,)), dma((n,)),
            ],
            compiler_params=pltpu.CompilerParams(
                collective_id=0, has_side_effects=True, vmem_limit_bytes=58_000_000),
            name="smoke_step",
        )(u_face, v_face, w_face, smoke, obstacles)

    placed = P("gz", None, None)
    return jax.shard_map(local, mesh=mesh, in_specs=(placed,) * 5, out_specs=(placed, placed), check_vma=False)
```

```python
import functools

import jax
import jax.numpy as jnp
from jax import lax
from jax.experimental import pallas as pl
from jax.experimental.pallas import tpu as pltpu
from jax.sharding import PartitionSpec as P

EPS = 1e-06
CFL = 0.5
BUOYANCY = 100.0

ROWS = 32
PAD = 8


def kernel(n, chunks, raw, u_hbm, v_hbm, w_hbm, s_hbm, ob_hbm, w, s,
           u, v, z, y, code, inv, ay, lw, lw_next, s_next, ob, cw, acc, cf, mx, mx_all, st, st_pair, st_all, total,
           in_sem, ob_send, ob_recv, raw_send, raw_recv, lw_send, lw_recv, dn_send, dn_recv, up_send, up_recv,
           yd_send, yd_recv, mx_send, mx_recv, st_send, st_recv, pair_send, pair_recv):
    depth, ny, nx = w.shape
    top = depth - 1
    nb = ny // ROWS
    crow = ny // chunks
    me = lax.axis_index("gz")
    has_low, has_high = me > 0, me < n - 1
    low, high = jnp.maximum(me - 1, 0), jnp.minimum(me + 1, n - 1)
    odd = lax.rem(me, 2) == 1
    even = jnp.logical_not(odd)
    partner = me + 1 - 2 * lax.rem(me, 2)

    def at(device):
        return dict(device_id=(device,), device_id_type=pl.DeviceIdType.MESH)

    ins = [(u_hbm, u), (v_hbm, v), (w_hbm, w), (s_hbm, s)]

    def load(k, p, first=0, rows=ny, sem=None):
        src, dst = ins[k]
        part = pl.ds(first, rows)
        return pltpu.make_async_copy(src.at[p, part], dst.at[p, part], in_sem.at[k * depth + p if sem is None else sem])

    raw_rows = raw * crow
    ob_in = pltpu.make_async_copy(ob_hbm, ob.at[pl.ds(2, depth)], in_sem.at[4 * depth])
    raw_in = [load(k, 0, 0, raw_rows, 4 * depth + k - 1) for k in (2, 3)]
    rest_in = {(k, p): load(k, p, raw_rows, ny - raw_rows) if k >= 2 and p == 0 else load(k, p)
               for k in range(4) for p in range(depth)}
    ob_in.start()
    for copy in raw_in:
        copy.start()
    for copy in rest_in.values():
        copy.start()

    barrier = pltpu.get_barrier_semaphore()

    def greet(i, carry):
        pl.semaphore_signal(barrier, inc=1, **at(lax.rem(me + i, n)))
        return carry

    lax.fori_loop(1, n, greet, 0)

    zrow = jnp.zeros((PAD, nx), jnp.float32)
    for p in range(1, depth + 2):
        z[p, 0:PAD, :] = zrow
        z[p, ny + PAD : ny + 2 * PAD, :] = zrow
    for p in range(1, depth + 1):
        y[p, 0:PAD, :] = zrow
        y[p, ny + PAD : ny + 2 * PAD, :] = zrow
    for p in range(depth):
        v[p, ny : ny + PAD, :] = zrow
    acc[...] = jnp.zeros_like(acc)

    def zero_planes(ref, planes, offset):
        def body(i, carry):
            for p in planes:
                ref[p, pl.ds(pl.multiple_of(i * ROWS + offset, 8), ROWS), :] = jnp.zeros((ROWS, nx), jnp.float32)
            return carry
        lax.fori_loop(0, nb, body, 0)

    ob_in.wait()
    for copy in raw_in:
        copy.wait()
    pl.semaphore_wait(barrier, n - 1)

    ob_down = pltpu.make_async_remote_copy(
        ob.at[pl.ds(2, 1)], ob.at[pl.ds(depth + 2, 1)], ob_send.at[0], ob_recv.at[0], **at(low))
    ob_up = pltpu.make_async_remote_copy(
        ob.at[pl.ds(depth, 2)], ob.at[pl.ds(0, 2)], ob_send.at[1], ob_recv.at[1], **at(high))

    def raw_copies(c):
        rows = pl.ds(c * crow, crow)
        return [
            pltpu.make_async_remote_copy(
                src.at[0, rows], dst.at[0, rows], raw_send.at[2 * c + j], raw_recv.at[2 * c + j], **at(low))
            for j, (src, dst) in enumerate([(w, lw_next), (s, s_next)])
        ]

    def send_raw(first, last):
        @pl.when(has_low)
        def _():
            for c in range(first, last):
                for copy in raw_copies(c):
                    copy.start()

    @pl.when(has_low)
    def _():
        ob_down.start()

    @pl.when(has_high)
    def _():
        ob_up.start()

    send_raw(0, raw // 2)

    @pl.when(jnp.logical_not(has_low))
    def _():
        ob[0:2] = jnp.zeros((2,) + ob.shape[1:], jnp.int32)
        zero_planes(z, (0, 1), PAD)

    @pl.when(jnp.logical_not(has_high))
    def _():
        ob[depth + 2 : depth + 3] = jnp.zeros((1,) + ob.shape[1:], jnp.int32)
        zero_planes(z, (depth + 2,), PAD)
        zero_planes(lw_next, (0,), 0)

    peak = jnp.zeros((8, nx), jnp.float32)
    for k in range(3):
        ref = ins[k][1]
        for p in range(depth):
            rest_in[k, p].wait()

            def body(i, m, ref=ref, p=p):
                a = jnp.abs(ref[p, pl.ds(pl.multiple_of(i * ROWS, 8), ROWS), :])
                return jnp.maximum(m, jnp.max(a.reshape(ROWS // 8, 8, nx), axis=0))

            peak = lax.fori_loop(0, nb, body, peak)
    m = jnp.max(peak, axis=0, keepdims=True)
    part = m[:, 0:128]
    for c in range(128, nx, 128):
        part = jnp.maximum(part, m[:, c : c + 128])
    mx[...] = part

    def spread(src, dst, send, recv, step, count):
        def copy(i):
            return pltpu.make_async_remote_copy(
                src, dst.at[i], send.at[i], recv.at[i], **at(lax.rem(me + step * i, n)))

        def start(i, carry):
            copy(i).start()
            return carry

        def wait(i, carry):
            copy(i).wait_recv()
            copy(i).wait_send()
            return carry

        return (lambda: lax.fori_loop(1, count, start, 0)), (lambda: lax.fori_loop(1, count, wait, 0))

    mx_start, mx_wait = spread(mx, mx_all, mx_send, mx_recv, 1, n)
    mx_start()
    send_raw(raw // 2, raw)

    @pl.when(has_low)
    def _():
        ob_down.wait_send()
        ob_up.wait_recv()

    @pl.when(has_high)
    def _():
        ob_up.wait_send()
        ob_down.wait_recv()

    row_id = lax.broadcasted_iota(jnp.int32, (nb, nx), 0)
    col_id = lax.broadcasted_iota(jnp.int32, (nb, nx), 1)
    srl = lax.shift_right_logical
    c1, c31 = jnp.int32(1), jnp.int32(31)
    full1, full31 = jnp.full((nb, nx), c1), jnp.full((nb, nx), c31)
    for p in range(depth + 1):
        mid = ob[p + 1]
        after = jnp.where(row_id == nb - 1, 0, pltpu.roll(mid, nb - 1, 0))
        before = jnp.where(row_id == 0, 0, pltpu.roll(mid, 1, 0))
        a = srl(mid, full1) | (after << full31)
        b = (mid << full1) | srl(before, full31)
        c = jnp.where(col_id == nx - 1, 0, pltpu.roll(mid, nx - 1, 1))
        d = jnp.where(col_id == 0, 0, pltpu.roll(mid, 1, 1))
        e, f = ob[p], ob[p + 2]
        s1, k1 = a ^ b ^ c, (a & b) | (c & (a | b))
        s2, k2 = d ^ e ^ f, (d & e) | (f & (d | e))
        k3 = s1 & s2
        cw[p, 0] = s1 ^ s2
        cw[p, 1] = k1 ^ k2 ^ k3
        cw[p, 2] = (k1 & k2) | (k3 & (k1 | k2))
        cw[p, 3] = mid
    @pl.when(jnp.logical_not(has_low))
    def _():
        cw[0, 3] = jnp.full((nb, nx), -1, jnp.int32)

    half = 16
    places = lax.broadcasted_iota(jnp.int32, (half, nx), 0)

    def code_rows(b):
        for p in range(depth + 1):
            for k0 in range(0, ROWS, half):
                bits = [
                    srl(jnp.broadcast_to(cw[p, j, pl.ds(b, 1), :], (half, nx)), places + k0) & 1
                    for j in range(4)
                ]
                k = (6 - (bits[0] + (bits[1] << 1) + (bits[2] << 2))).astype(jnp.float32)
                rows = pl.ds(pl.multiple_of(b * ROWS + k0, 8), half)
                code[p, rows, :] = k
                inv[p, rows, :] = jnp.where(bits[3] == 1, 0.0, 1.0 / jnp.maximum(k, 1.0))

    for p in range(depth):
        rest_in[3, p].wait()
    mx_wait()
    mx_all[0] = mx[...]
    fastest = jnp.max(jnp.max(mx_all[...], axis=0), axis=1, keepdims=True)
    cf[0:1, :] = (CFL / (jnp.broadcast_to(fastest, (1, nx)) + EPS)) * BUOYANCY

    lane = lax.broadcasted_iota(jnp.int32, (ROWS, nx), 1)

    def lifted(p, r):
        rows = pl.ds(r, ROWS)
        return w[p, rows, :] + cf[0:1, :] * s[p, rows, :]

    def over(c, fn):
        def inner(i, k):
            fn(pl.multiple_of(c * crow + i * ROWS, 8))
            return k
        lax.fori_loop(0, crow // ROWS, inner, 0)

    def staged(first, second):
        def body(c, carry):
            @pl.when(c < chunks)
            def _():
                first(c)

            @pl.when(c > 0)
            def _():
                second(c - 1)
            return carry
        lax.fori_loop(0, chunks + 1, body, 0)

    def when(cond, fn):
        @pl.when(cond)
        def _():
            fn()

    def lw_copy(c):
        rows = pl.ds(pl.multiple_of(c * crow, 8), crow)
        return pltpu.make_async_remote_copy(
            lw.at[0, rows], lw_next.at[0, rows], lw_send.at[c], lw_recv.at[c], **at(low))

    def padded_copy(ref, src, dst, send, recv, base, device):
        def copy(c):
            rows = pl.ds(pl.multiple_of(c * crow + PAD, 8), crow)
            return pltpu.make_async_remote_copy(
                ref.at[src, rows], ref.at[dst, rows], send.at[base + c], recv.at[base + c], **at(device))
        return copy

    z_down = padded_copy(z, 2, depth + 2, dn_send, dn_recv, 0, low)
    top_up = padded_copy(z, top + 2, 1, up_send, up_recv, 0, high)
    next_up = padded_copy(z, top + 1, 0, up_send, up_recv, chunks, high)
    y_down = padded_copy(y, 1, depth + 1, yd_send, yd_recv, 0, low)

    def flat(p, r):
        a = u[p, pl.ds(r, ROWS), :]
        b = v[p, pl.ds(r, ROWS + PAD), :]
        return jnp.where(lane == nx - 1, 0.0, pltpu.roll(a, nx - 1, 1)) - a + (b[1 : ROWS + 1] - b[:ROWS])

    def inner_rows(r):
        return pl.ds(pl.multiple_of(r + PAD, 8), ROWS)

    def first_rows(r):
        code_rows(r // ROWS)
        rows = pl.ds(r, ROWS)
        lw[0, rows, :] = lifted(0, r)
        z[top + 2, inner_rows(r), :] = inv[top + 1, rows, :] * (flat(top, r) - lifted(top, r))

    def first_sends(c):
        when(jnp.logical_and(has_low, c >= raw), lambda: lw_copy(c).start())
        when(has_high, lambda: top_up(c).start())

    staged(lambda c: over(c, first_rows), first_sends)

    def z_rows(p, r):
        rows = pl.ds(r, ROWS)
        own = lw[0, rows, :] if p == 0 else lifted(p, r)
        z[p + 2, inner_rows(r), :] = inv[p + 1, rows, :] * (flat(p, r) + (lifted(p + 1, r) - own))

    for p in range(top):
        def z_sends(c, p=p):
            if p == 0:
                when(has_low, lambda: z_down(c).start())
            if p == top - 1:
                when(has_high, lambda: next_up(c).start())
        staged(lambda c, p=p: over(c, functools.partial(z_rows, p)), z_sends)

    @pl.when(has_high)
    def _():
        for c in range(raw):
            for copy in raw_copies(c):
                copy.wait_recv()

        def lift(i, carry):
            rows = pl.ds(pl.multiple_of(i * ROWS, 8), ROWS)
            lw_next[0, rows, :] = lw_next[0, rows, :] + cf[0:1, :] * s_next[0, rows, :]
            return carry

        lax.fori_loop(0, raw_rows // ROWS, lift, 0)

    def around(ref, slot, r):
        x = ref[slot, pl.ds(r, ROWS + 2 * PAD), :]
        mid = x[PAD : PAD + ROWS]
        beside = x[PAD + 1 : PAD + 1 + ROWS] + x[PAD - 1 : PAD - 1 + ROWS]
        beside = beside + jnp.where(lane == nx - 1, 0.0, pltpu.roll(mid, nx - 1, 1))
        beside = beside + jnp.where(lane == 0, 0.0, pltpu.roll(mid, 1, 1))
        return mid, beside

    def add(j, x):
        acc[j] += jnp.sum(x.reshape(ROWS // 8, 8, nx), axis=0)

    def y_rows(p, r):
        inner, rows = inner_rows(r), pl.ds(r, ROWS)
        k, scale = code[p + 1, rows, :], inv[p + 1, rows, :]
        mid, beside = around(z, p + 2, r)
        q = k * mid - (beside + z[p + 1, inner, :] + z[p + 3, inner, :])
        out = q * scale
        y[p + 1, inner, :] = out
        if p >= 0:
            d = jnp.maximum(k, 1.0) * mid
            add(0, d * mid)
            add(1, d * d)
            add(2, jnp.where(scale > 0.0, 1.0, 0.0))
            add(3, mid * q)
            add(4, q * out)

    def complete_rows(r):
        inner, rows = inner_rows(r), pl.ds(r, ROWS)
        z[top + 2, inner, :] = z[top + 2, inner, :] + inv[top + 1, rows, :] * lw_next[0, rows, :]
        z[1, inner, :] = z[1, inner, :] + inv[0, rows, :] * lw[0, rows, :]

    def low_rows(r):
        complete_rows(r)
        for p in range(top):
            y_rows(p, r)

    def low_chunk(c):
        @pl.when(has_high)
        def _():
            when(c >= raw, lambda: lw_copy(c).wait_recv())
            top_up(c).wait_send()

        when(has_low, lambda: top_up(c).wait_recv())
        over(c, low_rows)

    staged(low_chunk, lambda c: when(has_low, lambda: y_down(c).start()))

    def a_rows(p, r):
        inner, rows = inner_rows(r), pl.ds(r, ROWS)
        mid, beside = around(y, p + 1, r)
        below = y[p, inner, :]
        beside = beside + below
        if p < top:
            beside = beside + y[p + 2, inner, :]
        q = code[p + 1, rows, :] * mid - beside
        ay[p, rows, :] = jnp.where(inv[p + 1, rows, :] > 0.0, q, 0.0)
        add(5, mid * (q - below) if p == 0 else mid * q)

    def high_rows(r):
        y_rows(top, r)
        y_rows(-1, r)

    def high_chunk(c):
        when(has_high, lambda: z_down(c).wait_recv())
        when(has_low, lambda: next_up(c).wait_recv())
        over(c, high_rows)

    def image_rows(r):
        for p in range(depth):
            a_rows(p, r)

    staged(high_chunk, lambda c: over(c, image_rows))

    for j in range(6):
        t = jnp.sum(acc[j], axis=0, keepdims=True)
        part = t[:, 0:128]
        for c in range(128, nx, 128):
            part = part + t[:, c : c + 128]
        st[j : j + 1, :] = part
    st[6:8, :] = jnp.zeros((2, 128), jnp.float32)

    pair_in = pltpu.make_async_remote_copy(st, st_pair, pair_send.at[0], pair_recv.at[0], **at(partner))
    pair_out = pltpu.make_async_remote_copy(total, total, pair_send.at[1], pair_recv.at[1], **at(partner))
    st_start, st_wait = spread(st_pair, st_all, st_send, st_recv, 2, n // 2)

    @pl.when(even)
    def _():
        pair_in.start()

    @pl.when(odd)
    def _():
        pair_in.wait_recv()
        st_pair[...] = st_pair[...] + st[...]
        st_start()
        st_wait()
        st_all[0] = st_pair[...]
        total[...] = jnp.sum(st_all[...], axis=0)
        pair_out.start()

    @pl.when(has_low)
    def _():
        for c in range(raw):
            for copy in raw_copies(c):
                copy.wait_send()

    @pl.when(even)
    def _():
        pair_in.wait_send()
        pair_out.wait_recv()

    sums = jnp.broadcast_to(jnp.sum(total[...], axis=1, keepdims=True), (8, nx))
    gamma, squares, fluid = sums[0:1], sums[1:2], sums[2:3]
    delta, eta, theta = sums[3:4], sums[4:5], sums[5:6]
    alpha = gamma / delta
    gamma_next = gamma - 2.0 * alpha * delta + alpha * alpha * eta
    beta = gamma_next / gamma
    mixed = delta - alpha * eta
    curve = (delta - 2.0 * alpha * eta + alpha * alpha * theta) + 2.0 * beta * mixed + beta * beta * delta
    alpha_next = gamma_next / curve
    norm = 1.0 / jnp.sqrt(squares / jnp.maximum(fluid, 1.0) + EPS)
    cf[1:2, :] = alpha + alpha_next * (1.0 + beta)
    cf[2:3, :] = alpha * alpha_next
    cf[3:4, :] = norm
    cf[4:5, :] = alpha * alpha_next * norm

    def out_rows(r):
        inner, rows = inner_rows(r), pl.ds(r, ROWS)
        a, b = cf[1:2, :], cf[2:3, :]
        for p in range(depth):
            zz, yy = z[p + 2, inner, :], y[p + 1, inner, :]
            w[p, rows, :] = a * zz - b * yy
            s[p, rows, :] = (
                jnp.maximum(code[p + 1, rows, :], 1.0) * (zz - a * yy) + b * ay[p, rows, :]) * cf[3:4, :]

    def all_rows(i, carry):
        out_rows(pl.multiple_of(i * ROWS, 8))
        return carry

    lax.fori_loop(0, nb, all_rows, 0)

    def last_rows(r):
        inner, rows = inner_rows(r), pl.ds(r, ROWS)
        s[top, rows, :] = s[top, rows, :] - jnp.where(
            inv[top + 1, rows, :] > 0.0, cf[4:5, :] * y[depth + 1, inner, :], 0.0)

    @pl.when(has_high)
    def _():
        def last_chunk(c, carry):
            y_down(c).wait_recv()
            over(c, last_rows)
            return carry
        lax.fori_loop(0, chunks, last_chunk, 0)

    @pl.when(odd)
    def _():
        pair_out.wait_send()

    def drain(c, carry):
        @pl.when(has_low)
        def _():
            when(c >= raw, lambda: lw_copy(c).wait_send())
            z_down(c).wait_send()
            y_down(c).wait_send()

        when(has_high, lambda: next_up(c).wait_send())
        return carry

    lax.fori_loop(0, chunks, drain, 0)


def solution(mesh):
    n = mesh.shape["gz"]

    def local(u_face, v_face, w_face, smoke, obstacles):
        depth, ny, nx = u_face.shape
        nw = obstacles.shape[1]
        chunks, raw = 16, 2
        crow = ny // chunks
        f32, i32 = jnp.float32, jnp.int32
        dma = pltpu.SemaphoreType.DMA
        any_spec = pl.BlockSpec(memory_space=pl.ANY)
        vmem_spec = pl.BlockSpec(memory_space=pltpu.VMEM)
        shape = pltpu.VMEM((depth, ny, nx), f32)
        return pl.pallas_call(
            functools.partial(kernel, n, chunks, raw),
            out_shape=(shape, shape),
            in_specs=[any_spec] * 5,
            out_specs=(vmem_spec, vmem_spec),
            scratch_shapes=[
                pltpu.VMEM((depth, ny, nx), f32),
                pltpu.VMEM((depth, ny + PAD, nx), f32),
                pltpu.VMEM((depth + 3, ny + 2 * PAD, nx), f32),
                pltpu.VMEM((depth + 2, ny + 2 * PAD, nx), f32),
                pltpu.VMEM((depth + 1, ny, nx), f32),
                pltpu.VMEM((depth + 1, ny, nx), f32),
                pltpu.VMEM((depth, ny, nx), f32),
                pltpu.VMEM((1, ny, nx), f32),
                pltpu.VMEM((1, ny, nx), f32),
                pltpu.VMEM((1, raw * crow, nx), f32),
                pltpu.VMEM((depth + 3, nw, nx), i32),
                pltpu.VMEM((depth + 1, 4, nw, nx), i32),
                pltpu.VMEM((6, 8, nx), f32),
                pltpu.VMEM((8, nx), f32),
                pltpu.VMEM((1, 128), f32),
                pltpu.VMEM((n, 1, 128), f32),
                pltpu.VMEM((8, 128), f32),
                pltpu.VMEM((8, 128), f32),
                pltpu.VMEM((n // 2, 8, 128), f32),
                pltpu.VMEM((8, 128), f32),
                dma((4 * depth + 3,)),
                dma((2,)), dma((2,)),
                dma((2 * raw,)), dma((2 * raw,)),
                dma((chunks,)), dma((chunks,)),
                dma((chunks,)), dma((chunks,)),
                dma((2 * chunks,)), dma((2 * chunks,)),
                dma((chunks,)), dma((chunks,)),
                dma((n,)), dma((n,)),
                dma((n // 2,)), dma((n // 2,)),
                dma((2,)), dma((2,)),
            ],
            compiler_params=pltpu.CompilerParams(
                collective_id=0, has_side_effects=True, vmem_limit_bytes=58_000_000),
            name="smoke_step",
        )(u_face, v_face, w_face, smoke, obstacles)

    placed = P("gz", None, None)
    return jax.shard_map(local, mesh=mesh, in_specs=(placed,) * 5, out_specs=(placed, placed), check_vma=False)
```

```python
import functools

import jax
import jax.numpy as jnp
from jax import lax
from jax.experimental import pallas as pl
from jax.experimental.pallas import tpu as pltpu
from jax.sharding import PartitionSpec as P

EPS = 1e-06
CFL = 0.5
BUOYANCY = 100.0

ROWS = 32
PAD = 8
SPAN = 8
LEAD = 4


def kernel(n, chunks, group, raw, u_hbm, v_hbm, w_hbm, s_hbm, ob_hbm, w, s,
           u, v, z, part_z, y, code, inv, ay, lw, lw_next, s_next, ob, cw, acc, cf, mx, mx_all, st, st_pair, st_all, total,
           in_sem, ob_send, ob_recv, raw_send, raw_recv, send, lw_recv, dn_recv, yd_recv, top_recv, next_recv,
           mx_send, mx_recv, st_send, st_recv, pair_send, pair_recv, gate):
    depth, ny, nx = w.shape
    top = depth - 1
    nb = ny // ROWS
    crow = ny // chunks
    grow = crow * group
    groups = chunks // group
    me = lax.axis_index("gz")
    has_low, has_high = me > 0, me < n - 1
    low, high = jnp.maximum(me - 1, 0), jnp.minimum(me + 1, n - 1)
    odd = lax.rem(me, 2) == 1
    even = jnp.logical_not(odd)
    partner = me + 1 - 2 * lax.rem(me, 2)
    place = lax.rem(me, SPAN)
    gated = jnp.logical_and(has_low, place == 0)
    gating = jnp.logical_and(place == 2, me + SPAN - 2 < n)

    def at(device):
        return dict(device_id=(device,), device_id_type=pl.DeviceIdType.MESH)

    ins = [(u_hbm, u), (v_hbm, v), (w_hbm, w), (s_hbm, s)]

    def load(k, p, first=0, rows=ny, sem=None):
        src, dst = ins[k]
        part = pl.ds(first, rows)
        return pltpu.make_async_copy(src.at[p, part], dst.at[p, part], in_sem.at[k * depth + p if sem is None else sem])

    raw_rows = raw * crow
    ob_in = pltpu.make_async_copy(ob_hbm, ob.at[pl.ds(2, depth)], in_sem.at[4 * depth])
    raw_in = [load(k, 0, 0, raw_rows, 4 * depth + k - 1) for k in (2, 3)]
    rest_in = {(k, p): load(k, p, raw_rows, ny - raw_rows) if k >= 2 and p == 0 else load(k, p)
               for k in range(4) for p in range(depth)}
    ob_in.start()
    for copy in raw_in:
        copy.start()
    for (k, _), copy in rest_in.items():
        if k < 3:
            copy.start()

    barrier = pltpu.get_barrier_semaphore()

    def greet(i, carry):
        pl.semaphore_signal(barrier, inc=1, **at(lax.rem(me + i, n)))
        return carry

    lax.fori_loop(1, n, greet, 0)

    zrow = jnp.zeros((PAD, nx), jnp.float32)
    for p in range(1, depth + 2):
        z[p, 0:PAD, :] = zrow
        z[p, ny + PAD : ny + 2 * PAD, :] = zrow
    for p in range(1, depth + 1):
        y[p, 0:PAD, :] = zrow
        y[p, ny + PAD : ny + 2 * PAD, :] = zrow
    for p in range(depth):
        v[p, ny : ny + PAD, :] = zrow
    acc[...] = jnp.zeros_like(acc)

    def zero_planes(ref, planes, offset):
        def body(i, carry):
            for p in planes:
                ref[p, pl.ds(pl.multiple_of(i * ROWS + offset, 8), ROWS), :] = jnp.zeros((ROWS, nx), jnp.float32)
            return carry
        lax.fori_loop(0, nb, body, 0)

    ob_in.wait()
    for copy in raw_in:
        copy.wait()
    pl.semaphore_wait(barrier, n - 1)

    ob_down = pltpu.make_async_remote_copy(
        ob.at[pl.ds(2, 1)], ob.at[pl.ds(depth + 2, 1)], ob_send.at[0], ob_recv.at[0], **at(low))
    ob_up = pltpu.make_async_remote_copy(
        ob.at[pl.ds(depth, 2)], ob.at[pl.ds(0, 2)], ob_send.at[1], ob_recv.at[1], **at(high))

    raw_part = pl.ds(0, raw_rows)
    raw_copies = [
        pltpu.make_async_remote_copy(
            src.at[0, raw_part], dst.at[0, raw_part], raw_send.at[j], raw_recv.at[j], **at(low))
        for j, (src, dst) in enumerate([(w, lw_next), (s, s_next)])
    ]

    @pl.when(has_low)
    def _():
        ob_down.start()

    @pl.when(has_high)
    def _():
        ob_up.start()

    @pl.when(jnp.logical_not(has_low))
    def _():
        ob[0:2] = jnp.zeros((2,) + ob.shape[1:], jnp.int32)
        zero_planes(z, (0, 1), PAD)

    @pl.when(jnp.logical_not(has_high))
    def _():
        ob[depth + 2 : depth + 3] = jnp.zeros((1,) + ob.shape[1:], jnp.int32)
        zero_planes(z, (depth + 2,), PAD)
        zero_planes(lw_next, (0,), 0)

    peak = jnp.zeros((8, nx), jnp.float32)
    for k in range(3):
        ref = ins[k][1]
        for p in range(depth):
            rest_in[k, p].wait()
            if k == 1:
                rest_in[3, p].start()

            def body(i, m, ref=ref, p=p):
                a = jnp.abs(ref[p, pl.ds(pl.multiple_of(i * ROWS, 8), ROWS), :])
                return jnp.maximum(m, jnp.max(a.reshape(ROWS // 8, 8, nx), axis=0))

            peak = lax.fori_loop(0, nb, body, peak)
    m = jnp.max(peak, axis=0, keepdims=True)
    part = m[:, 0:128]
    for c in range(128, nx, 128):
        part = jnp.maximum(part, m[:, c : c + 128])
    mx[...] = part

    def spread(src, dst, send, recv, step, count):
        def start(i, carry):
            pltpu.make_async_remote_copy(
                src, dst.at[i], send, recv, **at(lax.rem(me + step * i, n))).start()
            return carry

        everything = dst.at[pl.ds(1, count - 1)]
        whole = pltpu.make_async_remote_copy(everything, everything, send, recv, **at(lax.rem(me + step, n)))
        return (lambda: lax.fori_loop(1, count, start, 0)), whole

    mx_start, mx_whole = spread(mx, mx_all, mx_send, mx_recv, 1, n)
    mx_start()

    @pl.when(has_low)
    def _():
        for copy in raw_copies:
            copy.start()

    @pl.when(has_low)
    def _():
        ob_down.wait_send()
        ob_up.wait_recv()

    @pl.when(has_high)
    def _():
        ob_up.wait_send()
        ob_down.wait_recv()

    row_id = lax.broadcasted_iota(jnp.int32, (nb, nx), 0)
    col_id = lax.broadcasted_iota(jnp.int32, (nb, nx), 1)
    srl = lax.shift_right_logical
    c1, c31 = jnp.int32(1), jnp.int32(31)
    full1, full31 = jnp.full((nb, nx), c1), jnp.full((nb, nx), c31)
    for p in range(depth + 1):
        mid = ob[p + 1]
        after = jnp.where(row_id == nb - 1, 0, pltpu.roll(mid, nb - 1, 0))
        before = jnp.where(row_id == 0, 0, pltpu.roll(mid, 1, 0))
        a = srl(mid, full1) | (after << full31)
        b = (mid << full1) | srl(before, full31)
        c = jnp.where(col_id == nx - 1, 0, pltpu.roll(mid, nx - 1, 1))
        d = jnp.where(col_id == 0, 0, pltpu.roll(mid, 1, 1))
        e, f = ob[p], ob[p + 2]
        s1, k1 = a ^ b ^ c, (a & b) | (c & (a | b))
        s2, k2 = d ^ e ^ f, (d & e) | (f & (d | e))
        k3 = s1 & s2
        cw[p, 0] = s1 ^ s2
        cw[p, 1] = k1 ^ k2 ^ k3
        cw[p, 2] = (k1 & k2) | (k3 & (k1 | k2))
        cw[p, 3] = mid
    @pl.when(jnp.logical_not(has_low))
    def _():
        cw[0, 3] = jnp.full((nb, nx), -1, jnp.int32)

    half = 16
    places = lax.broadcasted_iota(jnp.int32, (half, nx), 0)

    def code_rows(b):
        for p in range(depth + 1):
            for k0 in range(0, ROWS, half):
                bits = [
                    srl(jnp.broadcast_to(cw[p, j, pl.ds(b, 1), :], (half, nx)), places + k0) & 1
                    for j in range(4)
                ]
                k = (6 - (bits[0] + (bits[1] << 1) + (bits[2] << 2))).astype(jnp.float32)
                rows = pl.ds(pl.multiple_of(b * ROWS + k0, 8), half)
                code[p, rows, :] = k
                inv[p, rows, :] = jnp.where(bits[3] == 1, 0.0, 1.0 / jnp.maximum(k, 1.0))

    for p in range(depth):
        rest_in[3, p].wait()
    mx_whole.wait_recv()
    mx_all[0] = mx[...]
    fastest = jnp.max(jnp.max(mx_all[...], axis=0), axis=1, keepdims=True)
    cf[0:1, :] = (CFL / (jnp.broadcast_to(fastest, (1, nx)) + EPS)) * BUOYANCY

    lane = lax.broadcasted_iota(jnp.int32, (ROWS, nx), 1)

    def lifted(p, r):
        rows = pl.ds(r, ROWS)
        return w[p, rows, :] + cf[0:1, :] * s[p, rows, :]

    def over(c, fn, rows=crow):
        def inner(i, k):
            fn(pl.multiple_of(c * rows + i * ROWS, 8))
            return k
        lax.fori_loop(0, rows // ROWS, inner, 0)

    def staged(first, second, count=chunks):
        def body(c, carry):
            @pl.when(c < count)
            def _():
                first(c)

            @pl.when(c > 0)
            def _():
                second(c - 1)
            return carry
        lax.fori_loop(0, count + 1, body, 0)

    def when(cond, fn):
        @pl.when(cond)
        def _():
            fn()

    class Flow:
        def __init__(self, src, dst, send, recv, device, per, src_pad=PAD, dst_pad=PAD, first=0):
            def copy(start, rows, index):
                def part(pad):
                    return pl.ds(pl.multiple_of(start + pad, 8), rows)
                return pltpu.make_async_remote_copy(
                    src[0].at[src[1], part(src_pad)], dst[0].at[dst[1], part(dst_pad)], send, recv.at[index], **at(device))

            self.start = lambda c: copy(c * crow, crow, c // per).start()
            self.wait_recv = lambda i: copy(i * crow * per, crow * per, i).wait_recv()
            self.wait_send = lambda: copy(first, ny - first, 0).wait_send()

    lw_down = Flow((lw, 0), (lw_next, 0), send.at[0], lw_recv, low, group, 0, 0, raw_rows)
    z_down = Flow((z, 2), (z, depth + 2), send.at[1], dn_recv, low, group)
    y_down = Flow((y, 1), (y, depth + 1), send.at[2], yd_recv, low, group)
    top_up = Flow((part_z, 0), (z, 1), send.at[3], top_recv, high, group, 0)
    next_up = Flow((z, top + 1), (z, 0), send.at[4], next_recv, high, 1)

    def flat(p, r):
        a = u[p, pl.ds(r, ROWS), :]
        b = v[p, pl.ds(r, ROWS + PAD), :]
        return jnp.where(lane == nx - 1, 0.0, pltpu.roll(a, nx - 1, 1)) - a + (b[1 : ROWS + 1] - b[:ROWS])

    def inner_rows(r):
        return pl.ds(pl.multiple_of(r + PAD, 8), ROWS)

    def first_rows(r):
        code_rows(r // ROWS)
        rows = pl.ds(r, ROWS)
        lw[0, rows, :] = lifted(0, r)
        part_z[0, rows, :] = inv[top + 1, rows, :] * (flat(top, r) - lifted(top, r))

    def first_sends(c):
        when(jnp.logical_and(has_low, c >= raw), lambda: lw_down.start(c))
        when(has_high, lambda: top_up.start(c))

    staged(lambda c: over(c, first_rows), first_sends)

    def z_rows(p, r):
        rows = pl.ds(r, ROWS)
        own = lw[0, rows, :] if p == 0 else lifted(p, r)
        z[p + 2, inner_rows(r), :] = inv[p + 1, rows, :] * (flat(p, r) + (lifted(p + 1, r) - own))

    for p in range(top):
        def z_sends(c, p=p):
            if p == 0:
                when(has_low, lambda: z_down.start(c))
            if p == top - 1:
                when(has_high, lambda: next_up.start(c))
        staged(lambda c, p=p: over(c, functools.partial(z_rows, p)), z_sends)

    @pl.when(has_high)
    def _():
        for copy in raw_copies:
            copy.wait_recv()

        def lift(i, carry):
            rows = pl.ds(pl.multiple_of(i * ROWS, 8), ROWS)
            lw_next[0, rows, :] = lw_next[0, rows, :] + cf[0:1, :] * s_next[0, rows, :]
            return carry

        lax.fori_loop(0, raw_rows // ROWS, lift, 0)

    def around(ref, slot, r):
        x = ref[slot, pl.ds(r, ROWS + 2 * PAD), :]
        mid = x[PAD : PAD + ROWS]
        beside = x[PAD + 1 : PAD + 1 + ROWS] + x[PAD - 1 : PAD - 1 + ROWS]
        beside = beside + jnp.where(lane == nx - 1, 0.0, pltpu.roll(mid, nx - 1, 1))
        beside = beside + jnp.where(lane == 0, 0.0, pltpu.roll(mid, 1, 1))
        return mid, beside

    def add(j, x):
        acc[j] += jnp.sum(x.reshape(ROWS // 8, 8, nx), axis=0)

    def y_rows(p, r):
        inner, rows = inner_rows(r), pl.ds(r, ROWS)
        k, scale = code[p + 1, rows, :], inv[p + 1, rows, :]
        mid, beside = around(z, p + 2, r)
        q = k * mid - (beside + z[p + 1, inner, :] + z[p + 3, inner, :])
        out = q * scale
        y[p + 1, inner, :] = out
        if p >= 0:
            d = jnp.maximum(k, 1.0) * mid
            add(0, d * mid)
            add(1, d * d)
            add(2, jnp.where(scale > 0.0, 1.0, 0.0))
            add(3, mid * q)
            add(4, q * out)

    def complete_rows(r):
        inner, rows = inner_rows(r), pl.ds(r, ROWS)
        z[top + 2, inner, :] = part_z[0, rows, :] + inv[top + 1, rows, :] * lw_next[0, rows, :]
        z[1, inner, :] = z[1, inner, :] + inv[0, rows, :] * lw[0, rows, :]

    def low_rows(r):
        complete_rows(r)
        for p in range(top):
            y_rows(p, r)

    def low_chunk(c):
        when(jnp.logical_and(has_high, c >= raw // group), lambda: lw_down.wait_recv(c))
        when(has_low, lambda: top_up.wait_recv(c))
        over(c, low_rows, grow)

    def start_y(c):
        for i in range(group):
            y_down.start(c * group + i)

    staged(low_chunk, lambda c: when(jnp.logical_and(has_low, jnp.logical_not(gated)), lambda: start_y(c)), groups)

    def a_rows(p, r):
        inner, rows = inner_rows(r), pl.ds(r, ROWS)
        mid, beside = around(y, p + 1, r)
        below = y[p, inner, :]
        beside = beside + below
        if p < top:
            beside = beside + y[p + 2, inner, :]
        q = code[p + 1, rows, :] * mid - beside
        ay[p, rows, :] = jnp.where(inv[p + 1, rows, :] > 0.0, q, 0.0)
        add(5, mid * (q - below) if p == 0 else mid * q)

    def high_rows(r):
        y_rows(top, r)
        y_rows(-1, r)

    def high_chunk(c):
        when(has_high, lambda: z_down.wait_recv(c))
        for i in range(group):
            chunk = c * group + i
            when(has_low, lambda: next_up.wait_recv(chunk))
            when(jnp.logical_and(gating, chunk == chunks - LEAD), lambda: pl.semaphore_signal(
                gate, inc=1, **at(jnp.minimum(me + SPAN - 2, n - 1))))
        over(c, high_rows, grow)

    def image_rows(r):
        for p in range(depth):
            a_rows(p, r)

    staged(high_chunk, lambda c: over(c, image_rows, grow), groups)

    @pl.when(gated)
    def _():
        pl.semaphore_wait(gate, 1)

        def start(c, carry):
            start_y(c)
            return carry

        lax.fori_loop(0, groups, start, 0)

    for j in range(6):
        t = jnp.sum(acc[j], axis=0, keepdims=True)
        part = t[:, 0:128]
        for c in range(128, nx, 128):
            part = part + t[:, c : c + 128]
        st[j : j + 1, :] = part
    st[6:8, :] = jnp.zeros((2, 128), jnp.float32)

    pair_in = pltpu.make_async_remote_copy(st, st_pair, pair_send.at[0], pair_recv.at[0], **at(partner))
    pair_out = pltpu.make_async_remote_copy(total, total, pair_send.at[1], pair_recv.at[1], **at(partner))
    st_start, st_whole = spread(st_pair, st_all, st_send, st_recv, 2, n // 2)

    @pl.when(even)
    def _():
        pair_in.start()

    @pl.when(odd)
    def _():
        pair_in.wait_recv()
        st_pair[...] = st_pair[...] + st[...]
        st_start()
        st_whole.wait_recv()
        st_all[0] = st_pair[...]
        total[...] = jnp.sum(st_all[...], axis=0)
        pair_out.start()

    @pl.when(has_low)
    def _():
        for copy in raw_copies:
            copy.wait_send()

    @pl.when(even)
    def _():
        pair_in.wait_send()
        pair_out.wait_recv()

    sums = jnp.broadcast_to(jnp.sum(total[...], axis=1, keepdims=True), (8, nx))
    gamma, squares, fluid = sums[0:1], sums[1:2], sums[2:3]
    delta, eta, theta = sums[3:4], sums[4:5], sums[5:6]
    alpha = gamma / delta
    gamma_next = gamma - 2.0 * alpha * delta + alpha * alpha * eta
    beta = gamma_next / gamma
    mixed = delta - alpha * eta
    curve = (delta - 2.0 * alpha * eta + alpha * alpha * theta) + 2.0 * beta * mixed + beta * beta * delta
    alpha_next = gamma_next / curve
    norm = 1.0 / jnp.sqrt(squares / jnp.maximum(fluid, 1.0) + EPS)
    cf[1:2, :] = alpha + alpha_next * (1.0 + beta)
    cf[2:3, :] = alpha * alpha_next
    cf[3:4, :] = norm
    cf[4:5, :] = alpha * alpha_next * norm

    def out_rows(r):
        inner, rows = inner_rows(r), pl.ds(r, ROWS)
        a, b = cf[1:2, :], cf[2:3, :]
        for p in range(depth):
            zz, yy = z[p + 2, inner, :], y[p + 1, inner, :]
            w[p, rows, :] = a * zz - b * yy
            s[p, rows, :] = (
                jnp.maximum(code[p + 1, rows, :], 1.0) * (zz - a * yy) + b * ay[p, rows, :]) * cf[3:4, :]

    def all_rows(i, carry):
        out_rows(pl.multiple_of(i * ROWS, 8))
        return carry

    lax.fori_loop(0, nb, all_rows, 0)

    def last_rows(r):
        inner, rows = inner_rows(r), pl.ds(r, ROWS)
        s[top, rows, :] = s[top, rows, :] - jnp.where(
            inv[top + 1, rows, :] > 0.0, cf[4:5, :] * y[depth + 1, inner, :], 0.0)

    @pl.when(has_high)
    def _():
        def last_chunk(c, carry):
            y_down.wait_recv(c)
            over(c, last_rows, grow)
            return carry
        lax.fori_loop(0, groups, last_chunk, 0)

    @pl.when(odd)
    def _():
        st_whole.wait_send()
        pair_out.wait_send()

    @pl.when(has_low)
    def _():
        for flow in (lw_down, z_down, y_down):
            flow.wait_send()

    @pl.when(has_high)
    def _():
        for flow in (top_up, next_up):
            flow.wait_send()

    mx_whole.wait_send()


def store(w, s, w_hbm, s_hbm, sem):
    copies = [
        pltpu.make_async_copy(src.at[p], dst.at[p], sem.at[j, p])
        for j, (src, dst) in enumerate([(w, w_hbm), (s, s_hbm)]) for p in range(w.shape[0])
    ]
    for copy in copies:
        copy.start()
    for copy in copies:
        copy.wait()


def solution(mesh):
    n = mesh.shape["gz"]

    def local(u_face, v_face, w_face, smoke, obstacles):
        depth, ny, nx = u_face.shape
        nw = obstacles.shape[1]
        chunks, group, raw = 16, 2, 2
        crow = ny // chunks
        f32, i32 = jnp.float32, jnp.int32
        dma = pltpu.SemaphoreType.DMA
        any_spec = pl.BlockSpec(memory_space=pl.ANY)
        vmem_spec = pl.BlockSpec(memory_space=pltpu.VMEM)
        shape = pltpu.VMEM((depth, ny, nx), f32)
        results = pl.pallas_call(
            functools.partial(kernel, n, chunks, group, raw),
            out_shape=(shape, shape),
            in_specs=[any_spec] * 5,
            out_specs=(vmem_spec, vmem_spec),
            scratch_shapes=[
                pltpu.VMEM((depth, ny, nx), f32),
                pltpu.VMEM((depth, ny + PAD, nx), f32),
                pltpu.VMEM((depth + 3, ny + 2 * PAD, nx), f32),
                pltpu.VMEM((1, ny, nx), f32),
                pltpu.VMEM((depth + 2, ny + 2 * PAD, nx), f32),
                pltpu.VMEM((depth + 1, ny, nx), f32),
                pltpu.VMEM((depth + 1, ny, nx), f32),
                pltpu.VMEM((depth, ny, nx), f32),
                pltpu.VMEM((1, ny, nx), f32),
                pltpu.VMEM((1, ny, nx), f32),
                pltpu.VMEM((1, raw * crow, nx), f32),
                pltpu.VMEM((depth + 3, nw, nx), i32),
                pltpu.VMEM((depth + 1, 4, nw, nx), i32),
                pltpu.VMEM((6, 8, nx), f32),
                pltpu.VMEM((8, nx), f32),
                pltpu.VMEM((1, 128), f32),
                pltpu.VMEM((n, 1, 128), f32),
                pltpu.VMEM((8, 128), f32),
                pltpu.VMEM((8, 128), f32),
                pltpu.VMEM((n // 2, 8, 128), f32),
                pltpu.VMEM((8, 128), f32),
                dma((4 * depth + 3,)),
                dma((2,)), dma((2,)),
                dma((2,)), dma((2,)),
                dma((5,)),
                dma((chunks // group,)), dma((chunks // group,)), dma((chunks // group,)), dma((chunks // group,)),
                dma((chunks,)),
                dma, dma, dma, dma,
                dma((2,)), dma((2,)),
                pltpu.SemaphoreType.REGULAR,
            ],
            compiler_params=pltpu.CompilerParams(
                collective_id=0, has_side_effects=True, vmem_limit_bytes=58_000_000),
            name="smoke_step",
        )(u_face, v_face, w_face, smoke, obstacles)
        out = jax.ShapeDtypeStruct((depth, ny, nx), f32)
        return pl.pallas_call(
            store,
            out_shape=(out, out),
            in_specs=[vmem_spec] * 2,
            out_specs=(any_spec, any_spec),
            scratch_shapes=[dma((2, depth))],
            compiler_params=pltpu.CompilerParams(vmem_limit_bytes=1_000_000),
            name="store",
        )(*results)

    placed = P("gz", None, None)
    return jax.shard_map(local, mesh=mesh, in_specs=(placed,) * 5, out_specs=(placed, placed), check_vma=False)
```

```python
import functools

import jax
import jax.numpy as jnp
from jax import lax
from jax.experimental import pallas as pl
from jax.experimental.pallas import tpu as pltpu
from jax.sharding import PartitionSpec as P

EPS = 1e-06
CFL = 0.5
BUOYANCY = 100.0

ROWS = 32
PAD = 8
SPAN = 8
LEAD = 4
OPEN = 5


def kernel(n, chunks, group, raw, u_hbm, v_hbm, w_hbm, s_hbm, ob_hbm, w, s,
           u, v, z, part_z, y, code, inv, ay, lw, lw_next, s_next, relay, ob, cw, acc, cf, mx, mx_all, st, st_pair, st_all, total,
           in_sem, ob_send, ob_recv, raw_send, raw_recv, send, lw_recv, dn_recv, yd_recv, top_recv, next_recv, relay_recv, relay_send,
           mx_send, mx_recv, st_send, st_recv, pair_send, pair_recv, gate):
    depth, ny, nx = w.shape
    top = depth - 1
    nb = ny // ROWS
    crow = ny // chunks
    grow = crow * group
    groups = chunks // group
    me = lax.axis_index("gz")
    has_low, has_high = me > 0, me < n - 1
    low, high = jnp.maximum(me - 1, 0), jnp.minimum(me + 1, n - 1)
    odd = lax.rem(me, 2) == 1
    even = jnp.logical_not(odd)
    partner = me + 1 - 2 * lax.rem(me, 2)
    place = lax.rem(me, SPAN)
    gated = jnp.logical_and(has_low, place == 0)
    gating = jnp.logical_and(place == 2, me + SPAN - 2 < n)

    span, spans = me // SPAN, n // SPAN
    plane_units = groups
    head = plane_units // 2
    few = plane_units // 4
    every = head + plane_units

    def piece(count):
        return head - jnp.maximum(count - plane_units, 0), head + jnp.minimum(count, plane_units)

    def select(cases):
        first, last = 0, 0
        for cond, (lo, hi) in cases:
            first, last = jnp.where(cond, lo, first), jnp.where(cond, hi, last)
        return first, last

    def cross_up(lower):
        return piece(jnp.minimum(head * (spans - 1 - lower), every))

    def cross_down(upper):
        return piece(jnp.minimum(head * upper, every))

    side = (every - few, every)
    whole_spans = n % SPAN == 0
    crossing = jnp.logical_and(whole_spans, span + 1 < spans)
    crossed = jnp.logical_and(whole_spans, span > 0)
    up_first, up_last = select([(jnp.logical_and(whole_spans, place == 3), side), (jnp.logical_and(crossing, place == 7), cross_up(span))])
    dn_first, dn_last = select([(jnp.logical_and(whole_spans, place == 4), side), (jnp.logical_and(crossed, place == 0), cross_down(span))])
    up_via = jnp.clip(jnp.where(place == 3, me + 4, me - 2), 0, n - 1)
    dn_via = jnp.clip(jnp.where(place == 4, me - 4, me + 3), 0, n - 1)
    relays_up = jnp.logical_and(whole_spans, jnp.logical_or(place == 7, jnp.logical_and(place == 5, crossing)))
    relays_down = jnp.logical_and(whole_spans, jnp.logical_or(place == 0, jnp.logical_and(place == 3, crossed)))
    near = jnp.logical_or(place == 7, place == 0)
    rl_first, rl_last = select([
        (jnp.logical_and(whole_spans, near), side),
        (jnp.logical_and(crossing, place == 5), cross_up(span)),
        (jnp.logical_and(crossed, place == 3), cross_down(span)),
    ])
    rl_target = jnp.clip(
        jnp.where(place == 7, me - 3, jnp.where(place == 5, me + 3, jnp.where(place == 0, me + 3, me - 4))), 0, n - 1)

    def at(device):
        return dict(device_id=(device,), device_id_type=pl.DeviceIdType.MESH)

    ins = [(u_hbm, u), (v_hbm, v), (w_hbm, w), (s_hbm, s)]

    def load(k, p, first=0, rows=ny, sem=None):
        src, dst = ins[k]
        part = pl.ds(first, rows)
        return pltpu.make_async_copy(src.at[p, part], dst.at[p, part], in_sem.at[k * depth + p if sem is None else sem])

    raw_rows = raw * crow
    ob_in = pltpu.make_async_copy(ob_hbm, ob.at[pl.ds(2, depth)], in_sem.at[4 * depth])
    raw_in = [load(k, 0, 0, raw_rows, 4 * depth + k - 1) for k in (2, 3)]
    rest_in = {(k, p): load(k, p, raw_rows, ny - raw_rows) if k >= 2 and p == 0 else load(k, p)
               for k in range(4) for p in range(depth)}
    ob_in.start()
    for copy in raw_in:
        copy.start()
    for (k, _), copy in rest_in.items():
        if k < 3:
            copy.start()

    barrier = pltpu.get_barrier_semaphore()

    def greet(i, carry):
        pl.semaphore_signal(barrier, inc=1, **at(lax.rem(me + i, n)))
        return carry

    lax.fori_loop(1, n, greet, 0)

    zrow = jnp.zeros((PAD, nx), jnp.float32)
    for p in range(1, depth + 2):
        z[p, 0:PAD, :] = zrow
        z[p, ny + PAD : ny + 2 * PAD, :] = zrow
    for p in range(1, depth + 1):
        y[p, 0:PAD, :] = zrow
        y[p, ny + PAD : ny + 2 * PAD, :] = zrow
    for p in range(depth):
        v[p, ny : ny + PAD, :] = zrow
    acc[...] = jnp.zeros_like(acc)

    def zero_planes(ref, planes, offset):
        def body(i, carry):
            for p in planes:
                ref[p, pl.ds(pl.multiple_of(i * ROWS + offset, 8), ROWS), :] = jnp.zeros((ROWS, nx), jnp.float32)
            return carry
        lax.fori_loop(0, nb, body, 0)

    ob_in.wait()
    for copy in raw_in:
        copy.wait()
    pl.semaphore_wait(barrier, n - 1)

    ob_down = pltpu.make_async_remote_copy(
        ob.at[pl.ds(2, 1)], ob.at[pl.ds(depth + 2, 1)], ob_send.at[0], ob_recv.at[0], **at(low))
    ob_up = pltpu.make_async_remote_copy(
        ob.at[pl.ds(depth, 2)], ob.at[pl.ds(0, 2)], ob_send.at[1], ob_recv.at[1], **at(high))

    raw_part = pl.ds(0, raw_rows)
    raw_copies = [
        pltpu.make_async_remote_copy(
            src.at[0, raw_part], dst.at[0, raw_part], raw_send.at[j], raw_recv.at[j], **at(low))
        for j, (src, dst) in enumerate([(w, lw_next), (s, s_next)])
    ]

    @pl.when(has_low)
    def _():
        ob_down.start()

    @pl.when(has_high)
    def _():
        ob_up.start()

    @pl.when(jnp.logical_not(has_low))
    def _():
        ob[0:2] = jnp.zeros((2,) + ob.shape[1:], jnp.int32)
        zero_planes(z, (0, 1), PAD)

    @pl.when(jnp.logical_not(has_high))
    def _():
        ob[depth + 2 : depth + 3] = jnp.zeros((1,) + ob.shape[1:], jnp.int32)
        zero_planes(z, (depth + 2,), PAD)
        zero_planes(lw_next, (0,), 0)

    peak = jnp.zeros((8, nx), jnp.float32)
    for k in range(3):
        ref = ins[k][1]
        for p in range(depth):
            rest_in[k, p].wait()
            if k == 1:
                rest_in[3, p].start()

            def body(i, m, ref=ref, p=p):
                a = jnp.abs(ref[p, pl.ds(pl.multiple_of(i * ROWS, 8), ROWS), :])
                return jnp.maximum(m, jnp.max(a.reshape(ROWS // 8, 8, nx), axis=0))

            peak = lax.fori_loop(0, nb, body, peak)
    m = jnp.max(peak, axis=0, keepdims=True)
    part = m[:, 0:128]
    for c in range(128, nx, 128):
        part = jnp.maximum(part, m[:, c : c + 128])
    mx[...] = part

    def spread(src, dst, send, recv, step, count):
        def start(i, carry):
            pltpu.make_async_remote_copy(
                src, dst.at[i], send, recv, **at(lax.rem(me + step * i, n))).start()
            return carry

        everything = dst.at[pl.ds(1, count - 1)]
        whole = pltpu.make_async_remote_copy(everything, everything, send, recv, **at(lax.rem(me + step, n)))
        return (lambda: lax.fori_loop(1, count, start, 0)), whole

    mx_start, mx_whole = spread(mx, mx_all, mx_send, mx_recv, 1, n)
    mx_start()

    @pl.when(has_low)
    def _():
        for copy in raw_copies:
            copy.start()

    @pl.when(has_low)
    def _():
        ob_down.wait_send()
        ob_up.wait_recv()

    @pl.when(has_high)
    def _():
        ob_up.wait_send()
        ob_down.wait_recv()

    row_id = lax.broadcasted_iota(jnp.int32, (nb, nx), 0)
    col_id = lax.broadcasted_iota(jnp.int32, (nb, nx), 1)
    srl = lax.shift_right_logical
    c1, c31 = jnp.int32(1), jnp.int32(31)
    full1, full31 = jnp.full((nb, nx), c1), jnp.full((nb, nx), c31)
    for p in range(depth + 1):
        mid = ob[p + 1]
        after = jnp.where(row_id == nb - 1, 0, pltpu.roll(mid, nb - 1, 0))
        before = jnp.where(row_id == 0, 0, pltpu.roll(mid, 1, 0))
        a = srl(mid, full1) | (after << full31)
        b = (mid << full1) | srl(before, full31)
        c = jnp.where(col_id == nx - 1, 0, pltpu.roll(mid, nx - 1, 1))
        d = jnp.where(col_id == 0, 0, pltpu.roll(mid, 1, 1))
        e, f = ob[p], ob[p + 2]
        s1, k1 = a ^ b ^ c, (a & b) | (c & (a | b))
        s2, k2 = d ^ e ^ f, (d & e) | (f & (d | e))
        k3 = s1 & s2
        cw[p, 0] = s1 ^ s2
        cw[p, 1] = k1 ^ k2 ^ k3
        cw[p, 2] = (k1 & k2) | (k3 & (k1 | k2))
        cw[p, 3] = mid
    @pl.when(jnp.logical_not(has_low))
    def _():
        cw[0, 3] = jnp.full((nb, nx), -1, jnp.int32)

    half = 16
    places = lax.broadcasted_iota(jnp.int32, (half, nx), 0)

    def code_rows(b):
        for p in range(depth + 1):
            for k0 in range(0, ROWS, half):
                bits = [
                    srl(jnp.broadcast_to(cw[p, j, pl.ds(b, 1), :], (half, nx)), places + k0) & 1
                    for j in range(4)
                ]
                k = (6 - (bits[0] + (bits[1] << 1) + (bits[2] << 2))).astype(jnp.float32)
                rows = pl.ds(pl.multiple_of(b * ROWS + k0, 8), half)
                code[p, rows, :] = k
                inv[p, rows, :] = jnp.where(bits[3] == 1, 0.0, 1.0 / jnp.maximum(k, 1.0))

    for p in range(depth):
        rest_in[3, p].wait()
    mx_whole.wait_recv()
    mx_all[0] = mx[...]
    fastest = jnp.max(jnp.max(mx_all[...], axis=0), axis=1, keepdims=True)
    cf[0:1, :] = (CFL / (jnp.broadcast_to(fastest, (1, nx)) + EPS)) * BUOYANCY

    lane = lax.broadcasted_iota(jnp.int32, (ROWS, nx), 1)

    def lifted(p, r):
        rows = pl.ds(r, ROWS)
        return w[p, rows, :] + cf[0:1, :] * s[p, rows, :]

    def over(c, fn, rows=crow):
        def inner(i, k):
            fn(pl.multiple_of(c * rows + i * ROWS, 8))
            return k
        lax.fori_loop(0, rows // ROWS, inner, 0)

    def staged(first, second, count=chunks):
        def body(c, carry):
            @pl.when(c < count)
            def _():
                first(c)

            @pl.when(c > 0)
            def _():
                second(c - 1)
            return carry
        lax.fori_loop(0, count + 1, body, 0)

    def when(cond, fn):
        @pl.when(cond)
        def _():
            fn()

    class Flow:
        def __init__(self, src, dst, send, recv, device, per, src_pad=PAD, dst_pad=PAD, first=0):
            def copy(start, rows, index):
                def part(pad):
                    return pl.ds(pl.multiple_of(start + pad, 8), rows)
                return pltpu.make_async_remote_copy(
                    src[0].at[src[1], part(src_pad)], dst[0].at[dst[1], part(dst_pad)], send, recv.at[index], **at(device))

            self.start = lambda c: copy(c * crow, crow, c // per).start()
            self.wait_recv = lambda i: copy(i * crow * per, crow * per, i).wait_recv()
            self.wait_send = lambda: copy(first, ny - first, 0).wait_send()

            def aside(c, unit):
                return pl.ds(pl.multiple_of(unit * grow + lax.rem(c, group) * crow, 8), crow)

            def detour(c, unit, via):
                rows = pl.ds(pl.multiple_of(c * crow + src_pad, 8), crow)
                pltpu.make_async_remote_copy(
                    src[0].at[src[1], rows], relay.at[0, aside(c, unit)], send, relay_recv.at[unit], **at(via)).start()

            def forward(c, unit):
                rows = pl.ds(pl.multiple_of(c * crow + dst_pad, 8), crow)
                pltpu.make_async_remote_copy(
                    relay.at[0, aside(c, unit)], dst[0].at[dst[1], rows], relay_send.at[unit], recv.at[c // per],
                    **at(rl_target)).start()

            self.detour, self.forward = detour, forward

    lw_down = Flow((lw, 0), (lw_next, 0), send.at[0], lw_recv, low, group, 0, 0, raw_rows)
    z_down = Flow((z, 2), (z, depth + 2), send.at[1], dn_recv, low, group)
    y_down = Flow((y, 1), (y, depth + 1), send.at[2], yd_recv, low, group)
    top_up = Flow((part_z, 0), (z, 1), send.at[3], top_recv, high, group, 0)
    next_up = Flow((z, top + 1), (z, 0), send.at[4], next_recv, high, 1)

    def send_chunk(flow, second, c, first, last, via):
        unit = c // group + (head if second else head - plane_units)
        aside = jnp.logical_and(unit >= first, unit < last)
        when(aside, lambda: flow.detour(c, jnp.maximum(unit, 0), via))
        when(jnp.logical_not(aside), lambda: flow.start(c))

    def forward_unit(cond, unit, second):
        def run(flow):
            pltpu.make_async_remote_copy(
                relay.at[0, pl.ds(0, grow)], relay.at[0, pl.ds(0, grow)], relay_send.at[unit], relay_recv.at[unit],
                **at(rl_target)).wait_recv()
            for i in range(group):
                flow.forward((unit + (-head if second else plane_units - head)) * group + i, unit)

        inside = jnp.logical_and(cond, jnp.logical_and(unit >= rl_first, unit < rl_last))
        when(jnp.logical_and(inside, relays_up), lambda: run(next_up if second else top_up))
        when(jnp.logical_and(inside, relays_down), lambda: run(z_down if second else lw_down))

    def flat(p, r):
        a = u[p, pl.ds(r, ROWS), :]
        b = v[p, pl.ds(r, ROWS + PAD), :]
        return jnp.where(lane == nx - 1, 0.0, pltpu.roll(a, nx - 1, 1)) - a + (b[1 : ROWS + 1] - b[:ROWS])

    def inner_rows(r):
        return pl.ds(pl.multiple_of(r + PAD, 8), ROWS)

    def first_rows(r):
        code_rows(r // ROWS)
        rows = pl.ds(r, ROWS)
        lw[0, rows, :] = lifted(0, r)
        part_z[0, rows, :] = inv[top + 1, rows, :] * (flat(top, r) - lifted(top, r))

    def first_sends(c):
        when(jnp.logical_and(has_low, c >= raw), lambda: send_chunk(lw_down, False, c, dn_first, dn_last, dn_via))
        when(has_high, lambda: send_chunk(top_up, False, c, up_first, up_last, up_via))

    staged(lambda c: over(c, first_rows), first_sends)

    def z_rows(p, r):
        rows = pl.ds(r, ROWS)
        own = lw[0, rows, :] if p == 0 else lifted(p, r)
        z[p + 2, inner_rows(r), :] = inv[p + 1, rows, :] * (flat(p, r) + (lifted(p + 1, r) - own))

    for p in range(top):
        def z_sends(c, p=p):
            if p == 0:
                when(has_low, lambda: send_chunk(z_down, True, c, dn_first, dn_last, dn_via))
            if p == top - 1:
                when(has_high, lambda: send_chunk(next_up, True, c, up_first, up_last, up_via))
        staged(lambda c, p=p: over(c, functools.partial(z_rows, p)), z_sends)

    @pl.when(has_high)
    def _():
        for copy in raw_copies:
            copy.wait_recv()

        def lift(i, carry):
            rows = pl.ds(pl.multiple_of(i * ROWS, 8), ROWS)
            lw_next[0, rows, :] = lw_next[0, rows, :] + cf[0:1, :] * s_next[0, rows, :]
            return carry

        lax.fori_loop(0, raw_rows // ROWS, lift, 0)

    def around(ref, slot, r):
        x = ref[slot, pl.ds(r, ROWS + 2 * PAD), :]
        mid = x[PAD : PAD + ROWS]
        beside = x[PAD + 1 : PAD + 1 + ROWS] + x[PAD - 1 : PAD - 1 + ROWS]
        beside = beside + jnp.where(lane == nx - 1, 0.0, pltpu.roll(mid, nx - 1, 1))
        beside = beside + jnp.where(lane == 0, 0.0, pltpu.roll(mid, 1, 1))
        return mid, beside

    def add(j, x):
        acc[j] += jnp.sum(x.reshape(ROWS // 8, 8, nx), axis=0)

    def y_rows(p, r):
        inner, rows = inner_rows(r), pl.ds(r, ROWS)
        k, scale = code[p + 1, rows, :], inv[p + 1, rows, :]
        mid, beside = around(z, p + 2, r)
        q = k * mid - (beside + z[p + 1, inner, :] + z[p + 3, inner, :])
        out = q * scale
        y[p + 1, inner, :] = out
        if p >= 0:
            d = jnp.maximum(k, 1.0) * mid
            add(0, d * mid)
            add(1, d * d)
            add(2, jnp.where(scale > 0.0, 1.0, 0.0))
            add(3, mid * q)
            add(4, q * out)

    def complete_rows(r):
        inner, rows = inner_rows(r), pl.ds(r, ROWS)
        z[top + 2, inner, :] = part_z[0, rows, :] + inv[top + 1, rows, :] * lw_next[0, rows, :]
        z[1, inner, :] = z[1, inner, :] + inv[0, rows, :] * lw[0, rows, :]

    def low_rows(r):
        complete_rows(r)
        for p in range(top):
            y_rows(p, r)

    def low_chunk(c):
        when(jnp.logical_and(has_high, c >= raw // group), lambda: lw_down.wait_recv(c))
        when(has_low, lambda: top_up.wait_recv(c))
        over(c, low_rows, grow)
        forward_unit(jnp.logical_and(near, c >= groups - few), every - groups + c, True)
        forward_unit(jnp.logical_and(jnp.logical_not(near), lax.rem(c, 2) == 1), c // 2, False)

    def start_y(c):
        for i in range(group):
            y_down.start(c * group + i)

    staged(low_chunk, lambda c: when(jnp.logical_and(has_low, jnp.logical_not(gated)), lambda: start_y(c)), groups)

    def a_rows(p, r):
        inner, rows = inner_rows(r), pl.ds(r, ROWS)
        mid, beside = around(y, p + 1, r)
        below = y[p, inner, :]
        beside = beside + below
        if p < top:
            beside = beside + y[p + 2, inner, :]
        q = code[p + 1, rows, :] * mid - beside
        ay[p, rows, :] = jnp.where(inv[p + 1, rows, :] > 0.0, q, 0.0)
        add(5, mid * (q - below) if p == 0 else mid * q)

    def high_rows(r):
        y_rows(top, r)
        y_rows(-1, r)

    def high_chunk(c):
        when(has_high, lambda: z_down.wait_recv(c))
        for i in range(group):
            chunk = c * group + i
            when(has_low, lambda: next_up.wait_recv(chunk))
            when(jnp.logical_and(gating, chunk == chunks - LEAD), lambda: pl.semaphore_signal(
                gate, inc=1, **at(jnp.minimum(me + SPAN - 2, n - 1))))
        @pl.when(jnp.logical_and(gated, c == OPEN))
        def _():
            pl.semaphore_wait(gate, 1)

            def start(i, carry):
                start_y(i)
                return carry

            lax.fori_loop(0, groups, start, 0)

        over(c, high_rows, grow)
        for i in range(2):
            forward_unit(jnp.logical_and(jnp.logical_not(near), c < groups // 2), head + jnp.minimum(2 * c, groups - 2) + i, True)

    def image_rows(r):
        for p in range(depth):
            a_rows(p, r)

    staged(high_chunk, lambda c: over(c, image_rows, grow), groups)

    for j in range(6):
        t = jnp.sum(acc[j], axis=0, keepdims=True)
        part = t[:, 0:128]
        for c in range(128, nx, 128):
            part = part + t[:, c : c + 128]
        st[j : j + 1, :] = part
    st[6:8, :] = jnp.zeros((2, 128), jnp.float32)

    pair_in = pltpu.make_async_remote_copy(st, st_pair, pair_send.at[0], pair_recv.at[0], **at(partner))
    pair_out = pltpu.make_async_remote_copy(total, total, pair_send.at[1], pair_recv.at[1], **at(partner))
    st_start, st_whole = spread(st_pair, st_all, st_send, st_recv, 2, n // 2)

    @pl.when(even)
    def _():
        pair_in.start()

    @pl.when(odd)
    def _():
        pair_in.wait_recv()
        st_pair[...] = st_pair[...] + st[...]
        st_start()
        st_whole.wait_recv()
        st_all[0] = st_pair[...]
        total[...] = jnp.sum(st_all[...], axis=0)
        pair_out.start()

    @pl.when(has_low)
    def _():
        for copy in raw_copies:
            copy.wait_send()

    @pl.when(even)
    def _():
        pair_in.wait_send()
        pair_out.wait_recv()

    sums = jnp.broadcast_to(jnp.sum(total[...], axis=1, keepdims=True), (8, nx))
    gamma, squares, fluid = sums[0:1], sums[1:2], sums[2:3]
    delta, eta, theta = sums[3:4], sums[4:5], sums[5:6]
    alpha = gamma / delta
    gamma_next = gamma - 2.0 * alpha * delta + alpha * alpha * eta
    beta = gamma_next / gamma
    mixed = delta - alpha * eta
    curve = (delta - 2.0 * alpha * eta + alpha * alpha * theta) + 2.0 * beta * mixed + beta * beta * delta
    alpha_next = gamma_next / curve
    norm = 1.0 / jnp.sqrt(squares / jnp.maximum(fluid, 1.0) + EPS)
    cf[1:2, :] = alpha + alpha_next * (1.0 + beta)
    cf[2:3, :] = alpha * alpha_next
    cf[3:4, :] = norm
    cf[4:5, :] = alpha * alpha_next * norm

    def out_rows(r):
        inner, rows = inner_rows(r), pl.ds(r, ROWS)
        a, b = cf[1:2, :], cf[2:3, :]
        for p in range(depth):
            zz, yy = z[p + 2, inner, :], y[p + 1, inner, :]
            w[p, rows, :] = a * zz - b * yy
            s[p, rows, :] = (
                jnp.maximum(code[p + 1, rows, :], 1.0) * (zz - a * yy) + b * ay[p, rows, :]) * cf[3:4, :]

    def all_rows(i, carry):
        out_rows(pl.multiple_of(i * ROWS, 8))
        return carry

    lax.fori_loop(0, nb, all_rows, 0)

    def last_rows(r):
        inner, rows = inner_rows(r), pl.ds(r, ROWS)
        s[top, rows, :] = s[top, rows, :] - jnp.where(
            inv[top + 1, rows, :] > 0.0, cf[4:5, :] * y[depth + 1, inner, :], 0.0)

    @pl.when(has_high)
    def _():
        def last_chunk(c, carry):
            y_down.wait_recv(c)
            over(c, last_rows, grow)
            return carry
        lax.fori_loop(0, groups, last_chunk, 0)

    @pl.when(odd)
    def _():
        st_whole.wait_send()
        pair_out.wait_send()

    @pl.when(has_low)
    def _():
        for flow in (lw_down, z_down, y_down):
            flow.wait_send()

    @pl.when(has_high)
    def _():
        for flow in (top_up, next_up):
            flow.wait_send()

    mx_whole.wait_send()

    def forwarded(unit, carry):
        part = relay.at[0, pl.ds(0, grow)]
        pltpu.make_async_remote_copy(part, part, relay_send.at[unit], relay_recv.at[unit], **at(rl_target)).wait_send()
        return carry

    lax.fori_loop(rl_first, rl_last, forwarded, 0)


def store(w, s, w_hbm, s_hbm, sem):
    copies = [
        pltpu.make_async_copy(src.at[p], dst.at[p], sem.at[j, p])
        for j, (src, dst) in enumerate([(w, w_hbm), (s, s_hbm)]) for p in range(w.shape[0])
    ]
    for copy in copies:
        copy.start()
    for copy in copies:
        copy.wait()


def solution(mesh):
    n = mesh.shape["gz"]

    def local(u_face, v_face, w_face, smoke, obstacles):
        depth, ny, nx = u_face.shape
        nw = obstacles.shape[1]
        chunks, group, raw = 16, 2, 2
        crow = ny // chunks
        f32, i32 = jnp.float32, jnp.int32
        dma = pltpu.SemaphoreType.DMA
        any_spec = pl.BlockSpec(memory_space=pl.ANY)
        vmem_spec = pl.BlockSpec(memory_space=pltpu.VMEM)
        shape = pltpu.VMEM((depth, ny, nx), f32)
        results = pl.pallas_call(
            functools.partial(kernel, n, chunks, group, raw),
            out_shape=(shape, shape),
            in_specs=[any_spec] * 5,
            out_specs=(vmem_spec, vmem_spec),
            scratch_shapes=[
                pltpu.VMEM((depth, ny, nx), f32),
                pltpu.VMEM((depth, ny + PAD, nx), f32),
                pltpu.VMEM((depth + 3, ny + 2 * PAD, nx), f32),
                pltpu.VMEM((1, ny, nx), f32),
                pltpu.VMEM((depth + 2, ny + 2 * PAD, nx), f32),
                pltpu.VMEM((depth + 1, ny, nx), f32),
                pltpu.VMEM((depth + 1, ny, nx), f32),
                pltpu.VMEM((depth, ny, nx), f32),
                pltpu.VMEM((1, ny, nx), f32),
                pltpu.VMEM((1, ny, nx), f32),
                pltpu.VMEM((1, raw * crow, nx), f32),
                pltpu.VMEM((1, 3 * ny // 2, nx), f32),
                pltpu.VMEM((depth + 3, nw, nx), i32),
                pltpu.VMEM((depth + 1, 4, nw, nx), i32),
                pltpu.VMEM((6, 8, nx), f32),
                pltpu.VMEM((8, nx), f32),
                pltpu.VMEM((1, 128), f32),
                pltpu.VMEM((n, 1, 128), f32),
                pltpu.VMEM((8, 128), f32),
                pltpu.VMEM((8, 128), f32),
                pltpu.VMEM((n // 2, 8, 128), f32),
                pltpu.VMEM((8, 128), f32),
                dma((4 * depth + 3,)),
                dma((2,)), dma((2,)),
                dma((2,)), dma((2,)),
                dma((5,)),
                dma((chunks // group,)), dma((chunks // group,)), dma((chunks // group,)), dma((chunks // group,)),
                dma((chunks,)),
                dma((3 * chunks // group // 2,)), dma((3 * chunks // group // 2,)),
                dma, dma, dma, dma,
                dma((2,)), dma((2,)),
                pltpu.SemaphoreType.REGULAR,
            ],
            compiler_params=pltpu.CompilerParams(
                collective_id=0, has_side_effects=True, vmem_limit_bytes=58_000_000),
            name="smoke_step",
        )(u_face, v_face, w_face, smoke, obstacles)
        out = jax.ShapeDtypeStruct((depth, ny, nx), f32)
        return pl.pallas_call(
            store,
            out_shape=(out, out),
            in_specs=[vmem_spec] * 2,
            out_specs=(any_spec, any_spec),
            scratch_shapes=[dma((2, depth))],
            compiler_params=pltpu.CompilerParams(vmem_limit_bytes=1_000_000),
            name="store",
        )(*results)

    placed = P("gz", None, None)
    return jax.shard_map(local, mesh=mesh, in_specs=(placed,) * 5, out_specs=(placed, placed), check_vma=False)
```

```python
import functools

import jax
import jax.numpy as jnp
from jax import lax
from jax.experimental import pallas as pl
from jax.experimental.pallas import tpu as pltpu
from jax.sharding import PartitionSpec as P

EPS = 1e-06
CFL = 0.5
BUOYANCY = 100.0

ROWS = 32
PAD = 8
SPAN = 8
LEAD = 4
LAG = 400
OPEN = 5


def kernel(n, chunks, group, raw_rows, u_hbm, v_hbm, w_hbm, s_hbm, ob_hbm, w, s,
           u, v, z, part_z, y, code, inv, ay, lw, lw_next, s_next, relay, ob, cw, acc, cf, mx, mx_all, st, st_pair, st_all, total,
           in_sem, ob_send, ob_recv, raw_send, raw_recv, send, lw_recv, dn_recv, yd_recv, top_recv, next_recv, relay_recv, relay_send,
           mx_send, mx_recv, st_send, st_recv, pair_send, pair_recv, gate):
    depth, ny, nx = w.shape
    top = depth - 1
    nb = ny // ROWS
    crow = ny // chunks
    grow = crow * group
    groups = chunks // group
    me = lax.axis_index("gz")
    has_low, has_high = me > 0, me < n - 1
    low, high = jnp.maximum(me - 1, 0), jnp.minimum(me + 1, n - 1)
    odd = lax.rem(me, 2) == 1
    even = jnp.logical_not(odd)
    partner = me + 1 - 2 * lax.rem(me, 2)
    place = lax.rem(me, SPAN)
    gated = jnp.logical_and(has_low, place == 0)
    gating = jnp.logical_and(place == 2, me + SPAN - 2 < n)

    span, spans = me // SPAN, n // SPAN
    plane_units = groups
    head = plane_units // 2
    few = plane_units // 4
    every = head + plane_units

    def piece(count):
        return head - jnp.maximum(count - plane_units, 0), head + jnp.minimum(count, plane_units)

    def select(cases):
        first, last = 0, 0
        for cond, (lo, hi) in cases:
            first, last = jnp.where(cond, lo, first), jnp.where(cond, hi, last)
        return first, last

    def cross_up(lower):
        return piece(jnp.minimum(head * (spans - 1 - lower), every))

    def cross_down(upper):
        return piece(jnp.minimum(head * upper, every))

    side = (every - few, every)
    whole_spans = n % SPAN == 0
    crossing = jnp.logical_and(whole_spans, span + 1 < spans)
    crossed = jnp.logical_and(whole_spans, span > 0)
    up_first, up_last = select([(jnp.logical_and(whole_spans, place == 3), side), (jnp.logical_and(crossing, place == 7), cross_up(span))])
    dn_first, dn_last = select([(jnp.logical_and(whole_spans, place == 4), side), (jnp.logical_and(crossed, place == 0), cross_down(span))])
    up_via = jnp.clip(jnp.where(place == 3, me + 4, me - 2), 0, n - 1)
    dn_via = jnp.clip(jnp.where(place == 4, me - 4, me + 3), 0, n - 1)
    relays_up = jnp.logical_and(whole_spans, jnp.logical_or(place == 7, jnp.logical_and(place == 5, crossing)))
    relays_down = jnp.logical_and(whole_spans, jnp.logical_or(place == 0, jnp.logical_and(place == 3, crossed)))
    near = jnp.logical_or(place == 7, place == 0)
    rl_first, rl_last = select([
        (jnp.logical_and(whole_spans, near), side),
        (jnp.logical_and(crossing, place == 5), cross_up(span)),
        (jnp.logical_and(crossed, place == 3), cross_down(span)),
    ])
    rl_target = jnp.clip(
        jnp.where(place == 7, me - 3, jnp.where(place == 5, me + 3, jnp.where(place == 0, me + 3, me - 4))), 0, n - 1)

    def at(device):
        return dict(device_id=(device,), device_id_type=pl.DeviceIdType.MESH)

    ins = [(u_hbm, u), (v_hbm, v), (w_hbm, w), (s_hbm, s)]

    def load(k, p, first=0, rows=ny, sem=None):
        src, dst = ins[k]
        part = pl.ds(first, rows)
        return pltpu.make_async_copy(src.at[p, part], dst.at[p, part], in_sem.at[k * depth + p if sem is None else sem])

    ob_in = pltpu.make_async_copy(ob_hbm, ob.at[pl.ds(2, depth)], in_sem.at[4 * depth])
    raw_in = [load(k, 0, 0, raw_rows, 4 * depth + k - 1) for k in (2, 3)]
    rest_in = {(k, p): load(k, p, raw_rows, ny - raw_rows) if k >= 2 and p == 0 else load(k, p)
               for k in range(4) for p in range(depth)}
    scan = [(k, p) for k in range(3) for p in range(depth - 1, -1, -1)]
    ob_in.start()
    for pair in scan:
        rest_in[pair].start()
    for copy in raw_in:
        copy.start()

    barrier = pltpu.get_barrier_semaphore()

    def greet(i, carry):
        pl.semaphore_signal(barrier, inc=1, **at(lax.rem(me + i, n)))
        return carry

    lax.fori_loop(1, n, greet, 0)

    zrow = jnp.zeros((PAD, nx), jnp.float32)
    for p in range(1, depth + 2):
        z[p, 0:PAD, :] = zrow
        z[p, ny + PAD : ny + 2 * PAD, :] = zrow
    for p in range(1, depth + 1):
        y[p, 0:PAD, :] = zrow
        y[p, ny + PAD : ny + 2 * PAD, :] = zrow
    for p in range(depth):
        v[p, ny : ny + PAD, :] = zrow
    acc[...] = jnp.zeros_like(acc)

    def zero_planes(ref, planes, offset):
        def body(i, carry):
            for p in planes:
                ref[p, pl.ds(pl.multiple_of(i * ROWS + offset, 8), ROWS), :] = jnp.zeros((ROWS, nx), jnp.float32)
            return carry
        lax.fori_loop(0, nb, body, 0)

    ob_in.wait()
    pl.semaphore_wait(barrier, n - 1)

    ob_down = pltpu.make_async_remote_copy(
        ob.at[pl.ds(2, 1)], ob.at[pl.ds(depth + 2, 1)], ob_send.at[0], ob_recv.at[0], **at(low))
    ob_up = pltpu.make_async_remote_copy(
        ob.at[pl.ds(depth, 2)], ob.at[pl.ds(0, 2)], ob_send.at[1], ob_recv.at[1], **at(high))

    raw_part = pl.ds(0, raw_rows)
    raw_copies = [
        pltpu.make_async_remote_copy(
            src.at[0, raw_part], dst.at[0, raw_part], raw_send.at[j], raw_recv.at[j], **at(low))
        for j, (src, dst) in enumerate([(w, lw_next), (s, s_next)])
    ]

    @pl.when(has_low)
    def _():
        ob_down.start()

    @pl.when(has_high)
    def _():
        ob_up.start()

    @pl.when(jnp.logical_not(has_low))
    def _():
        ob[0:2] = jnp.zeros((2,) + ob.shape[1:], jnp.int32)
        zero_planes(z, (0, 1), PAD)

    @pl.when(jnp.logical_not(has_high))
    def _():
        ob[depth + 2 : depth + 3] = jnp.zeros((1,) + ob.shape[1:], jnp.int32)
        zero_planes(z, (depth + 2,), PAD)
        zero_planes(lw_next, (0,), 0)

    def largest(k, p, first, last, m):
        def body(i, m):
            a = jnp.abs(ins[k][1][p, pl.ds(pl.multiple_of(i * ROWS, 8), ROWS), :])
            return jnp.maximum(m, jnp.max(a.reshape(ROWS // 8, 8, nx), axis=0))
        return lax.fori_loop(first, last, body, m)

    peak = jnp.zeros((8, nx), jnp.float32)
    for k, p in scan:
        rest_in[k, p].wait()
        if k == 1:
            rest_in[3, p].start()
        peak = largest(k, p, raw_rows // ROWS if (k, p) == (2, 0) else 0, nb, peak)
    raw_in[0].wait()
    peak = largest(2, 0, 0, raw_rows // ROWS, peak)
    m = jnp.max(peak, axis=0, keepdims=True)
    part = m[:, 0:128]
    for c in range(128, nx, 128):
        part = jnp.maximum(part, m[:, c : c + 128])
    mx[...] = part

    def spread(src, dst, send, recv, step, count):
        def start(i, carry):
            pltpu.make_async_remote_copy(
                src, dst.at[i], send, recv, **at(lax.rem(me + step * i, n))).start()
            return carry

        everything = dst.at[pl.ds(1, count - 1)]
        whole = pltpu.make_async_remote_copy(everything, everything, send, recv, **at(lax.rem(me + step, n)))
        return (lambda: lax.fori_loop(1, count, start, 0)), whole

    mx_start, mx_whole = spread(mx, mx_all, mx_send, mx_recv, 1, n)
    mx_start()
    raw_in[1].wait()

    @pl.when(has_low)
    def _():
        for copy in raw_copies:
            copy.start()

    @pl.when(has_low)
    def _():
        ob_down.wait_send()
        ob_up.wait_recv()

    @pl.when(has_high)
    def _():
        ob_up.wait_send()
        ob_down.wait_recv()

    row_id = lax.broadcasted_iota(jnp.int32, (nb, nx), 0)
    col_id = lax.broadcasted_iota(jnp.int32, (nb, nx), 1)
    srl = lax.shift_right_logical
    c1, c31 = jnp.int32(1), jnp.int32(31)
    full1, full31 = jnp.full((nb, nx), c1), jnp.full((nb, nx), c31)
    for p in range(depth + 1):
        mid = ob[p + 1]
        after = jnp.where(row_id == nb - 1, 0, pltpu.roll(mid, nb - 1, 0))
        before = jnp.where(row_id == 0, 0, pltpu.roll(mid, 1, 0))
        a = srl(mid, full1) | (after << full31)
        b = (mid << full1) | srl(before, full31)
        c = jnp.where(col_id == nx - 1, 0, pltpu.roll(mid, nx - 1, 1))
        d = jnp.where(col_id == 0, 0, pltpu.roll(mid, 1, 1))
        e, f = ob[p], ob[p + 2]
        s1, k1 = a ^ b ^ c, (a & b) | (c & (a | b))
        s2, k2 = d ^ e ^ f, (d & e) | (f & (d | e))
        k3 = s1 & s2
        cw[p, 0] = s1 ^ s2
        cw[p, 1] = k1 ^ k2 ^ k3
        cw[p, 2] = (k1 & k2) | (k3 & (k1 | k2))
        cw[p, 3] = mid
    @pl.when(jnp.logical_not(has_low))
    def _():
        cw[0, 3] = jnp.full((nb, nx), -1, jnp.int32)

    half = 16
    places = lax.broadcasted_iota(jnp.int32, (half, nx), 0)

    def code_rows(b):
        for p in range(depth + 1):
            for k0 in range(0, ROWS, half):
                bits = [
                    srl(jnp.broadcast_to(cw[p, j, pl.ds(b, 1), :], (half, nx)), places + k0) & 1
                    for j in range(4)
                ]
                k = (6 - (bits[0] + (bits[1] << 1) + (bits[2] << 2))).astype(jnp.float32)
                rows = pl.ds(pl.multiple_of(b * ROWS + k0, 8), half)
                code[p, rows, :] = k
                inv[p, rows, :] = jnp.where(bits[3] == 1, 0.0, 1.0 / jnp.maximum(k, 1.0))

    for p in range(depth):
        rest_in[3, p].wait()

    def ready(b, carry):
        code_rows(b)
        return carry

    lax.fori_loop(0, nb // 4, ready, 0)
    mx_whole.wait_recv()
    mx_all[0] = mx[...]
    fastest = jnp.max(jnp.max(mx_all[...], axis=0), axis=1, keepdims=True)
    cf[0:1, :] = (CFL / (jnp.broadcast_to(fastest, (1, nx)) + EPS)) * BUOYANCY

    lane = lax.broadcasted_iota(jnp.int32, (ROWS, nx), 1)

    def lifted(p, r):
        rows = pl.ds(r, ROWS)
        return w[p, rows, :] + cf[0:1, :] * s[p, rows, :]

    def over(c, fn, rows=crow):
        def inner(i, k):
            fn(pl.multiple_of(c * rows + i * ROWS, 8))
            return k
        lax.fori_loop(0, rows // ROWS, inner, 0)

    def staged(first, second, count=chunks):
        def body(c, carry):
            @pl.when(c < count)
            def _():
                first(c)

            @pl.when(c > 0)
            def _():
                second(c - 1)
            return carry
        lax.fori_loop(0, count + 1, body, 0)

    def when(cond, fn):
        @pl.when(cond)
        def _():
            fn()

    class Flow:
        def __init__(self, src, dst, send, recv, device, per, src_pad=PAD, dst_pad=PAD, first=0):
            def copy(start, rows, index):
                def part(pad):
                    return pl.ds(pl.multiple_of(start + pad, 8), rows)
                return pltpu.make_async_remote_copy(
                    src[0].at[src[1], part(src_pad)], dst[0].at[dst[1], part(dst_pad)], send, recv.at[index], **at(device))

            self.start = lambda c: copy(c * crow, crow, c // per).start()
            self.wait_recv = lambda i: copy(i * crow * per, crow * per, i).wait_recv()
            self.start_rest = lambda: copy(first, crow - first % crow, first // crow // per).start()
            self.wait_rest = lambda: copy(first, grow - first, 0).wait_recv()
            self.wait_send = lambda: copy(first, ny - first, 0).wait_send()

            def aside(c, unit):
                return pl.ds(pl.multiple_of(unit * grow + lax.rem(c, group) * crow, 8), crow)

            def detour(c, unit, via):
                rows = pl.ds(pl.multiple_of(c * crow + src_pad, 8), crow)
                pltpu.make_async_remote_copy(
                    src[0].at[src[1], rows], relay.at[0, aside(c, unit)], send, relay_recv.at[unit // 2], **at(via)).start()

            def forward(c, unit):
                rows = pl.ds(pl.multiple_of(c * crow + dst_pad, 8), crow)
                pltpu.make_async_remote_copy(
                    relay.at[0, aside(c, unit)], dst[0].at[dst[1], rows], relay_send, recv.at[c // per],
                    **at(rl_target)).start()

            self.detour, self.forward = detour, forward

    lw_down = Flow((lw, 0), (lw_next, 0), send.at[0], lw_recv, low, group, 0, 0, raw_rows)
    z_down = Flow((z, 2), (z, depth + 2), send.at[1], dn_recv, low, group)
    y_down = Flow((y, 1), (y, depth + 1), send.at[2], yd_recv, low, group)
    top_up = Flow((part_z, 0), (z, 1), send.at[3], top_recv, high, group, 0)
    next_up = Flow((z, top + 1), (z, 0), send.at[4], next_recv, high, 1)

    def send_chunk(flow, second, c, first, last, via):
        unit = c // group + (head if second else head - plane_units)
        aside = jnp.logical_and(unit >= first, unit < last)
        when(aside, lambda: flow.detour(c, jnp.maximum(unit, 0), via))
        when(jnp.logical_not(aside), lambda: flow.start(c))

    def set_aside(first, count):
        part = relay.at[0, pl.ds(0, count * grow)]
        return pltpu.make_async_remote_copy(part, part, relay_send, relay_recv.at[first // 2], **at(rl_target))

    def forward_pair(cond, unit, second):
        def run(flow):
            set_aside(unit, 2).wait_recv()
            for i in range(2 * group):
                flow.forward((unit + (-head if second else plane_units - head)) * group + i, unit + i // group)

        inside = jnp.logical_and(cond, jnp.logical_and(unit >= rl_first, unit < rl_last))
        when(jnp.logical_and(inside, relays_up), lambda: run(next_up if second else top_up))
        when(jnp.logical_and(inside, relays_down), lambda: run(z_down if second else lw_down))

    def flat(p, r):
        a = u[p, pl.ds(r, ROWS), :]
        b = v[p, pl.ds(r, ROWS + PAD), :]
        return jnp.where(lane == nx - 1, 0.0, pltpu.roll(a, nx - 1, 1)) - a + (b[1 : ROWS + 1] - b[:ROWS])

    def inner_rows(r):
        return pl.ds(pl.multiple_of(r + PAD, 8), ROWS)

    def lw_rows(r):
        lw[0, pl.ds(r, ROWS), :] = lifted(0, r)

    def shifted(c):
        return lax.rem(c + raw_rows // crow, chunks)

    def lw_sends(c):
        when(jnp.logical_and(has_low, c * crow >= raw_rows),
             lambda: send_chunk(lw_down, False, c, dn_first, dn_last, dn_via))
        if raw_rows % crow:
            when(jnp.logical_and(has_low, c == raw_rows // crow), lw_down.start_rest)

    staged(lambda c: over(shifted(c), lw_rows), lambda c: lw_sends(shifted(c)))

    def first_rows(r):
        when(r >= ny // 4, lambda: code_rows(r // ROWS))
        rows = pl.ds(r, ROWS)
        part_z[0, rows, :] = inv[top + 1, rows, :] * (flat(top, r) - lifted(top, r))

    staged(lambda c: over(c, first_rows),
           lambda c: when(has_high, lambda: send_chunk(top_up, False, c, up_first, up_last, up_via)))

    def z_rows(p, r):
        rows = pl.ds(r, ROWS)
        own = lw[0, rows, :] if p == 0 else lifted(p, r)
        z[p + 2, inner_rows(r), :] = inv[p + 1, rows, :] * (flat(p, r) + (lifted(p + 1, r) - own))

    for p in range(top):
        def z_sends(c, p=p):
            if p == 0:
                when(has_low, lambda: send_chunk(z_down, True, c, dn_first, dn_last, dn_via))
            if p == top - 1:
                when(has_high, lambda: send_chunk(next_up, True, c, up_first, up_last, up_via))
        staged(lambda c, p=p: over(c, functools.partial(z_rows, p)), z_sends)

    @pl.when(has_high)
    def _():
        for copy in raw_copies:
            copy.wait_recv()

        def lift(i, carry):
            rows = pl.ds(pl.multiple_of(i * ROWS, 8), ROWS)
            lw_next[0, rows, :] = lw_next[0, rows, :] + cf[0:1, :] * s_next[0, rows, :]
            return carry

        lax.fori_loop(0, raw_rows // ROWS, lift, 0)

    def around(ref, slot, r):
        x = ref[slot, pl.ds(r, ROWS + 2 * PAD), :]
        mid = x[PAD : PAD + ROWS]
        beside = x[PAD + 1 : PAD + 1 + ROWS] + x[PAD - 1 : PAD - 1 + ROWS]
        beside = beside + jnp.where(lane == nx - 1, 0.0, pltpu.roll(mid, nx - 1, 1))
        beside = beside + jnp.where(lane == 0, 0.0, pltpu.roll(mid, 1, 1))
        return mid, beside

    def add(j, x):
        acc[j] += jnp.sum(x.reshape(ROWS // 8, 8, nx), axis=0)

    def y_rows(p, r):
        inner, rows = inner_rows(r), pl.ds(r, ROWS)
        k, scale = code[p + 1, rows, :], inv[p + 1, rows, :]
        mid, beside = around(z, p + 2, r)
        q = k * mid - (beside + z[p + 1, inner, :] + z[p + 3, inner, :])
        out = q * scale
        y[p + 1, inner, :] = out
        if p >= 0:
            d = jnp.maximum(k, 1.0) * mid
            add(0, d * mid)
            add(1, d * d)
            add(2, jnp.where(scale > 0.0, 1.0, 0.0))
            add(3, mid * q)
            add(4, q * out)

    def complete_rows(r):
        inner, rows = inner_rows(r), pl.ds(r, ROWS)
        z[top + 2, inner, :] = part_z[0, rows, :] + inv[top + 1, rows, :] * lw_next[0, rows, :]
        z[1, inner, :] = z[1, inner, :] + inv[0, rows, :] * lw[0, rows, :]

    def low_rows(r):
        complete_rows(r)
        for p in range(top):
            y_rows(p, r)

    def low_chunk(c):
        when(jnp.logical_and(has_high, c > 0), lambda: lw_down.wait_recv(c))
        if raw_rows < grow:
            when(jnp.logical_and(has_high, c == 0), lw_down.wait_rest)
        when(has_low, lambda: top_up.wait_recv(c))
        over(c, low_rows, grow)
        forward_pair(jnp.logical_and(near, c == groups - 1), every - few, True)
        forward_pair(jnp.logical_and(jnp.logical_not(near), lax.rem(c, 4) == 3), c // 4 * 2, False)

    def start_y(c):
        for i in range(group):
            y_down.start(c * group + i)

    staged(low_chunk, lambda c: when(jnp.logical_and(has_low, jnp.logical_not(gated)), lambda: start_y(c)), groups)

    def a_rows(p, r):
        inner, rows = inner_rows(r), pl.ds(r, ROWS)
        mid, beside = around(y, p + 1, r)
        below = y[p, inner, :]
        beside = beside + below
        if p < top:
            beside = beside + y[p + 2, inner, :]
        q = code[p + 1, rows, :] * mid - beside
        ay[p, rows, :] = jnp.where(inv[p + 1, rows, :] > 0.0, q, 0.0)
        add(5, mid * (q - below) if p == 0 else mid * q)

    def high_rows(r):
        y_rows(top, r)
        y_rows(-1, r)

    def high_chunk(c):
        when(has_high, lambda: z_down.wait_recv(c))
        for i in range(group):
            chunk = c * group + i
            when(has_low, lambda: next_up.wait_recv(chunk))

            @pl.when(jnp.logical_and(gating, chunk == chunks - LEAD))
            def _():
                pl.delay(LAG)
                pl.semaphore_signal(gate, inc=1, **at(jnp.minimum(me + SPAN - 2, n - 1)))

        @pl.when(jnp.logical_and(gated, c == OPEN))
        def _():
            pl.semaphore_wait(gate, 1)

            def start(i, carry):
                start_y(i)
                return carry

            lax.fori_loop(0, groups, start, 0)

        over(c, high_rows, grow)
        forward_pair(jnp.logical_and(jnp.logical_not(near), c < groups // 2), head + jnp.minimum(2 * c, groups - 2), True)

    def image_rows(r):
        for p in range(depth):
            a_rows(p, r)

    staged(high_chunk, lambda c: over(c, image_rows, grow), groups)

    for j in range(6):
        t = jnp.sum(acc[j], axis=0, keepdims=True)
        part = t[:, 0:128]
        for c in range(128, nx, 128):
            part = part + t[:, c : c + 128]
        st[j : j + 1, :] = part
    st[6:8, :] = jnp.zeros((2, 128), jnp.float32)

    pair_in = pltpu.make_async_remote_copy(st, st_pair, pair_send.at[0], pair_recv.at[0], **at(partner))
    pair_out = pltpu.make_async_remote_copy(total, total, pair_send.at[1], pair_recv.at[1], **at(partner))
    st_start, st_whole = spread(st_pair, st_all, st_send, st_recv, 2, n // 2)

    @pl.when(even)
    def _():
        pair_in.start()

    @pl.when(odd)
    def _():
        pair_in.wait_recv()
        st_pair[...] = st_pair[...] + st[...]
        st_start()
        st_whole.wait_recv()
        st_all[0] = st_pair[...]
        total[...] = jnp.sum(st_all[...], axis=0)
        pair_out.start()

    @pl.when(has_low)
    def _():
        for copy in raw_copies:
            copy.wait_send()

    @pl.when(even)
    def _():
        pair_in.wait_send()
        pair_out.wait_recv()

    sums = jnp.broadcast_to(jnp.sum(total[...], axis=1, keepdims=True), (8, nx))
    gamma, squares, fluid = sums[0:1], sums[1:2], sums[2:3]
    delta, eta, theta = sums[3:4], sums[4:5], sums[5:6]
    alpha = gamma / delta
    gamma_next = gamma - 2.0 * alpha * delta + alpha * alpha * eta
    beta = gamma_next / gamma
    mixed = delta - alpha * eta
    curve = (delta - 2.0 * alpha * eta + alpha * alpha * theta) + 2.0 * beta * mixed + beta * beta * delta
    alpha_next = gamma_next / curve
    norm = 1.0 / jnp.sqrt(squares / jnp.maximum(fluid, 1.0) + EPS)
    cf[1:2, :] = alpha + alpha_next * (1.0 + beta)
    cf[2:3, :] = alpha * alpha_next
    cf[3:4, :] = norm
    cf[4:5, :] = alpha * alpha_next * norm

    def out_rows(r):
        inner, rows = inner_rows(r), pl.ds(r, ROWS)
        a, b = cf[1:2, :], cf[2:3, :]
        for p in range(depth):
            zz, yy = z[p + 2, inner, :], y[p + 1, inner, :]
            w[p, rows, :] = a * zz - b * yy
            s[p, rows, :] = (
                jnp.maximum(code[p + 1, rows, :], 1.0) * (zz - a * yy) + b * ay[p, rows, :]) * cf[3:4, :]

    def all_rows(i, carry):
        out_rows(pl.multiple_of(i * ROWS, 8))
        return carry

    lax.fori_loop(0, nb, all_rows, 0)

    def last_rows(r):
        inner, rows = inner_rows(r), pl.ds(r, ROWS)
        s[top, rows, :] = s[top, rows, :] - jnp.where(
            inv[top + 1, rows, :] > 0.0, cf[4:5, :] * y[depth + 1, inner, :], 0.0)

    @pl.when(has_high)
    def _():
        def last_chunk(c, carry):
            y_down.wait_recv(c)
            over(c, last_rows, grow)
            return carry
        lax.fori_loop(0, groups, last_chunk, 0)

    @pl.when(odd)
    def _():
        st_whole.wait_send()
        pair_out.wait_send()

    @pl.when(has_low)
    def _():
        for flow in (lw_down, z_down, y_down):
            flow.wait_send()

    @pl.when(has_high)
    def _():
        for flow in (top_up, next_up):
            flow.wait_send()

    mx_whole.wait_send()

    for count in (few, head, 2 * head, every):
        when(rl_last - rl_first == count, lambda count=count: set_aside(0, count).wait_send())


def store(w, s, w_hbm, s_hbm, sem):
    copies = [
        pltpu.make_async_copy(src.at[p], dst.at[p], sem.at[j, p])
        for j, (src, dst) in enumerate([(w, w_hbm), (s, s_hbm)]) for p in range(w.shape[0])
    ]
    for copy in copies:
        copy.start()
    for copy in copies:
        copy.wait()


def solution(mesh):
    n = mesh.shape["gz"]

    def local(u_face, v_face, w_face, smoke, obstacles):
        depth, ny, nx = u_face.shape
        nw = obstacles.shape[1]
        chunks, group = 16, 2
        raw_rows = 3 * ny // 32
        f32, i32 = jnp.float32, jnp.int32
        dma = pltpu.SemaphoreType.DMA
        any_spec = pl.BlockSpec(memory_space=pl.ANY)
        vmem_spec = pl.BlockSpec(memory_space=pltpu.VMEM)
        shape = pltpu.VMEM((depth, ny, nx), f32)
        results = pl.pallas_call(
            functools.partial(kernel, n, chunks, group, raw_rows),
            out_shape=(shape, shape),
            in_specs=[any_spec] * 5,
            out_specs=(vmem_spec, vmem_spec),
            scratch_shapes=[
                pltpu.VMEM((depth, ny, nx), f32),
                pltpu.VMEM((depth, ny + PAD, nx), f32),
                pltpu.VMEM((depth + 3, ny + 2 * PAD, nx), f32),
                pltpu.VMEM((1, ny, nx), f32),
                pltpu.VMEM((depth + 2, ny + 2 * PAD, nx), f32),
                pltpu.VMEM((depth + 1, ny, nx), f32),
                pltpu.VMEM((depth + 1, ny, nx), f32),
                pltpu.VMEM((depth, ny, nx), f32),
                pltpu.VMEM((1, ny, nx), f32),
                pltpu.VMEM((1, ny, nx), f32),
                pltpu.VMEM((1, raw_rows, nx), f32),
                pltpu.VMEM((1, 3 * ny // 2, nx), f32),
                pltpu.VMEM((depth + 3, nw, nx), i32),
                pltpu.VMEM((depth + 1, 4, nw, nx), i32),
                pltpu.VMEM((6, 8, nx), f32),
                pltpu.VMEM((8, nx), f32),
                pltpu.VMEM((1, 128), f32),
                pltpu.VMEM((n, 1, 128), f32),
                pltpu.VMEM((8, 128), f32),
                pltpu.VMEM((8, 128), f32),
                pltpu.VMEM((n // 2, 8, 128), f32),
                pltpu.VMEM((8, 128), f32),
                dma((4 * depth + 3,)),
                dma((2,)), dma((2,)),
                dma((2,)), dma((2,)),
                dma((5,)),
                dma((chunks // group,)), dma((chunks // group,)), dma((chunks // group,)), dma((chunks // group,)),
                dma((chunks,)),
                dma((3 * chunks // group // 4,)), dma,
                dma, dma, dma, dma,
                dma((2,)), dma((2,)),
                pltpu.SemaphoreType.REGULAR,
            ],
            compiler_params=pltpu.CompilerParams(
                collective_id=0, has_side_effects=True, vmem_limit_bytes=58_000_000),
            name="smoke_step",
        )(u_face, v_face, w_face, smoke, obstacles)
        out = jax.ShapeDtypeStruct((depth, ny, nx), f32)
        return pl.pallas_call(
            store,
            out_shape=(out, out),
            in_specs=[vmem_spec] * 2,
            out_specs=(any_spec, any_spec),
            scratch_shapes=[dma((2, depth))],
            compiler_params=pltpu.CompilerParams(vmem_limit_bytes=1_000_000),
            name="store",
        )(*results)

    placed = P("gz", None, None)
    return jax.shard_map(local, mesh=mesh, in_specs=(placed,) * 5, out_specs=(placed, placed), check_vma=False)
```

```python
import functools

import jax
import jax.numpy as jnp
from jax import lax
from jax.experimental import pallas as pl
from jax.experimental.pallas import tpu as pltpu
from jax.sharding import PartitionSpec as P

EPS = 1e-06
CFL = 0.5
BUOYANCY = 100.0

ROWS = 32
PAD = 8
SPAN = 8
LEAD = 4
LAG = 700
OPEN = 5


def kernel(n, chunks, group, raw_rows, u_hbm, v_hbm, w_hbm, s_hbm, ob_hbm, w, s,
           u, v, z, part_z, y, code, inv, ay, lw, lw_next, s_next, relay, ob, cw, acc, cf, mx, mx_all, st, st_pair, st_all, total,
           in_sem, ob_send, ob_recv, raw_send, raw_recv, send, lw_recv, dn_recv, yd_recv, top_recv, next_recv, relay_recv, relay_send,
           mx_send, mx_recv, st_send, st_recv, pair_send, pair_recv, gate):
    depth, ny, nx = w.shape
    top = depth - 1
    nb = ny // ROWS
    crow = ny // chunks
    grow = crow * group
    groups = chunks // group
    me = lax.axis_index("gz")
    has_low, has_high = me > 0, me < n - 1
    low, high = jnp.maximum(me - 1, 0), jnp.minimum(me + 1, n - 1)
    odd = lax.rem(me, 2) == 1
    even = jnp.logical_not(odd)
    partner = me + 1 - 2 * lax.rem(me, 2)
    place = lax.rem(me, SPAN)
    gated = jnp.logical_and(has_low, place == 0)
    gating = jnp.logical_and(place == 2, me + SPAN - 2 < n)

    span, spans = me // SPAN, n // SPAN
    plane_units = groups
    head = plane_units // 2
    few = plane_units // 4
    every = head + plane_units

    def piece(count):
        return head - jnp.maximum(count - plane_units, 0), head + jnp.minimum(count, plane_units)

    def select(cases):
        first, last = 0, 0
        for cond, (lo, hi) in cases:
            first, last = jnp.where(cond, lo, first), jnp.where(cond, hi, last)
        return first, last

    def cross_up(lower):
        return piece(jnp.minimum(head * (spans - 1 - lower), every))

    def cross_down(upper):
        return piece(jnp.minimum(head * upper, every))

    side = (every - few, every)
    whole_spans = n % SPAN == 0
    crossing = jnp.logical_and(whole_spans, span + 1 < spans)
    crossed = jnp.logical_and(whole_spans, span > 0)
    up_first, up_last = select([(jnp.logical_and(whole_spans, place == 3), side), (jnp.logical_and(crossing, place == 7), cross_up(span))])
    dn_first, dn_last = select([(jnp.logical_and(whole_spans, place == 4), side), (jnp.logical_and(crossed, place == 0), cross_down(span))])
    up_via = jnp.clip(jnp.where(place == 3, me + 4, me - 2), 0, n - 1)
    dn_via = jnp.clip(jnp.where(place == 4, me - 4, me + 3), 0, n - 1)
    relays_up = jnp.logical_and(whole_spans, jnp.logical_or(place == 7, jnp.logical_and(place == 5, crossing)))
    relays_down = jnp.logical_and(whole_spans, jnp.logical_or(place == 0, jnp.logical_and(place == 3, crossed)))
    near = jnp.logical_or(place == 7, place == 0)
    rl_first, rl_last = select([
        (jnp.logical_and(whole_spans, near), side),
        (jnp.logical_and(crossing, place == 5), cross_up(span)),
        (jnp.logical_and(crossed, place == 3), cross_down(span)),
    ])
    rl_target = jnp.clip(
        jnp.where(place == 7, me - 3, jnp.where(place == 5, me + 3, jnp.where(place == 0, me + 3, me - 4))), 0, n - 1)

    def at(device):
        return dict(device_id=(device,), device_id_type=pl.DeviceIdType.MESH)

    ins = [(u_hbm, u), (v_hbm, v), (w_hbm, w), (s_hbm, s)]

    def load(k, p, first=0, rows=ny, sem=None):
        src, dst = ins[k]
        part = pl.ds(first, rows)
        return pltpu.make_async_copy(src.at[p, part], dst.at[p, part], in_sem.at[k * depth + p if sem is None else sem])

    ob_in = pltpu.make_async_copy(ob_hbm, ob.at[pl.ds(2, depth)], in_sem.at[4 * depth])
    raw_in = [load(k, 0, 0, raw_rows, 4 * depth + k - 1) for k in (2, 3)]
    rest_in = {(k, p): load(k, p, raw_rows, ny - raw_rows) if k >= 2 and p == 0 else load(k, p)
               for k in range(4) for p in range(depth)}
    scan = [(k, p) for k in range(3) for p in range(depth - 1, -1, -1)]
    ob_in.start()
    for pair in scan:
        rest_in[pair].start()
    for copy in raw_in:
        copy.start()

    barrier = pltpu.get_barrier_semaphore()

    def greet(i, carry):
        pl.semaphore_signal(barrier, inc=1, **at(lax.rem(me + i, n)))
        return carry

    lax.fori_loop(1, n, greet, 0)

    zrow = jnp.zeros((PAD, nx), jnp.float32)
    for p in range(1, depth + 2):
        z[p, 0:PAD, :] = zrow
        z[p, ny + PAD : ny + 2 * PAD, :] = zrow
    for p in range(1, depth + 1):
        y[p, 0:PAD, :] = zrow
        y[p, ny + PAD : ny + 2 * PAD, :] = zrow
    for p in range(depth):
        v[p, ny : ny + PAD, :] = zrow
    acc[...] = jnp.zeros_like(acc)

    def zero_planes(ref, planes, offset):
        def body(i, carry):
            for p in planes:
                ref[p, pl.ds(pl.multiple_of(i * ROWS + offset, 8), ROWS), :] = jnp.zeros((ROWS, nx), jnp.float32)
            return carry
        lax.fori_loop(0, nb, body, 0)

    ob_in.wait()
    pl.semaphore_wait(barrier, n - 1)

    ob_down = pltpu.make_async_remote_copy(
        ob.at[pl.ds(2, 1)], ob.at[pl.ds(depth + 2, 1)], ob_send.at[0], ob_recv.at[0], **at(low))
    ob_up = pltpu.make_async_remote_copy(
        ob.at[pl.ds(depth, 2)], ob.at[pl.ds(0, 2)], ob_send.at[1], ob_recv.at[1], **at(high))

    raw_part = pl.ds(0, raw_rows)
    raw_copies = [
        pltpu.make_async_remote_copy(
            src.at[0, raw_part], dst.at[0, raw_part], raw_send.at[j], raw_recv.at[j], **at(low))
        for j, (src, dst) in enumerate([(w, lw_next), (s, s_next)])
    ]

    @pl.when(has_low)
    def _():
        ob_down.start()

    @pl.when(has_high)
    def _():
        ob_up.start()

    @pl.when(jnp.logical_not(has_low))
    def _():
        ob[0:2] = jnp.zeros((2,) + ob.shape[1:], jnp.int32)
        zero_planes(z, (0, 1), PAD)

    @pl.when(jnp.logical_not(has_high))
    def _():
        ob[depth + 2 : depth + 3] = jnp.zeros((1,) + ob.shape[1:], jnp.int32)
        zero_planes(z, (depth + 2,), PAD)
        zero_planes(lw_next, (0,), 0)

    def largest(k, p, first, last, m):
        def body(i, m):
            a = jnp.abs(ins[k][1][p, pl.ds(pl.multiple_of(i * ROWS, 8), ROWS), :])
            return jnp.maximum(m, jnp.max(a.reshape(ROWS // 8, 8, nx), axis=0))
        return lax.fori_loop(first, last, body, m)

    peak = jnp.zeros((8, nx), jnp.float32)
    for k, p in scan:
        rest_in[k, p].wait()
        if k == 1:
            rest_in[3, p].start()
        peak = largest(k, p, raw_rows // ROWS if (k, p) == (2, 0) else 0, nb, peak)
    raw_in[0].wait()
    peak = largest(2, 0, 0, raw_rows // ROWS, peak)
    m = jnp.max(peak, axis=0, keepdims=True)
    part = m[:, 0:128]
    for c in range(128, nx, 128):
        part = jnp.maximum(part, m[:, c : c + 128])
    mx[...] = part

    def spread(src, dst, send, recv, step, count):
        def start(i, carry):
            pltpu.make_async_remote_copy(
                src, dst.at[i], send, recv, **at(lax.rem(me + step * i, n))).start()
            return carry

        everything = dst.at[pl.ds(1, count - 1)]
        whole = pltpu.make_async_remote_copy(everything, everything, send, recv, **at(lax.rem(me + step, n)))
        return (lambda: lax.fori_loop(1, count, start, 0)), whole

    mx_start, mx_whole = spread(mx, mx_all, mx_send, mx_recv, 1, n)
    mx_start()
    raw_in[1].wait()

    @pl.when(has_low)
    def _():
        for copy in raw_copies:
            copy.start()

    @pl.when(has_low)
    def _():
        ob_down.wait_send()
        ob_up.wait_recv()

    @pl.when(has_high)
    def _():
        ob_up.wait_send()
        ob_down.wait_recv()

    row_id = lax.broadcasted_iota(jnp.int32, (nb, nx), 0)
    col_id = lax.broadcasted_iota(jnp.int32, (nb, nx), 1)
    srl = lax.shift_right_logical
    c1, c31 = jnp.int32(1), jnp.int32(31)
    full1, full31 = jnp.full((nb, nx), c1), jnp.full((nb, nx), c31)
    for p in range(depth + 1):
        mid = ob[p + 1]
        after = jnp.where(row_id == nb - 1, 0, pltpu.roll(mid, nb - 1, 0))
        before = jnp.where(row_id == 0, 0, pltpu.roll(mid, 1, 0))
        a = srl(mid, full1) | (after << full31)
        b = (mid << full1) | srl(before, full31)
        c = jnp.where(col_id == nx - 1, 0, pltpu.roll(mid, nx - 1, 1))
        d = jnp.where(col_id == 0, 0, pltpu.roll(mid, 1, 1))
        e, f = ob[p], ob[p + 2]
        s1, k1 = a ^ b ^ c, (a & b) | (c & (a | b))
        s2, k2 = d ^ e ^ f, (d & e) | (f & (d | e))
        k3 = s1 & s2
        cw[p, 0] = s1 ^ s2
        cw[p, 1] = k1 ^ k2 ^ k3
        cw[p, 2] = (k1 & k2) | (k3 & (k1 | k2))
        cw[p, 3] = mid
    @pl.when(jnp.logical_not(has_low))
    def _():
        cw[0, 3] = jnp.full((nb, nx), -1, jnp.int32)

    half = 16
    places = lax.broadcasted_iota(jnp.int32, (half, nx), 0)

    def code_rows(b):
        for p in range(depth + 1):
            for k0 in range(0, ROWS, half):
                bits = [
                    srl(jnp.broadcast_to(cw[p, j, pl.ds(b, 1), :], (half, nx)), places + k0) & 1
                    for j in range(4)
                ]
                k = (6 - (bits[0] + (bits[1] << 1) + (bits[2] << 2))).astype(jnp.float32)
                rows = pl.ds(pl.multiple_of(b * ROWS + k0, 8), half)
                code[p, rows, :] = k
                inv[p, rows, :] = jnp.where(bits[3] == 1, 0.0, 1.0 / jnp.maximum(k, 1.0))

    for p in range(depth):
        rest_in[3, p].wait()

    def ready(b, carry):
        code_rows(b)
        return carry

    lax.fori_loop(0, nb // 4, ready, 0)
    mx_whole.wait_recv()
    mx_all[0] = mx[...]
    fastest = jnp.max(jnp.max(mx_all[...], axis=0), axis=1, keepdims=True)
    cf[0:1, :] = (CFL / (jnp.broadcast_to(fastest, (1, nx)) + EPS)) * BUOYANCY

    lane = lax.broadcasted_iota(jnp.int32, (ROWS, nx), 1)

    def lifted(p, r):
        rows = pl.ds(r, ROWS)
        return w[p, rows, :] + cf[0:1, :] * s[p, rows, :]

    def over(c, fn, rows=crow):
        def inner(i, k):
            fn(pl.multiple_of(c * rows + i * ROWS, 8))
            return k
        lax.fori_loop(0, rows // ROWS, inner, 0)

    def staged(first, second, count=chunks):
        def body(c, carry):
            @pl.when(c < count)
            def _():
                first(c)

            @pl.when(c > 0)
            def _():
                second(c - 1)
            return carry
        lax.fori_loop(0, count + 1, body, 0)

    def when(cond, fn):
        @pl.when(cond)
        def _():
            fn()

    class Flow:
        def __init__(self, src, dst, send, recv, device, per, src_pad=PAD, dst_pad=PAD, first=0):
            def copy(start, rows, index):
                def part(pad):
                    return pl.ds(pl.multiple_of(start + pad, 8), rows)
                return pltpu.make_async_remote_copy(
                    src[0].at[src[1], part(src_pad)], dst[0].at[dst[1], part(dst_pad)], send, recv.at[index], **at(device))

            self.start = lambda c: copy(c * crow, crow, c // per).start()
            self.wait_recv = lambda i: copy(i * crow * per, crow * per, i).wait_recv()
            self.start_rest = lambda: copy(first, crow - first % crow, first // crow // per).start()
            self.wait_rest = lambda: copy(first, grow - first, 0).wait_recv()
            self.wait_send = lambda: copy(first, ny - first, 0).wait_send()

            def aside(c, unit):
                return pl.ds(pl.multiple_of(unit * grow + lax.rem(c, group) * crow, 8), crow)

            def detour(c, unit, via):
                rows = pl.ds(pl.multiple_of(c * crow + src_pad, 8), crow)
                pltpu.make_async_remote_copy(
                    src[0].at[src[1], rows], relay.at[0, aside(c, unit)], send, relay_recv.at[unit // 2], **at(via)).start()

            def forward(c, unit):
                rows = pl.ds(pl.multiple_of(c * crow + dst_pad, 8), crow)
                pltpu.make_async_remote_copy(
                    relay.at[0, aside(c, unit)], dst[0].at[dst[1], rows], relay_send, recv.at[c // per],
                    **at(rl_target)).start()

            self.detour, self.forward = detour, forward

    lw_down = Flow((lw, 0), (lw_next, 0), send.at[0], lw_recv, low, group, 0, 0, raw_rows)
    z_down = Flow((z, 2), (z, depth + 2), send.at[1], dn_recv, low, group)
    y_down = Flow((y, 1), (y, depth + 1), send.at[2], yd_recv, low, group)
    top_up = Flow((part_z, 0), (z, 1), send.at[3], top_recv, high, group, 0)
    next_up = Flow((z, top + 1), (z, 0), send.at[4], next_recv, high, 1)

    def send_chunk(flow, second, c, first, last, via):
        unit = c // group + (head if second else head - plane_units)
        aside = jnp.logical_and(unit >= first, unit < last)
        when(aside, lambda: flow.detour(c, jnp.maximum(unit, 0), via))
        when(jnp.logical_not(aside), lambda: flow.start(c))

    def set_aside(first, count):
        part = relay.at[0, pl.ds(0, count * grow)]
        return pltpu.make_async_remote_copy(part, part, relay_send, relay_recv.at[first // 2], **at(rl_target))

    def forward_pair(cond, unit, second):
        def run(flow):
            set_aside(unit, 2).wait_recv()
            for i in range(2 * group):
                flow.forward((unit + (-head if second else plane_units - head)) * group + i, unit + i // group)

        inside = jnp.logical_and(cond, jnp.logical_and(unit >= rl_first, unit < rl_last))
        when(jnp.logical_and(inside, relays_up), lambda: run(next_up if second else top_up))
        when(jnp.logical_and(inside, relays_down), lambda: run(z_down if second else lw_down))

    def flat(p, r):
        a = u[p, pl.ds(r, ROWS), :]
        b = v[p, pl.ds(r, ROWS + PAD), :]
        return jnp.where(lane == nx - 1, 0.0, pltpu.roll(a, nx - 1, 1)) - a + (b[1 : ROWS + 1] - b[:ROWS])

    def inner_rows(r):
        return pl.ds(pl.multiple_of(r + PAD, 8), ROWS)

    def lw_rows(r):
        lw[0, pl.ds(r, ROWS), :] = lifted(0, r)

    def shifted(c):
        return lax.rem(c + raw_rows // crow, chunks)

    def lw_sends(c):
        when(jnp.logical_and(has_low, c * crow >= raw_rows),
             lambda: send_chunk(lw_down, False, c, dn_first, dn_last, dn_via))
        if raw_rows % crow:
            when(jnp.logical_and(has_low, c == raw_rows // crow), lw_down.start_rest)

    staged(lambda c: over(shifted(c), lw_rows), lambda c: lw_sends(shifted(c)))

    def first_rows(r):
        when(r >= ny // 4, lambda: code_rows(r // ROWS))
        rows = pl.ds(r, ROWS)
        part_z[0, rows, :] = inv[top + 1, rows, :] * (flat(top, r) - lifted(top, r))

    staged(lambda c: over(c, first_rows),
           lambda c: when(has_high, lambda: send_chunk(top_up, False, c, up_first, up_last, up_via)))

    def z_rows(p, r):
        rows = pl.ds(r, ROWS)
        own = lw[0, rows, :] if p == 0 else lifted(p, r)
        z[p + 2, inner_rows(r), :] = inv[p + 1, rows, :] * (flat(p, r) + (lifted(p + 1, r) - own))

    for p in range(top):
        def z_sends(c, p=p):
            if p == 0:
                when(has_low, lambda: send_chunk(z_down, True, c, dn_first, dn_last, dn_via))
            if p == top - 1:
                when(has_high, lambda: send_chunk(next_up, True, c, up_first, up_last, up_via))
        staged(lambda c, p=p: over(c, functools.partial(z_rows, p)), z_sends)

    @pl.when(has_high)
    def _():
        for copy in raw_copies:
            copy.wait_recv()

        def lift(i, carry):
            rows = pl.ds(pl.multiple_of(i * ROWS, 8), ROWS)
            lw_next[0, rows, :] = lw_next[0, rows, :] + cf[0:1, :] * s_next[0, rows, :]
            return carry

        lax.fori_loop(0, raw_rows // ROWS, lift, 0)

    def around(ref, slot, r):
        x = ref[slot, pl.ds(r, ROWS + 2 * PAD), :]
        mid = x[PAD : PAD + ROWS]
        beside = x[PAD + 1 : PAD + 1 + ROWS] + x[PAD - 1 : PAD - 1 + ROWS]
        beside = beside + jnp.where(lane == nx - 1, 0.0, pltpu.roll(mid, nx - 1, 1))
        beside = beside + jnp.where(lane == 0, 0.0, pltpu.roll(mid, 1, 1))
        return mid, beside

    def add(j, x):
        acc[j] += jnp.sum(x.reshape(ROWS // 8, 8, nx), axis=0)

    def y_rows(p, r):
        inner, rows = inner_rows(r), pl.ds(r, ROWS)
        k, scale = code[p + 1, rows, :], inv[p + 1, rows, :]
        mid, beside = around(z, p + 2, r)
        q = k * mid - (beside + z[p + 1, inner, :] + z[p + 3, inner, :])
        out = q * scale
        y[p + 1, inner, :] = out
        if p >= 0:
            d = jnp.maximum(k, 1.0) * mid
            add(0, d * mid)
            add(1, d * d)
            add(2, jnp.where(scale > 0.0, 1.0, 0.0))
            add(3, mid * q)
            add(4, q * out)

    def complete_rows(r):
        inner, rows = inner_rows(r), pl.ds(r, ROWS)
        z[top + 2, inner, :] = part_z[0, rows, :] + inv[top + 1, rows, :] * lw_next[0, rows, :]
        z[1, inner, :] = z[1, inner, :] + inv[0, rows, :] * lw[0, rows, :]

    def low_rows(r):
        complete_rows(r)
        for p in range(top):
            y_rows(p, r)

    def low_chunk(c):
        when(jnp.logical_and(has_high, c > 0), lambda: lw_down.wait_recv(c))
        if raw_rows < grow:
            when(jnp.logical_and(has_high, c == 0), lw_down.wait_rest)
        when(has_low, lambda: top_up.wait_recv(c))
        over(c, low_rows, grow)
        forward_pair(jnp.logical_and(near, c == groups - 1), every - few, True)
        forward_pair(jnp.logical_and(jnp.logical_not(near), lax.rem(c, 4) == 3), c // 4 * 2, False)

    def start_y(c):
        for i in range(group):
            y_down.start(c * group + i)

    staged(low_chunk, lambda c: when(jnp.logical_and(has_low, jnp.logical_not(gated)), lambda: start_y(c)), groups)

    def a_rows(p, r):
        inner, rows = inner_rows(r), pl.ds(r, ROWS)
        mid, beside = around(y, p + 1, r)
        below = y[p, inner, :]
        beside = beside + below
        if p < top:
            beside = beside + y[p + 2, inner, :]
        q = code[p + 1, rows, :] * mid - beside
        ay[p, rows, :] = jnp.where(inv[p + 1, rows, :] > 0.0, q, 0.0)
        add(5, mid * (q - below) if p == 0 else mid * q)

    def high_rows(r):
        y_rows(top, r)
        y_rows(-1, r)

    def high_chunk(c):
        when(has_high, lambda: z_down.wait_recv(c))
        for i in range(group):
            chunk = c * group + i
            when(has_low, lambda: next_up.wait_recv(chunk))

            @pl.when(jnp.logical_and(gating, chunk == chunks - LEAD))
            def _():
                pl.delay(LAG)
                pl.semaphore_signal(gate, inc=1, **at(jnp.minimum(me + SPAN - 2, n - 1)))

        @pl.when(jnp.logical_and(gated, c == OPEN))
        def _():
            pl.semaphore_wait(gate, 1)

            def start(i, carry):
                start_y(i)
                return carry

            lax.fori_loop(0, groups, start, 0)

        over(c, high_rows, grow)
        forward_pair(jnp.logical_and(jnp.logical_not(near), c < groups // 2), head + jnp.minimum(2 * c, groups - 2), True)

    def image_rows(r):
        for p in range(depth):
            a_rows(p, r)

    staged(high_chunk, lambda c: over(c, image_rows, grow), groups)

    lanes = lax.broadcasted_iota(jnp.int32, (1, 128), 1)
    sums = jnp.zeros((1, 128), jnp.float32)
    for j in range(6):
        t = jnp.sum(jnp.sum(acc[j], axis=0, keepdims=True), axis=1, keepdims=True)
        sums = jnp.where(lanes == j, jnp.broadcast_to(t, (1, 128)), sums)
    st[...] = sums

    pair_in = pltpu.make_async_remote_copy(st, st_pair, pair_send.at[0], pair_recv.at[0], **at(partner))
    pair_out = pltpu.make_async_remote_copy(total, total, pair_send.at[1], pair_recv.at[1], **at(partner))
    st_start, st_whole = spread(st_pair, st_all, st_send, st_recv, 2, n // 2)

    @pl.when(even)
    def _():
        pair_in.start()

    @pl.when(odd)
    def _():
        pair_in.wait_recv()
        st_pair[...] = st_pair[...] + st[...]
        st_start()
        st_whole.wait_recv()
        st_all[0] = st_pair[...]
        total[...] = jnp.sum(st_all[...], axis=0)
        pair_out.start()

    @pl.when(has_low)
    def _():
        for copy in raw_copies:
            copy.wait_send()

    @pl.when(even)
    def _():
        pair_in.wait_send()
        pair_out.wait_recv()

    def summed(j):
        t = jnp.sum(jnp.where(lanes == j, total[...], 0.0), axis=1, keepdims=True)
        return jnp.broadcast_to(t, (1, nx))

    gamma, squares, fluid, delta, eta, theta = (summed(j) for j in range(6))
    alpha = gamma / delta
    gamma_next = gamma - 2.0 * alpha * delta + alpha * alpha * eta
    beta = gamma_next / gamma
    mixed = delta - alpha * eta
    curve = (delta - 2.0 * alpha * eta + alpha * alpha * theta) + 2.0 * beta * mixed + beta * beta * delta
    alpha_next = gamma_next / curve
    norm = 1.0 / jnp.sqrt(squares / jnp.maximum(fluid, 1.0) + EPS)
    cf[1:2, :] = alpha + alpha_next * (1.0 + beta)
    cf[2:3, :] = alpha * alpha_next
    cf[3:4, :] = norm
    cf[4:5, :] = alpha * alpha_next * norm

    def out_rows(r):
        inner, rows = inner_rows(r), pl.ds(r, ROWS)
        a, b = cf[1:2, :], cf[2:3, :]
        for p in range(depth):
            zz, yy = z[p + 2, inner, :], y[p + 1, inner, :]
            w[p, rows, :] = a * zz - b * yy
            s[p, rows, :] = (
                jnp.maximum(code[p + 1, rows, :], 1.0) * (zz - a * yy) + b * ay[p, rows, :]) * cf[3:4, :]

    def all_rows(i, carry):
        out_rows(pl.multiple_of(i * ROWS, 8))
        return carry

    lax.fori_loop(0, nb, all_rows, 0)

    def last_rows(r):
        inner, rows = inner_rows(r), pl.ds(r, ROWS)
        s[top, rows, :] = s[top, rows, :] - jnp.where(
            inv[top + 1, rows, :] > 0.0, cf[4:5, :] * y[depth + 1, inner, :], 0.0)

    @pl.when(has_high)
    def _():
        def last_chunk(c, carry):
            y_down.wait_recv(c)
            over(c, last_rows, grow)
            return carry
        lax.fori_loop(0, groups, last_chunk, 0)

    @pl.when(odd)
    def _():
        st_whole.wait_send()
        pair_out.wait_send()

    @pl.when(has_low)
    def _():
        for flow in (lw_down, z_down, y_down):
            flow.wait_send()

    @pl.when(has_high)
    def _():
        for flow in (top_up, next_up):
            flow.wait_send()

    mx_whole.wait_send()

    for count in (few, head, 2 * head, every):
        when(rl_last - rl_first == count, lambda count=count: set_aside(0, count).wait_send())


def store(w, s, w_hbm, s_hbm, sem):
    copies = [
        pltpu.make_async_copy(src.at[p], dst.at[p], sem.at[j, p])
        for j, (src, dst) in enumerate([(w, w_hbm), (s, s_hbm)]) for p in range(w.shape[0])
    ]
    for copy in copies:
        copy.start()
    for copy in copies:
        copy.wait()


def solution(mesh):
    n = mesh.shape["gz"]

    def local(u_face, v_face, w_face, smoke, obstacles):
        depth, ny, nx = u_face.shape
        nw = obstacles.shape[1]
        chunks, group = 16, 2
        raw_rows = 3 * ny // 32
        f32, i32 = jnp.float32, jnp.int32
        dma = pltpu.SemaphoreType.DMA
        any_spec = pl.BlockSpec(memory_space=pl.ANY)
        vmem_spec = pl.BlockSpec(memory_space=pltpu.VMEM)
        shape = pltpu.VMEM((depth, ny, nx), f32)
        results = pl.pallas_call(
            functools.partial(kernel, n, chunks, group, raw_rows),
            out_shape=(shape, shape),
            in_specs=[any_spec] * 5,
            out_specs=(vmem_spec, vmem_spec),
            scratch_shapes=[
                pltpu.VMEM((depth, ny, nx), f32),
                pltpu.VMEM((depth, ny + PAD, nx), f32),
                pltpu.VMEM((depth + 3, ny + 2 * PAD, nx), f32),
                pltpu.VMEM((1, ny, nx), f32),
                pltpu.VMEM((depth + 2, ny + 2 * PAD, nx), f32),
                pltpu.VMEM((depth + 1, ny, nx), f32),
                pltpu.VMEM((depth + 1, ny, nx), f32),
                pltpu.VMEM((depth, ny, nx), f32),
                pltpu.VMEM((1, ny, nx), f32),
                pltpu.VMEM((1, ny, nx), f32),
                pltpu.VMEM((1, raw_rows, nx), f32),
                pltpu.VMEM((1, 3 * ny // 2, nx), f32),
                pltpu.VMEM((depth + 3, nw, nx), i32),
                pltpu.VMEM((depth + 1, 4, nw, nx), i32),
                pltpu.VMEM((6, 8, nx), f32),
                pltpu.VMEM((8, nx), f32),
                pltpu.VMEM((1, 128), f32),
                pltpu.VMEM((n, 1, 128), f32),
                pltpu.VMEM((1, 128), f32),
                pltpu.VMEM((1, 128), f32),
                pltpu.VMEM((n // 2, 1, 128), f32),
                pltpu.VMEM((1, 128), f32),
                dma((4 * depth + 3,)),
                dma((2,)), dma((2,)),
                dma((2,)), dma((2,)),
                dma((5,)),
                dma((chunks // group,)), dma((chunks // group,)), dma((chunks // group,)), dma((chunks // group,)),
                dma((chunks,)),
                dma((3 * chunks // group // 4,)), dma,
                dma, dma, dma, dma,
                dma((2,)), dma((2,)),
                pltpu.SemaphoreType.REGULAR,
            ],
            compiler_params=pltpu.CompilerParams(
                collective_id=0, has_side_effects=True, vmem_limit_bytes=58_000_000),
            name="smoke_step",
        )(u_face, v_face, w_face, smoke, obstacles)
        out = jax.ShapeDtypeStruct((depth, ny, nx), f32)
        return pl.pallas_call(
            store,
            out_shape=(out, out),
            in_specs=[vmem_spec] * 2,
            out_specs=(any_spec, any_spec),
            scratch_shapes=[dma((2, depth))],
            compiler_params=pltpu.CompilerParams(vmem_limit_bytes=1_000_000),
            name="store",
        )(*results)

    placed = P("gz", None, None)
    return jax.shard_map(local, mesh=mesh, in_specs=(placed,) * 5, out_specs=(placed, placed), check_vma=False)
```

```python
import functools

import jax
import jax.numpy as jnp
from jax import lax
from jax.experimental import pallas as pl
from jax.experimental.pallas import tpu as pltpu
from jax.sharding import PartitionSpec as P

EPS = 1e-06
CFL = 0.5
BUOYANCY = 100.0

ROWS = 32
PAD = 8
SPAN = 8
LEAD = 4
LAG = 700
OPEN = 5


def kernel(n, chunks, group, raw_rows, u_hbm, v_hbm, w_hbm, s_hbm, ob_hbm, w, s,
           u, v, z, part_z, y, code, inv, ay, lw, lw_next, s_next, relay, ob, cw, acc, cf, mx, mx_all, st, st_pair, st_all, total,
           in_sem, ob_send, ob_recv, raw_send, raw_recv, send, lw_recv, dn_recv, yd_recv, top_recv, next_recv, relay_recv, relay_send,
           mx_send, mx_recv, st_send, st_recv, pair_send, pair_recv, gate):
    depth, ny, nx = w.shape
    top = depth - 1
    nb = ny // ROWS
    crow = ny // chunks
    grow = crow * group
    groups = chunks // group
    me = lax.axis_index("gz")
    has_low, has_high = me > 0, me < n - 1
    low, high = jnp.maximum(me - 1, 0), jnp.minimum(me + 1, n - 1)
    odd = lax.rem(me, 2) == 1
    even = jnp.logical_not(odd)
    partner = me + 1 - 2 * lax.rem(me, 2)
    place = lax.rem(me, SPAN)
    gated = jnp.logical_and(has_low, place == 0)
    gating = jnp.logical_and(place == 2, me + SPAN - 2 < n)

    span, spans = me // SPAN, n // SPAN
    plane_units = groups
    head = plane_units // 2
    few = plane_units // 4
    every = head + plane_units

    def piece(count):
        return head - jnp.maximum(count - plane_units, 0), head + jnp.minimum(count, plane_units)

    def select(cases):
        first, last = 0, 0
        for cond, (lo, hi) in cases:
            first, last = jnp.where(cond, lo, first), jnp.where(cond, hi, last)
        return first, last

    def cross_up(lower):
        return piece(jnp.minimum(head * (spans - 1 - lower), every))

    def cross_down(upper):
        return piece(jnp.minimum(head * upper, every))

    side = (every - few, every)
    whole_spans = n % SPAN == 0
    crossing = jnp.logical_and(whole_spans, span + 1 < spans)
    crossed = jnp.logical_and(whole_spans, span > 0)
    up_first, up_last = select([(jnp.logical_and(whole_spans, place == 3), side), (jnp.logical_and(crossing, place == 7), cross_up(span))])
    dn_first, dn_last = select([(jnp.logical_and(whole_spans, place == 4), side), (jnp.logical_and(crossed, place == 0), cross_down(span))])
    up_via = jnp.clip(jnp.where(place == 3, me + 4, me - 2), 0, n - 1)
    dn_via = jnp.clip(jnp.where(place == 4, me - 4, me + 3), 0, n - 1)
    relays_up = jnp.logical_and(whole_spans, jnp.logical_or(place == 7, jnp.logical_and(place == 5, crossing)))
    relays_down = jnp.logical_and(whole_spans, jnp.logical_or(place == 0, jnp.logical_and(place == 3, crossed)))
    near = jnp.logical_or(place == 7, place == 0)
    rl_first, rl_last = select([
        (jnp.logical_and(whole_spans, near), side),
        (jnp.logical_and(crossing, place == 5), cross_up(span)),
        (jnp.logical_and(crossed, place == 3), cross_down(span)),
    ])
    rl_target = jnp.clip(
        jnp.where(place == 7, me - 3, jnp.where(place == 5, me + 3, jnp.where(place == 0, me + 3, me - 4))), 0, n - 1)

    def at(device):
        return dict(device_id=(device,), device_id_type=pl.DeviceIdType.MESH)

    ins = [(u_hbm, u), (v_hbm, v), (w_hbm, w), (s_hbm, s)]

    def load(k, p, first=0, rows=ny, sem=None):
        src, dst = ins[k]
        part = pl.ds(first, rows)
        return pltpu.make_async_copy(src.at[p, part], dst.at[p, part], in_sem.at[k * depth + p if sem is None else sem])

    ob_in = pltpu.make_async_copy(ob_hbm, ob.at[pl.ds(2, depth)], in_sem.at[4 * depth])
    raw_in = [load(k, 0, 0, raw_rows, 4 * depth + k - 1) for k in (2, 3)]
    rest_in = {(k, p): load(k, p, raw_rows, ny - raw_rows) if k >= 2 and p == 0 else load(k, p)
               for k in range(4) for p in range(depth)}
    scan = [(k, p) for k in range(3) for p in range(depth - 1, -1, -1)]
    ob_in.start()
    for pair in scan:
        rest_in[pair].start()
    for copy in raw_in:
        copy.start()

    barrier = pltpu.get_barrier_semaphore()

    def greet(i, carry):
        pl.semaphore_signal(barrier, inc=1, **at(lax.rem(me + i, n)))
        return carry

    lax.fori_loop(1, n, greet, 0)

    zrow = jnp.zeros((PAD, nx), jnp.float32)
    for p in range(1, depth + 2):
        z[p, 0:PAD, :] = zrow
        z[p, ny + PAD : ny + 2 * PAD, :] = zrow
    for p in range(1, depth + 1):
        y[p, 0:PAD, :] = zrow
        y[p, ny + PAD : ny + 2 * PAD, :] = zrow
    for p in range(depth):
        v[p, ny : ny + PAD, :] = zrow
    acc[...] = jnp.zeros_like(acc)

    def zero_planes(ref, planes, offset):
        def body(i, carry):
            for p in planes:
                ref[p, pl.ds(pl.multiple_of(i * ROWS + offset, 8), ROWS), :] = jnp.zeros((ROWS, nx), jnp.float32)
            return carry
        lax.fori_loop(0, nb, body, 0)

    ob_in.wait()
    pl.semaphore_wait(barrier, n - 1)

    ob_down = pltpu.make_async_remote_copy(
        ob.at[pl.ds(2, 1)], ob.at[pl.ds(depth + 2, 1)], ob_send.at[0], ob_recv.at[0], **at(low))
    ob_up = pltpu.make_async_remote_copy(
        ob.at[pl.ds(depth, 2)], ob.at[pl.ds(0, 2)], ob_send.at[1], ob_recv.at[1], **at(high))

    raw_part = pl.ds(0, raw_rows)
    raw_copies = [
        pltpu.make_async_remote_copy(
            src.at[0, raw_part], dst.at[0, raw_part], raw_send, raw_recv, **at(low))
        for src, dst in [(w, lw_next), (s, s_next)]
    ]
    both = lw_next.at[0, pl.ds(0, 2 * raw_rows)]
    raw_whole = pltpu.make_async_remote_copy(both, both, raw_send, raw_recv, **at(low))

    @pl.when(has_low)
    def _():
        ob_down.start()

    @pl.when(has_high)
    def _():
        ob_up.start()

    @pl.when(jnp.logical_not(has_low))
    def _():
        ob[0:2] = jnp.zeros((2,) + ob.shape[1:], jnp.int32)
        zero_planes(z, (0, 1), PAD)

    @pl.when(jnp.logical_not(has_high))
    def _():
        ob[depth + 2 : depth + 3] = jnp.zeros((1,) + ob.shape[1:], jnp.int32)
        zero_planes(z, (depth + 2,), PAD)
        zero_planes(lw_next, (0,), 0)

    def largest(k, p, first, last, m):
        def body(i, m):
            a = jnp.abs(ins[k][1][p, pl.ds(pl.multiple_of(i * ROWS, 8), ROWS), :])
            return jnp.maximum(m, jnp.max(a.reshape(ROWS // 8, 8, nx), axis=0))
        return lax.fori_loop(first, last, body, m)

    peak = jnp.zeros((8, nx), jnp.float32)
    for k, p in scan:
        rest_in[k, p].wait()
        if k == 1:
            rest_in[3, p].start()
        peak = largest(k, p, raw_rows // ROWS if (k, p) == (2, 0) else 0, nb, peak)
    raw_in[0].wait()
    peak = largest(2, 0, 0, raw_rows // ROWS, peak)
    m = jnp.max(peak, axis=0, keepdims=True)
    part = m[:, 0:128]
    for c in range(128, nx, 128):
        part = jnp.maximum(part, m[:, c : c + 128])
    mx[...] = part

    def spread(src, dst, send, recv, step, count):
        def start(i, carry):
            pltpu.make_async_remote_copy(
                src, dst.at[i], send, recv, **at(lax.rem(me + step * i, n))).start()
            return carry

        everything = dst.at[pl.ds(1, count - 1)]
        whole = pltpu.make_async_remote_copy(everything, everything, send, recv, **at(lax.rem(me + step, n)))
        return (lambda: lax.fori_loop(1, count, start, 0)), whole

    mx_start, mx_whole = spread(mx, mx_all, mx_send, mx_recv, 1, n)
    mx_start()
    raw_in[1].wait()

    @pl.when(has_low)
    def _():
        for copy in raw_copies:
            copy.start()

    @pl.when(has_low)
    def _():
        ob_down.wait_send()
        ob_up.wait_recv()

    @pl.when(has_high)
    def _():
        ob_up.wait_send()
        ob_down.wait_recv()

    row_id = lax.broadcasted_iota(jnp.int32, (nb, nx), 0)
    col_id = lax.broadcasted_iota(jnp.int32, (nb, nx), 1)
    srl = lax.shift_right_logical
    c1, c31 = jnp.int32(1), jnp.int32(31)
    full1, full31 = jnp.full((nb, nx), c1), jnp.full((nb, nx), c31)
    for p in range(depth + 1):
        mid = ob[p + 1]
        after = jnp.where(row_id == nb - 1, 0, pltpu.roll(mid, nb - 1, 0))
        before = jnp.where(row_id == 0, 0, pltpu.roll(mid, 1, 0))
        a = srl(mid, full1) | (after << full31)
        b = (mid << full1) | srl(before, full31)
        c = jnp.where(col_id == nx - 1, 0, pltpu.roll(mid, nx - 1, 1))
        d = jnp.where(col_id == 0, 0, pltpu.roll(mid, 1, 1))
        e, f = ob[p], ob[p + 2]
        s1, k1 = a ^ b ^ c, (a & b) | (c & (a | b))
        s2, k2 = d ^ e ^ f, (d & e) | (f & (d | e))
        k3 = s1 & s2
        cw[p, 0] = s1 ^ s2
        cw[p, 1] = k1 ^ k2 ^ k3
        cw[p, 2] = (k1 & k2) | (k3 & (k1 | k2))
        cw[p, 3] = mid
    @pl.when(jnp.logical_not(has_low))
    def _():
        cw[0, 3] = jnp.full((nb, nx), -1, jnp.int32)

    half = 16
    places = lax.broadcasted_iota(jnp.int32, (half, nx), 0)

    def code_rows(b):
        for p in range(depth + 1):
            for k0 in range(0, ROWS, half):
                bits = [
                    srl(jnp.broadcast_to(cw[p, j, pl.ds(b, 1), :], (half, nx)), places + k0) & 1
                    for j in range(4)
                ]
                k = (6 - (bits[0] + (bits[1] << 1) + (bits[2] << 2))).astype(jnp.float32)
                rows = pl.ds(pl.multiple_of(b * ROWS + k0, 8), half)
                code[p, rows, :] = k
                inv[p, rows, :] = jnp.where(bits[3] == 1, 0.0, 1.0 / jnp.maximum(k, 1.0))

    for p in range(depth):
        rest_in[3, p].wait()

    def ready(b, carry):
        code_rows(b)
        return carry

    lax.fori_loop(0, nb // 4, ready, 0)
    mx_whole.wait_recv()
    mx_all[0] = mx[...]
    fastest = jnp.max(jnp.max(mx_all[...], axis=0), axis=1, keepdims=True)
    cf[0:1, :] = (CFL / (jnp.broadcast_to(fastest, (1, nx)) + EPS)) * BUOYANCY

    lane = lax.broadcasted_iota(jnp.int32, (ROWS, nx), 1)

    def lifted(p, r):
        rows = pl.ds(r, ROWS)
        return w[p, rows, :] + cf[0:1, :] * s[p, rows, :]

    def over(c, fn, rows=crow):
        def inner(i, k):
            fn(pl.multiple_of(c * rows + i * ROWS, 8))
            return k
        lax.fori_loop(0, rows // ROWS, inner, 0)

    def staged(first, second, count=chunks):
        def body(c, carry):
            @pl.when(c < count)
            def _():
                first(c)

            @pl.when(c > 0)
            def _():
                second(c - 1)
            return carry
        lax.fori_loop(0, count + 1, body, 0)

    def when(cond, fn):
        @pl.when(cond)
        def _():
            fn()

    class Flow:
        def __init__(self, src, dst, send, recv, device, per, src_pad=PAD, dst_pad=PAD, first=0):
            def copy(start, rows, index):
                def part(pad):
                    return pl.ds(pl.multiple_of(start + pad, 8), rows)
                return pltpu.make_async_remote_copy(
                    src[0].at[src[1], part(src_pad)], dst[0].at[dst[1], part(dst_pad)], send, recv.at[index], **at(device))

            self.start = lambda c: copy(c * crow, crow, c // per).start()
            self.wait_recv = lambda i: copy(i * crow * per, crow * per, i).wait_recv()
            self.start_rest = lambda: copy(first, crow - first % crow, first // crow // per).start()
            self.wait_rest = lambda: copy(first, grow - first, 0).wait_recv()

            def aside(c, unit):
                return pl.ds(pl.multiple_of(unit * grow + lax.rem(c, group) * crow, 8), crow)

            def detour(c, unit, via):
                rows = pl.ds(pl.multiple_of(c * crow + src_pad, 8), crow)
                pltpu.make_async_remote_copy(
                    src[0].at[src[1], rows], relay.at[0, aside(c, unit)], send, relay_recv.at[unit // 2], **at(via)).start()

            def forward(c, unit):
                rows = pl.ds(pl.multiple_of(c * crow + dst_pad, 8), crow)
                pltpu.make_async_remote_copy(
                    relay.at[0, aside(c, unit)], dst[0].at[dst[1], rows], relay_send, recv.at[c // per],
                    **at(rl_target)).start()

            self.detour, self.forward = detour, forward

    lw_down = Flow((lw, 0), (lw_next, 0), send.at[0], lw_recv, low, group, 0, 0, raw_rows)
    z_down = Flow((z, 2), (z, depth + 2), send.at[0], dn_recv, low, group)
    y_down = Flow((y, 1), (y, depth + 1), send.at[0], yd_recv, low, 2 * group)
    top_up = Flow((part_z, 0), (z, 1), send.at[1], top_recv, high, group, 0)
    next_up = Flow((z, top + 1), (z, 0), send.at[1], next_recv, high, 1)

    def send_chunk(flow, second, c, first, last, via):
        unit = c // group + (head if second else head - plane_units)
        aside = jnp.logical_and(unit >= first, unit < last)
        when(aside, lambda: flow.detour(c, jnp.maximum(unit, 0), via))
        when(jnp.logical_not(aside), lambda: flow.start(c))

    def set_aside(first, count):
        part = relay.at[0, pl.ds(0, count * grow)]
        return pltpu.make_async_remote_copy(part, part, relay_send, relay_recv.at[first // 2], **at(rl_target))

    def forward_pair(cond, unit, second):
        def run(flow):
            set_aside(unit, 2).wait_recv()
            for i in range(2 * group):
                flow.forward((unit + (-head if second else plane_units - head)) * group + i, unit + i // group)

        inside = jnp.logical_and(cond, jnp.logical_and(unit >= rl_first, unit < rl_last))
        when(jnp.logical_and(inside, relays_up), lambda: run(next_up if second else top_up))
        when(jnp.logical_and(inside, relays_down), lambda: run(z_down if second else lw_down))

    def flat(p, r):
        a = u[p, pl.ds(r, ROWS), :]
        b = v[p, pl.ds(r, ROWS + PAD), :]
        return jnp.where(lane == nx - 1, 0.0, pltpu.roll(a, nx - 1, 1)) - a + (b[1 : ROWS + 1] - b[:ROWS])

    def inner_rows(r):
        return pl.ds(pl.multiple_of(r + PAD, 8), ROWS)

    def lw_rows(r):
        lw[0, pl.ds(r, ROWS), :] = lifted(0, r)

    def shifted(c):
        return lax.rem(c + raw_rows // crow, chunks)

    def lw_sends(c):
        when(jnp.logical_and(has_low, c * crow >= raw_rows),
             lambda: send_chunk(lw_down, False, c, dn_first, dn_last, dn_via))
        if raw_rows % crow:
            when(jnp.logical_and(has_low, c == raw_rows // crow), lw_down.start_rest)

    staged(lambda c: over(shifted(c), lw_rows), lambda c: lw_sends(shifted(c)))

    def first_rows(r):
        when(r >= ny // 4, lambda: code_rows(r // ROWS))
        rows = pl.ds(r, ROWS)
        part_z[0, rows, :] = inv[top + 1, rows, :] * (flat(top, r) - lifted(top, r))

    staged(lambda c: over(c, first_rows),
           lambda c: when(has_high, lambda: send_chunk(top_up, False, c, up_first, up_last, up_via)))

    def z_rows(p, r):
        rows = pl.ds(r, ROWS)
        own = lw[0, rows, :] if p == 0 else lifted(p, r)
        z[p + 2, inner_rows(r), :] = inv[p + 1, rows, :] * (flat(p, r) + (lifted(p + 1, r) - own))

    for p in range(top):
        def z_sends(c, p=p):
            if p == 0:
                when(has_low, lambda: send_chunk(z_down, True, c, dn_first, dn_last, dn_via))
            if p == top - 1:
                when(has_high, lambda: send_chunk(next_up, True, c, up_first, up_last, up_via))
        staged(lambda c, p=p: over(c, functools.partial(z_rows, p)), z_sends)

    @pl.when(has_high)
    def _():
        raw_whole.wait_recv()

        def lift(i, carry):
            rows = pl.ds(pl.multiple_of(i * ROWS, 8), ROWS)
            lw_next[0, rows, :] = lw_next[0, rows, :] + cf[0:1, :] * s_next[0, rows, :]
            return carry

        lax.fori_loop(0, raw_rows // ROWS, lift, 0)

    def around(ref, slot, r):
        x = ref[slot, pl.ds(r, ROWS + 2 * PAD), :]
        mid = x[PAD : PAD + ROWS]
        beside = x[PAD + 1 : PAD + 1 + ROWS] + x[PAD - 1 : PAD - 1 + ROWS]
        beside = beside + jnp.where(lane == nx - 1, 0.0, pltpu.roll(mid, nx - 1, 1))
        beside = beside + jnp.where(lane == 0, 0.0, pltpu.roll(mid, 1, 1))
        return mid, beside

    def add(j, x):
        acc[j] += jnp.sum(x.reshape(ROWS // 8, 8, nx), axis=0)

    def y_rows(p, r):
        inner, rows = inner_rows(r), pl.ds(r, ROWS)
        k, scale = code[p + 1, rows, :], inv[p + 1, rows, :]
        mid, beside = around(z, p + 2, r)
        q = k * mid - (beside + z[p + 1, inner, :] + z[p + 3, inner, :])
        out = q * scale
        y[p + 1, inner, :] = out
        if p >= 0:
            d = jnp.maximum(k, 1.0) * mid
            add(0, d * mid)
            add(1, d * d)
            add(2, jnp.where(scale > 0.0, 1.0, 0.0))
            add(3, mid * q)
            add(4, q * out)

    def complete_rows(r):
        inner, rows = inner_rows(r), pl.ds(r, ROWS)
        z[top + 2, inner, :] = part_z[0, rows, :] + inv[top + 1, rows, :] * lw_next[0, rows, :]
        z[1, inner, :] = z[1, inner, :] + inv[0, rows, :] * lw[0, rows, :]

    def low_rows(r):
        complete_rows(r)
        for p in range(top):
            y_rows(p, r)

    def low_chunk(c):
        when(jnp.logical_and(has_high, c > 0), lambda: lw_down.wait_recv(c))
        if raw_rows < grow:
            when(jnp.logical_and(has_high, c == 0), lw_down.wait_rest)
        when(has_low, lambda: top_up.wait_recv(c))
        over(c, low_rows, grow)
        forward_pair(jnp.logical_and(near, c == groups - 1), every - few, True)
        forward_pair(jnp.logical_and(jnp.logical_not(near), lax.rem(c, 4) == 3), c // 4 * 2, False)

    def start_y(c):
        for i in range(group):
            y_down.start(c * group + i)

    staged(low_chunk, lambda c: when(jnp.logical_and(has_low, jnp.logical_not(gated)), lambda: start_y(c)), groups)

    def a_rows(p, r):
        inner, rows = inner_rows(r), pl.ds(r, ROWS)
        mid, beside = around(y, p + 1, r)
        below = y[p, inner, :]
        beside = beside + below
        if p < top:
            beside = beside + y[p + 2, inner, :]
        q = code[p + 1, rows, :] * mid - beside
        ay[p, rows, :] = jnp.where(inv[p + 1, rows, :] > 0.0, q, 0.0)
        add(5, mid * (q - below) if p == 0 else mid * q)

    def high_rows(r):
        y_rows(top, r)
        y_rows(-1, r)

    def high_chunk(c):
        when(has_high, lambda: z_down.wait_recv(c))
        for i in range(group):
            chunk = c * group + i
            when(has_low, lambda: next_up.wait_recv(chunk))

            @pl.when(jnp.logical_and(gating, chunk == chunks - LEAD))
            def _():
                pl.delay(LAG)
                pl.semaphore_signal(gate, inc=1, **at(jnp.minimum(me + SPAN - 2, n - 1)))

        @pl.when(jnp.logical_and(gated, c == OPEN))
        def _():
            pl.semaphore_wait(gate, 1)

            def start(i, carry):
                start_y(i)
                return carry

            lax.fori_loop(0, groups, start, 0)

        over(c, high_rows, grow)
        forward_pair(jnp.logical_and(jnp.logical_not(near), c < groups // 2), head + jnp.minimum(2 * c, groups - 2), True)

    def image_rows(r):
        for p in range(depth):
            a_rows(p, r)

    staged(high_chunk, lambda c: over(c, image_rows, grow), groups)

    lanes = lax.broadcasted_iota(jnp.int32, (1, 128), 1)
    sums = jnp.zeros((1, 128), jnp.float32)
    for j in range(6):
        t = jnp.sum(jnp.sum(acc[j], axis=0, keepdims=True), axis=1, keepdims=True)
        sums = jnp.where(lanes == j, jnp.broadcast_to(t, (1, 128)), sums)
    st[...] = sums

    pair_in = pltpu.make_async_remote_copy(st, st_pair, pair_send, pair_recv, **at(partner))
    pair_out = pltpu.make_async_remote_copy(total, total, pair_send, pair_recv, **at(partner))
    st_start, st_whole = spread(st_pair, st_all, st_send, st_recv, 2, n // 2)

    @pl.when(even)
    def _():
        pair_in.start()

    @pl.when(odd)
    def _():
        pair_in.wait_recv()
        st_pair[...] = st_pair[...] + st[...]
        st_start()
        st_whole.wait_recv()
        st_all[0] = st_pair[...]
        total[...] = jnp.sum(st_all[...], axis=0)
        pair_out.start()

    @pl.when(has_low)
    def _():
        raw_whole.wait_send()

    @pl.when(even)
    def _():
        pair_in.wait_send()
        pair_out.wait_recv()

    def summed(j):
        t = jnp.sum(jnp.where(lanes == j, total[...], 0.0), axis=1, keepdims=True)
        return jnp.broadcast_to(t, (1, nx))

    gamma, squares, fluid, delta, eta, theta = (summed(j) for j in range(6))
    alpha = gamma / delta
    gamma_next = gamma - 2.0 * alpha * delta + alpha * alpha * eta
    beta = gamma_next / gamma
    mixed = delta - alpha * eta
    curve = (delta - 2.0 * alpha * eta + alpha * alpha * theta) + 2.0 * beta * mixed + beta * beta * delta
    alpha_next = gamma_next / curve
    norm = 1.0 / jnp.sqrt(squares / jnp.maximum(fluid, 1.0) + EPS)
    cf[1:2, :] = alpha + alpha_next * (1.0 + beta)
    cf[2:3, :] = alpha * alpha_next
    cf[3:4, :] = norm
    cf[4:5, :] = alpha * alpha_next * norm

    def out_rows(r):
        inner, rows = inner_rows(r), pl.ds(r, ROWS)
        a, b = cf[1:2, :], cf[2:3, :]
        for p in range(depth):
            zz, yy = z[p + 2, inner, :], y[p + 1, inner, :]
            w[p, rows, :] = a * zz - b * yy
            s[p, rows, :] = (
                jnp.maximum(code[p + 1, rows, :], 1.0) * (zz - a * yy) + b * ay[p, rows, :]) * cf[3:4, :]

    def all_rows(i, carry):
        out_rows(pl.multiple_of(i * ROWS, 8))
        return carry

    lax.fori_loop(0, nb, all_rows, 0)

    def last_rows(r):
        inner, rows = inner_rows(r), pl.ds(r, ROWS)
        s[top, rows, :] = s[top, rows, :] - jnp.where(
            inv[top + 1, rows, :] > 0.0, cf[4:5, :] * y[depth + 1, inner, :], 0.0)

    @pl.when(has_high)
    def _():
        def last_chunk(c, carry):
            when(lax.rem(c, 2) == 0, lambda: y_down.wait_recv(c // 2))
            over(c, last_rows, grow)
            return carry
        lax.fori_loop(0, groups, last_chunk, 0)

    @pl.when(odd)
    def _():
        st_whole.wait_send()
        pair_out.wait_send()

    def all_sent(index, planes, rows):
        part = code.at[pl.ds(0, planes), pl.ds(0, rows)]
        pltpu.make_async_remote_copy(part, part, send.at[index], lw_recv.at[0], **at(low)).wait_send()

    when(has_low, lambda: all_sent(0, 3, ny - raw_rows // 3))
    when(has_high, lambda: all_sent(1, 2, ny))

    mx_whole.wait_send()

    for count in (few, head, 2 * head, every):
        when(rl_last - rl_first == count, lambda count=count: set_aside(0, count).wait_send())


def store(w, s, w_hbm, s_hbm, sem):
    copies = [
        pltpu.make_async_copy(src.at[p], dst.at[p], sem.at[j, p])
        for j, (src, dst) in enumerate([(w, w_hbm), (s, s_hbm)]) for p in range(w.shape[0])
    ]
    for copy in copies:
        copy.start()
    for copy in copies:
        copy.wait()


def solution(mesh):
    n = mesh.shape["gz"]

    def local(u_face, v_face, w_face, smoke, obstacles):
        depth, ny, nx = u_face.shape
        nw = obstacles.shape[1]
        chunks, group = 16, 2
        raw_rows = 3 * ny // 32
        f32, i32 = jnp.float32, jnp.int32
        dma = pltpu.SemaphoreType.DMA
        any_spec = pl.BlockSpec(memory_space=pl.ANY)
        vmem_spec = pl.BlockSpec(memory_space=pltpu.VMEM)
        shape = pltpu.VMEM((depth, ny, nx), f32)
        results = pl.pallas_call(
            functools.partial(kernel, n, chunks, group, raw_rows),
            out_shape=(shape, shape),
            in_specs=[any_spec] * 5,
            out_specs=(vmem_spec, vmem_spec),
            scratch_shapes=[
                pltpu.VMEM((depth, ny, nx), f32),
                pltpu.VMEM((depth, ny + PAD, nx), f32),
                pltpu.VMEM((depth + 3, ny + 2 * PAD, nx), f32),
                pltpu.VMEM((1, ny, nx), f32),
                pltpu.VMEM((depth + 2, ny + 2 * PAD, nx), f32),
                pltpu.VMEM((depth + 1, ny, nx), f32),
                pltpu.VMEM((depth + 1, ny, nx), f32),
                pltpu.VMEM((depth, ny, nx), f32),
                pltpu.VMEM((1, ny, nx), f32),
                pltpu.VMEM((1, ny, nx), f32),
                pltpu.VMEM((1, raw_rows, nx), f32),
                pltpu.VMEM((1, 3 * ny // 2, nx), f32),
                pltpu.VMEM((depth + 3, nw, nx), i32),
                pltpu.VMEM((depth + 1, 4, nw, nx), i32),
                pltpu.VMEM((6, 8, nx), f32),
                pltpu.VMEM((8, nx), f32),
                pltpu.VMEM((1, 128), f32),
                pltpu.VMEM((n, 1, 128), f32),
                pltpu.VMEM((1, 128), f32),
                pltpu.VMEM((1, 128), f32),
                pltpu.VMEM((n // 2, 1, 128), f32),
                pltpu.VMEM((1, 128), f32),
                dma((4 * depth + 3,)),
                dma((2,)), dma((2,)),
                dma, dma,
                dma((2,)),
                dma((chunks // group,)), dma((chunks // group,)), dma((chunks // group // 2,)), dma((chunks // group,)),
                dma((chunks,)),
                dma((3 * chunks // group // 4,)), dma,
                dma, dma, dma, dma,
                dma, dma,
                pltpu.SemaphoreType.REGULAR,
            ],
            compiler_params=pltpu.CompilerParams(
                collective_id=0, has_side_effects=True, vmem_limit_bytes=58_000_000),
            name="smoke_step",
        )(u_face, v_face, w_face, smoke, obstacles)
        out = jax.ShapeDtypeStruct((depth, ny, nx), f32)
        return pl.pallas_call(
            store,
            out_shape=(out, out),
            in_specs=[vmem_spec] * 2,
            out_specs=(any_spec, any_spec),
            scratch_shapes=[dma((2, depth))],
            compiler_params=pltpu.CompilerParams(vmem_limit_bytes=1_000_000),
            name="store",
        )(*results)

    placed = P("gz", None, None)
    return jax.shard_map(local, mesh=mesh, in_specs=(placed,) * 5, out_specs=(placed, placed), check_vma=False)
```

```python
import functools

import jax
import jax.numpy as jnp
from jax import lax
from jax.experimental import pallas as pl
from jax.experimental.pallas import tpu as pltpu
from jax.sharding import PartitionSpec as P

EPS = 1e-06
CFL = 0.5
BUOYANCY = 100.0

ROWS = 32
PAD = 8
SPAN = 8
LEAD = 4
LAG = 700
OPEN = 6


def kernel(n, chunks, group, raw_rows, u_hbm, v_hbm, w_hbm, s_hbm, ob_hbm, w, s,
           u, v, z, part_z, y, code, inv, ay, lw, lw_next, s_next, relay, ob, cw, acc, cf, mx, mx_all, st, st_pair, st_all, total,
           in_sem, ob_send, ob_recv, raw_send, raw_recv, send, lw_recv, dn_recv, yd_recv, top_recv, next_recv, relay_recv, relay_send,
           mx_send, mx_recv, st_send, st_recv, pair_send, pair_recv, gate):
    depth, ny, nx = w.shape
    top = depth - 1
    nb = ny // ROWS
    crow = ny // chunks
    grow = crow * group
    groups = chunks // group
    me = lax.axis_index("gz")
    has_low, has_high = me > 0, me < n - 1
    low, high = jnp.maximum(me - 1, 0), jnp.minimum(me + 1, n - 1)
    odd = lax.rem(me, 2) == 1
    even = jnp.logical_not(odd)
    partner = me + 1 - 2 * lax.rem(me, 2)
    place = lax.rem(me, SPAN)
    gated = jnp.logical_and(has_low, place == 0)
    gating = jnp.logical_and(place == 2, me + SPAN - 2 < n)

    span, spans = me // SPAN, n // SPAN
    plane_units = groups
    head = plane_units // 2
    few = plane_units // 4
    every = head + plane_units

    def piece(count):
        return head - jnp.maximum(count - plane_units, 0), head + jnp.minimum(count, plane_units)

    def select(cases):
        first, last = 0, 0
        for cond, (lo, hi) in cases:
            first, last = jnp.where(cond, lo, first), jnp.where(cond, hi, last)
        return first, last

    def cross_up(lower):
        return piece(jnp.minimum(head * (spans - 1 - lower), every))

    def cross_down(upper):
        return piece(jnp.minimum(head * upper, every))

    side = (every - few, every)
    whole_spans = n % SPAN == 0
    crossing = jnp.logical_and(whole_spans, span + 1 < spans)
    crossed = jnp.logical_and(whole_spans, span > 0)
    up_first, up_last = select([(jnp.logical_and(whole_spans, place == 3), side), (jnp.logical_and(crossing, place == 7), cross_up(span))])
    dn_first, dn_last = select([(jnp.logical_and(whole_spans, place == 4), side), (jnp.logical_and(crossed, place == 0), cross_down(span))])
    up_via = jnp.clip(jnp.where(place == 3, me + 4, me - 2), 0, n - 1)
    dn_via = jnp.clip(jnp.where(place == 4, me - 4, me + 3), 0, n - 1)
    relays_up = jnp.logical_and(whole_spans, jnp.logical_or(place == 7, jnp.logical_and(place == 5, crossing)))
    relays_down = jnp.logical_and(whole_spans, jnp.logical_or(place == 0, jnp.logical_and(place == 3, crossed)))
    near = jnp.logical_or(place == 7, place == 0)
    rl_first, rl_last = select([
        (jnp.logical_and(whole_spans, near), side),
        (jnp.logical_and(crossing, place == 5), cross_up(span)),
        (jnp.logical_and(crossed, place == 3), cross_down(span)),
    ])
    rl_target = jnp.clip(
        jnp.where(place == 7, me - 3, jnp.where(place == 5, me + 3, jnp.where(place == 0, me + 3, me - 4))), 0, n - 1)

    def at(device):
        return dict(device_id=(device,), device_id_type=pl.DeviceIdType.MESH)

    ins = [(u_hbm, u), (v_hbm, v), (w_hbm, w), (s_hbm, s)]

    def load(k, p, first=0, rows=ny, sem=None):
        src, dst = ins[k]
        part = pl.ds(first, rows)
        return pltpu.make_async_copy(src.at[p, part], dst.at[p, part], in_sem.at[k * depth + p if sem is None else sem])

    ob_in = pltpu.make_async_copy(ob_hbm, ob.at[pl.ds(2, depth)], in_sem.at[4 * depth])
    raw_in = [load(k, 0, 0, raw_rows, 4 * depth + k - 1) for k in (2, 3)]
    rest_in = {(k, p): load(k, p, raw_rows, ny - raw_rows) if k >= 2 and p == 0 else load(k, p)
               for k in range(4) for p in range(depth)}
    scan = [(k, p) for k in range(3) for p in range(depth - 1, -1, -1)]
    ob_in.start()
    for pair in scan:
        rest_in[pair].start()
    for copy in raw_in:
        copy.start()

    barrier = pltpu.get_barrier_semaphore()

    def greet(i, carry):
        pl.semaphore_signal(barrier, inc=1, **at(lax.rem(me + i, n)))
        return carry

    lax.fori_loop(1, n, greet, 0)

    zrow = jnp.zeros((PAD, nx), jnp.float32)
    for p in range(1, depth + 2):
        z[p, 0:PAD, :] = zrow
        z[p, ny + PAD : ny + 2 * PAD, :] = zrow
    for p in range(1, depth + 1):
        y[p, 0:PAD, :] = zrow
        y[p, ny + PAD : ny + 2 * PAD, :] = zrow
    for p in range(depth):
        v[p, ny : ny + PAD, :] = zrow
    acc[...] = jnp.zeros_like(acc)

    def zero_planes(ref, planes, offset):
        def body(i, carry):
            for p in planes:
                ref[p, pl.ds(pl.multiple_of(i * ROWS + offset, 8), ROWS), :] = jnp.zeros((ROWS, nx), jnp.float32)
            return carry
        lax.fori_loop(0, nb, body, 0)

    ob_in.wait()
    pl.semaphore_wait(barrier, n - 1)

    ob_down = pltpu.make_async_remote_copy(
        ob.at[pl.ds(2, 1)], ob.at[pl.ds(depth + 2, 1)], ob_send.at[0], ob_recv.at[0], **at(low))
    ob_up = pltpu.make_async_remote_copy(
        ob.at[pl.ds(depth, 2)], ob.at[pl.ds(0, 2)], ob_send.at[1], ob_recv.at[1], **at(high))

    raw_part = pl.ds(0, raw_rows)
    raw_copies = [
        pltpu.make_async_remote_copy(
            src.at[0, raw_part], dst.at[0, raw_part], raw_send, raw_recv, **at(low))
        for src, dst in [(w, lw_next), (s, s_next)]
    ]
    both = lw_next.at[0, pl.ds(0, 2 * raw_rows)]
    raw_whole = pltpu.make_async_remote_copy(both, both, raw_send, raw_recv, **at(low))

    @pl.when(has_low)
    def _():
        ob_down.start()

    @pl.when(has_high)
    def _():
        ob_up.start()

    @pl.when(jnp.logical_not(has_low))
    def _():
        ob[0:2] = jnp.zeros((2,) + ob.shape[1:], jnp.int32)
        zero_planes(z, (0, 1), PAD)

    @pl.when(jnp.logical_not(has_high))
    def _():
        ob[depth + 2 : depth + 3] = jnp.zeros((1,) + ob.shape[1:], jnp.int32)
        zero_planes(z, (depth + 2,), PAD)
        zero_planes(lw_next, (0,), 0)

    def largest(k, p, first, last, m):
        def body(i, m):
            a = jnp.abs(ins[k][1][p, pl.ds(pl.multiple_of(i * ROWS, 8), ROWS), :])
            return jnp.maximum(m, jnp.max(a.reshape(ROWS // 8, 8, nx), axis=0))
        return lax.fori_loop(first, last, body, m)

    peak = jnp.zeros((8, nx), jnp.float32)
    for k, p in scan:
        rest_in[k, p].wait()
        if k == 1:
            rest_in[3, p].start()
        peak = largest(k, p, raw_rows // ROWS if (k, p) == (2, 0) else 0, nb, peak)
    raw_in[0].wait()
    peak = largest(2, 0, 0, raw_rows // ROWS, peak)
    m = jnp.max(peak, axis=0, keepdims=True)
    part = m[:, 0:128]
    for c in range(128, nx, 128):
        part = jnp.maximum(part, m[:, c : c + 128])
    mx[...] = part

    def spread(src, dst, send, recv, step, count):
        def start(i, carry):
            pltpu.make_async_remote_copy(
                src, dst.at[i], send, recv, **at(lax.rem(me + step * i, n))).start()
            return carry

        everything = dst.at[pl.ds(1, count - 1)]
        whole = pltpu.make_async_remote_copy(everything, everything, send, recv, **at(lax.rem(me + step, n)))
        return (lambda: lax.fori_loop(1, count, start, 0)), whole

    mx_start, mx_whole = spread(mx, mx_all, mx_send, mx_recv, 1, n)
    mx_start()
    raw_in[1].wait()

    @pl.when(has_low)
    def _():
        for copy in raw_copies:
            copy.start()

    @pl.when(has_low)
    def _():
        ob_down.wait_send()
        ob_up.wait_recv()

    @pl.when(has_high)
    def _():
        ob_up.wait_send()
        ob_down.wait_recv()

    row_id = lax.broadcasted_iota(jnp.int32, (nb, nx), 0)
    col_id = lax.broadcasted_iota(jnp.int32, (nb, nx), 1)
    srl = lax.shift_right_logical
    c1, c31 = jnp.int32(1), jnp.int32(31)
    full1, full31 = jnp.full((nb, nx), c1), jnp.full((nb, nx), c31)
    for p in range(depth + 1):
        mid = ob[p + 1]
        after = jnp.where(row_id == nb - 1, 0, pltpu.roll(mid, nb - 1, 0))
        before = jnp.where(row_id == 0, 0, pltpu.roll(mid, 1, 0))
        a = srl(mid, full1) | (after << full31)
        b = (mid << full1) | srl(before, full31)
        c = jnp.where(col_id == nx - 1, 0, pltpu.roll(mid, nx - 1, 1))
        d = jnp.where(col_id == 0, 0, pltpu.roll(mid, 1, 1))
        e, f = ob[p], ob[p + 2]
        s1, k1 = a ^ b ^ c, (a & b) | (c & (a | b))
        s2, k2 = d ^ e ^ f, (d & e) | (f & (d | e))
        k3 = s1 & s2
        cw[p, 0] = s1 ^ s2
        cw[p, 1] = k1 ^ k2 ^ k3
        cw[p, 2] = (k1 & k2) | (k3 & (k1 | k2))
        cw[p, 3] = mid
    @pl.when(jnp.logical_not(has_low))
    def _():
        cw[0, 3] = jnp.full((nb, nx), -1, jnp.int32)

    half = 16
    places = lax.broadcasted_iota(jnp.int32, (half, nx), 0)

    def code_rows(b):
        for p in range(depth + 1):
            for k0 in range(0, ROWS, half):
                bits = [
                    srl(jnp.broadcast_to(cw[p, j, pl.ds(b, 1), :], (half, nx)), places + k0) & 1
                    for j in range(4)
                ]
                k = (6 - (bits[0] + (bits[1] << 1) + (bits[2] << 2))).astype(jnp.float32)
                rows = pl.ds(pl.multiple_of(b * ROWS + k0, 8), half)
                code[p, rows, :] = k
                inv[p, rows, :] = jnp.where(bits[3] == 1, 0.0, 1.0 / jnp.maximum(k, 1.0))

    for p in range(depth):
        rest_in[3, p].wait()

    def ready(b, carry):
        code_rows(b)
        return carry

    lax.fori_loop(0, nb // 4, ready, 0)
    mx_whole.wait_recv()
    mx_all[0] = mx[...]
    fastest = jnp.max(jnp.max(mx_all[...], axis=0), axis=1, keepdims=True)
    cf[0:1, :] = (CFL / (jnp.broadcast_to(fastest, (1, nx)) + EPS)) * BUOYANCY

    lane = lax.broadcasted_iota(jnp.int32, (ROWS, nx), 1)

    def lifted(p, r):
        rows = pl.ds(r, ROWS)
        return w[p, rows, :] + cf[0:1, :] * s[p, rows, :]

    def over(c, fn, rows=crow):
        def inner(i, k):
            fn(pl.multiple_of(c * rows + i * ROWS, 8))
            return k
        lax.fori_loop(0, rows // ROWS, inner, 0)

    def staged(first, second, count=chunks):
        def body(c, carry):
            @pl.when(c < count)
            def _():
                first(c)

            @pl.when(c > 0)
            def _():
                second(c - 1)
            return carry
        lax.fori_loop(0, count + 1, body, 0)

    def when(cond, fn):
        @pl.when(cond)
        def _():
            fn()

    class Flow:
        def __init__(self, src, dst, send, recv, device, per, src_pad=PAD, dst_pad=PAD, first=0):
            def copy(start, rows, index):
                def part(pad):
                    return pl.ds(pl.multiple_of(start + pad, 8), rows)
                return pltpu.make_async_remote_copy(
                    src[0].at[src[1], part(src_pad)], dst[0].at[dst[1], part(dst_pad)], send, recv.at[index], **at(device))

            self.start = lambda c: copy(c * crow, crow, c // per).start()
            self.wait_recv = lambda i: copy(i * crow * per, crow * per, i).wait_recv()
            self.start_rest = lambda: copy(first, crow - first % crow, first // crow // per).start()
            self.wait_rest = lambda: copy(first, grow - first, 0).wait_recv()

            def aside(c, unit):
                return pl.ds(pl.multiple_of(unit * grow + lax.rem(c, group) * crow, 8), crow)

            def detour(c, unit, via):
                rows = pl.ds(pl.multiple_of(c * crow + src_pad, 8), crow)
                pltpu.make_async_remote_copy(
                    src[0].at[src[1], rows], relay.at[0, aside(c, unit)], send, relay_recv.at[unit // 2], **at(via)).start()

            def forward(c, unit):
                rows = pl.ds(pl.multiple_of(c * crow + dst_pad, 8), crow)
                pltpu.make_async_remote_copy(
                    relay.at[0, aside(c, unit)], dst[0].at[dst[1], rows], relay_send, recv.at[c // per],
                    **at(rl_target)).start()

            self.detour, self.forward = detour, forward

    lw_down = Flow((lw, 0), (lw_next, 0), send.at[0], lw_recv, low, group, 0, 0, raw_rows)
    z_down = Flow((z, 2), (z, depth + 2), send.at[0], dn_recv, low, group)
    y_down = Flow((y, 1), (y, depth + 1), send.at[0], yd_recv, low, 2 * group)
    top_up = Flow((part_z, 0), (z, 1), send.at[1], top_recv, high, group, 0)
    next_up = Flow((z, top + 1), (z, 0), send.at[1], next_recv, high, 1)

    def send_chunk(flow, second, c, first, last, via):
        unit = c // group + (head if second else head - plane_units)
        aside = jnp.logical_and(unit >= first, unit < last)
        when(aside, lambda: flow.detour(c, jnp.maximum(unit, 0), via))
        when(jnp.logical_not(aside), lambda: flow.start(c))

    def set_aside(first, count):
        part = relay.at[0, pl.ds(0, count * grow)]
        return pltpu.make_async_remote_copy(part, part, relay_send, relay_recv.at[first // 2], **at(rl_target))

    def forward_pair(cond, unit, second):
        def run(flow):
            set_aside(unit, 2).wait_recv()
            for i in range(2 * group):
                flow.forward((unit + (-head if second else plane_units - head)) * group + i, unit + i // group)

        inside = jnp.logical_and(cond, jnp.logical_and(unit >= rl_first, unit < rl_last))
        when(jnp.logical_and(inside, relays_up), lambda: run(next_up if second else top_up))
        when(jnp.logical_and(inside, relays_down), lambda: run(z_down if second else lw_down))

    def flat(p, r):
        a = u[p, pl.ds(r, ROWS), :]
        b = v[p, pl.ds(r, ROWS + PAD), :]
        return jnp.where(lane == nx - 1, 0.0, pltpu.roll(a, nx - 1, 1)) - a + (b[1 : ROWS + 1] - b[:ROWS])

    def inner_rows(r):
        return pl.ds(pl.multiple_of(r + PAD, 8), ROWS)

    def lw_rows(r):
        lw[0, pl.ds(r, ROWS), :] = lifted(0, r)

    def shifted(c):
        return lax.rem(c + raw_rows // crow, chunks)

    def lw_sends(c):
        when(jnp.logical_and(has_low, c * crow >= raw_rows),
             lambda: send_chunk(lw_down, False, c, dn_first, dn_last, dn_via))
        if raw_rows % crow:
            when(jnp.logical_and(has_low, c == raw_rows // crow), lw_down.start_rest)

    staged(lambda c: over(shifted(c), lw_rows), lambda c: lw_sends(shifted(c)))

    def first_rows(r):
        when(r >= ny // 4, lambda: code_rows(r // ROWS))
        rows = pl.ds(r, ROWS)
        part_z[0, rows, :] = inv[top + 1, rows, :] * (flat(top, r) - lifted(top, r))

    staged(lambda c: over(c, first_rows),
           lambda c: when(has_high, lambda: send_chunk(top_up, False, c, up_first, up_last, up_via)))

    def z_rows(p, r):
        rows = pl.ds(r, ROWS)
        own = lw[0, rows, :] if p == 0 else lifted(p, r)
        z[p + 2, inner_rows(r), :] = inv[p + 1, rows, :] * (flat(p, r) + (lifted(p + 1, r) - own))

    for p in range(top):
        def z_sends(c, p=p):
            if p == 0:
                when(has_low, lambda: send_chunk(z_down, True, c, dn_first, dn_last, dn_via))
            if p == top - 1:
                when(has_high, lambda: send_chunk(next_up, True, c, up_first, up_last, up_via))
        staged(lambda c, p=p: over(c, functools.partial(z_rows, p)), z_sends)

    @pl.when(has_high)
    def _():
        raw_whole.wait_recv()

        def lift(i, carry):
            rows = pl.ds(pl.multiple_of(i * ROWS, 8), ROWS)
            lw_next[0, rows, :] = lw_next[0, rows, :] + cf[0:1, :] * s_next[0, rows, :]
            return carry

        lax.fori_loop(0, raw_rows // ROWS, lift, 0)

    def around(ref, slot, r):
        x = ref[slot, pl.ds(r, ROWS + 2 * PAD), :]
        mid = x[PAD : PAD + ROWS]
        beside = x[PAD + 1 : PAD + 1 + ROWS] + x[PAD - 1 : PAD - 1 + ROWS]
        beside = beside + jnp.where(lane == nx - 1, 0.0, pltpu.roll(mid, nx - 1, 1))
        beside = beside + jnp.where(lane == 0, 0.0, pltpu.roll(mid, 1, 1))
        return mid, beside

    def add(j, x):
        acc[j] += jnp.sum(x.reshape(ROWS // 8, 8, nx), axis=0)

    def y_rows(p, r):
        inner, rows = inner_rows(r), pl.ds(r, ROWS)
        k, scale = code[p + 1, rows, :], inv[p + 1, rows, :]
        mid, beside = around(z, p + 2, r)
        q = k * mid - (beside + z[p + 1, inner, :] + z[p + 3, inner, :])
        out = q * scale
        y[p + 1, inner, :] = out
        if p >= 0:
            d = jnp.maximum(k, 1.0) * mid
            add(0, d * mid)
            add(1, d * d)
            add(2, jnp.where(scale > 0.0, 1.0, 0.0))
            add(3, mid * q)
            add(4, q * out)

    def complete_rows(r):
        inner, rows = inner_rows(r), pl.ds(r, ROWS)
        z[top + 2, inner, :] = part_z[0, rows, :] + inv[top + 1, rows, :] * lw_next[0, rows, :]
        z[1, inner, :] = z[1, inner, :] + inv[0, rows, :] * lw[0, rows, :]

    def low_rows(r):
        complete_rows(r)
        for p in range(top):
            y_rows(p, r)

    def low_chunk(c):
        when(jnp.logical_and(has_high, c > 0), lambda: lw_down.wait_recv(c))
        if raw_rows < grow:
            when(jnp.logical_and(has_high, c == 0), lw_down.wait_rest)
        when(has_low, lambda: top_up.wait_recv(c))
        over(c, low_rows, grow)
        forward_pair(jnp.logical_and(near, c == groups - 1), every - few, True)
        forward_pair(jnp.logical_and(jnp.logical_not(near), lax.rem(c, 4) == 3), c // 4 * 2, False)

    def start_y(c):
        for i in range(group):
            y_down.start(c * group + i)

    staged(low_chunk, lambda c: when(jnp.logical_and(has_low, jnp.logical_not(gated)), lambda: start_y(c)), groups)

    def a_rows(p, r):
        inner, rows = inner_rows(r), pl.ds(r, ROWS)
        mid, beside = around(y, p + 1, r)
        below = y[p, inner, :]
        beside = beside + below
        if p < top:
            beside = beside + y[p + 2, inner, :]
        q = code[p + 1, rows, :] * mid - beside
        ay[p, rows, :] = jnp.where(inv[p + 1, rows, :] > 0.0, q, 0.0)
        add(5, mid * (q - below) if p == 0 else mid * q)

    def high_rows(r):
        y_rows(top, r)
        y_rows(-1, r)

    def high_chunk(c):
        when(has_high, lambda: z_down.wait_recv(c))
        for i in range(group):
            chunk = c * group + i
            when(has_low, lambda: next_up.wait_recv(chunk))

            @pl.when(jnp.logical_and(gating, chunk == chunks - LEAD))
            def _():
                pl.delay(LAG)
                pl.semaphore_signal(gate, inc=1, **at(jnp.minimum(me + SPAN - 2, n - 1)))

        @pl.when(jnp.logical_and(gated, c == OPEN))
        def _():
            pl.semaphore_wait(gate, 1)

            def start(i, carry):
                start_y(i)
                return carry

            lax.fori_loop(0, groups, start, 0)

        over(c, high_rows, grow)
        forward_pair(jnp.logical_and(jnp.logical_not(near), c < groups // 2), head + jnp.minimum(2 * c, groups - 2), True)

    def image_rows(r):
        for p in range(depth):
            a_rows(p, r)

    staged(high_chunk, lambda c: over(c, image_rows, grow), groups)

    lanes = lax.broadcasted_iota(jnp.int32, (1, 128), 1)
    sums = jnp.zeros((1, 128), jnp.float32)
    for j in range(6):
        t = jnp.sum(jnp.sum(acc[j], axis=0, keepdims=True), axis=1, keepdims=True)
        sums = jnp.where(lanes == j, jnp.broadcast_to(t, (1, 128)), sums)
    st[...] = sums

    pair_in = pltpu.make_async_remote_copy(st, st_pair, pair_send, pair_recv, **at(partner))
    pair_out = pltpu.make_async_remote_copy(total, total, pair_send, pair_recv, **at(partner))
    st_start, st_whole = spread(st_pair, st_all, st_send, st_recv, 2, n // 2)

    @pl.when(even)
    def _():
        pair_in.start()

    @pl.when(odd)
    def _():
        pair_in.wait_recv()
        st_pair[...] = st_pair[...] + st[...]
        st_start()
        st_whole.wait_recv()
        st_all[0] = st_pair[...]
        total[...] = jnp.sum(st_all[...], axis=0)
        pair_out.start()

    @pl.when(has_low)
    def _():
        raw_whole.wait_send()

    @pl.when(even)
    def _():
        pair_in.wait_send()
        pair_out.wait_recv()

    def summed(j):
        t = jnp.sum(jnp.where(lanes == j, total[...], 0.0), axis=1, keepdims=True)
        return jnp.broadcast_to(t, (1, nx))

    gamma, squares, fluid, delta, eta, theta = (summed(j) for j in range(6))
    alpha = gamma / delta
    gamma_next = gamma - 2.0 * alpha * delta + alpha * alpha * eta
    beta = gamma_next / gamma
    mixed = delta - alpha * eta
    curve = (delta - 2.0 * alpha * eta + alpha * alpha * theta) + 2.0 * beta * mixed + beta * beta * delta
    alpha_next = gamma_next / curve
    norm = 1.0 / jnp.sqrt(squares / jnp.maximum(fluid, 1.0) + EPS)
    cf[1:2, :] = alpha + alpha_next * (1.0 + beta)
    cf[2:3, :] = alpha * alpha_next
    cf[3:4, :] = norm
    cf[4:5, :] = alpha * alpha_next * norm

    def out_rows(r):
        inner, rows = inner_rows(r), pl.ds(r, ROWS)
        a, b = cf[1:2, :], cf[2:3, :]
        for p in range(depth):
            zz, yy = z[p + 2, inner, :], y[p + 1, inner, :]
            w[p, rows, :] = a * zz - b * yy
            s[p, rows, :] = (
                jnp.maximum(code[p + 1, rows, :], 1.0) * (zz - a * yy) + b * ay[p, rows, :]) * cf[3:4, :]

    def all_rows(i, carry):
        out_rows(pl.multiple_of(i * ROWS, 8))
        return carry

    lax.fori_loop(0, nb, all_rows, 0)

    def last_rows(r):
        inner, rows = inner_rows(r), pl.ds(r, ROWS)
        s[top, rows, :] = s[top, rows, :] - jnp.where(
            inv[top + 1, rows, :] > 0.0, cf[4:5, :] * y[depth + 1, inner, :], 0.0)

    @pl.when(has_high)
    def _():
        def last_chunk(c, carry):
            when(lax.rem(c, 2) == 0, lambda: y_down.wait_recv(c // 2))
            over(c, last_rows, grow)
            return carry
        lax.fori_loop(0, groups, last_chunk, 0)

    @pl.when(odd)
    def _():
        st_whole.wait_send()
        pair_out.wait_send()

    def all_sent(index, planes, rows):
        part = code.at[pl.ds(0, planes), pl.ds(0, rows)]
        pltpu.make_async_remote_copy(part, part, send.at[index], lw_recv.at[0], **at(low)).wait_send()

    when(has_low, lambda: all_sent(0, 3, ny - raw_rows // 3))
    when(has_high, lambda: all_sent(1, 2, ny))

    mx_whole.wait_send()

    for count in (few, head, 2 * head, every):
        when(rl_last - rl_first == count, lambda count=count: set_aside(0, count).wait_send())


def store(w, s, w_hbm, s_hbm, sem):
    copies = [
        pltpu.make_async_copy(src.at[p], dst.at[p], sem.at[j, p])
        for j, (src, dst) in enumerate([(w, w_hbm), (s, s_hbm)]) for p in range(w.shape[0])
    ]
    for copy in copies:
        copy.start()
    for copy in copies:
        copy.wait()


def solution(mesh):
    n = mesh.shape["gz"]

    def local(u_face, v_face, w_face, smoke, obstacles):
        depth, ny, nx = u_face.shape
        nw = obstacles.shape[1]
        chunks, group = 16, 2
        raw_rows = 3 * ny // 32
        f32, i32 = jnp.float32, jnp.int32
        dma = pltpu.SemaphoreType.DMA
        any_spec = pl.BlockSpec(memory_space=pl.ANY)
        vmem_spec = pl.BlockSpec(memory_space=pltpu.VMEM)
        shape = pltpu.VMEM((depth, ny, nx), f32)
        results = pl.pallas_call(
            functools.partial(kernel, n, chunks, group, raw_rows),
            out_shape=(shape, shape),
            in_specs=[any_spec] * 5,
            out_specs=(vmem_spec, vmem_spec),
            scratch_shapes=[
                pltpu.VMEM((depth, ny, nx), f32),
                pltpu.VMEM((depth, ny + PAD, nx), f32),
                pltpu.VMEM((depth + 3, ny + 2 * PAD, nx), f32),
                pltpu.VMEM((1, ny, nx), f32),
                pltpu.VMEM((depth + 2, ny + 2 * PAD, nx), f32),
                pltpu.VMEM((depth + 1, ny, nx), f32),
                pltpu.VMEM((depth + 1, ny, nx), f32),
                pltpu.VMEM((depth, ny, nx), f32),
                pltpu.VMEM((1, ny, nx), f32),
                pltpu.VMEM((1, ny, nx), f32),
                pltpu.VMEM((1, raw_rows, nx), f32),
                pltpu.VMEM((1, 3 * ny // 2, nx), f32),
                pltpu.VMEM((depth + 3, nw, nx), i32),
                pltpu.VMEM((depth + 1, 4, nw, nx), i32),
                pltpu.VMEM((6, 8, nx), f32),
                pltpu.VMEM((8, nx), f32),
                pltpu.VMEM((1, 128), f32),
                pltpu.VMEM((n, 1, 128), f32),
                pltpu.VMEM((1, 128), f32),
                pltpu.VMEM((1, 128), f32),
                pltpu.VMEM((n // 2, 1, 128), f32),
                pltpu.VMEM((1, 128), f32),
                dma((4 * depth + 3,)),
                dma((2,)), dma((2,)),
                dma, dma,
                dma((2,)),
                dma((chunks // group,)), dma((chunks // group,)), dma((chunks // group // 2,)), dma((chunks // group,)),
                dma((chunks,)),
                dma((3 * chunks // group // 4,)), dma,
                dma, dma, dma, dma,
                dma, dma,
                pltpu.SemaphoreType.REGULAR,
            ],
            compiler_params=pltpu.CompilerParams(
                collective_id=0, has_side_effects=True, vmem_limit_bytes=58_000_000),
            name="smoke_step",
        )(u_face, v_face, w_face, smoke, obstacles)
        out = jax.ShapeDtypeStruct((depth, ny, nx), f32)
        return pl.pallas_call(
            store,
            out_shape=(out, out),
            in_specs=[vmem_spec] * 2,
            out_specs=(any_spec, any_spec),
            scratch_shapes=[dma((2, depth))],
            compiler_params=pltpu.CompilerParams(vmem_limit_bytes=1_000_000),
            name="store",
        )(*results)

    placed = P("gz", None, None)
    return jax.shard_map(local, mesh=mesh, in_specs=(placed,) * 5, out_specs=(placed, placed), check_vma=False)
```
